32 devices in a mesh: tok: 8 (over z, y), head: 4 (over x, core).
Axes of the slice: x: 2, y: 2, z: 4, core: 2. Of those that a mesh axis runs over, the one named last changes fastest.
Arguments:
- query_rows: bfloat16 [4096, 4, 1024], P('tok', 'head'), may hold values from -6 to 6
- key_rows: bfloat16 [4096, 4, 128], P('tok', 'head'), may hold values from -6 to 6
- value_rows: bfloat16 [4096, 4, 128], P('tok', 'head'), may hold values from -6 to 6
- output_gradient: bfloat16 [4096, 4, 1024], P('tok', 'head'), may hold values from -6 to 6
- row_logsumexp: bfloat16 [4, 8, 4096], P('head', None, 'tok'), may hold values from 3 to 7
- row_delta_sums: bfloat16 [4, 8, 4096], P('head', None, 'tok'), may hold values from -5 to 5
- segments: int32 [4096], replicated, may hold values from 0 to 4095, as said below
- query_key_value_weight: bfloat16 [4096, 4, 1280], P('tok', 'head'), may hold values from -0.09375 to 0.09375
Outputs:
- grad_input: bfloat16 [4096, 4096], P('tok', 'head')
The draws below stay inside these ranges and needn't reach their ends.
Inputs may be any that keep to these rules, and one draw needn't show every extreme that they name: `segments`: numbers never fall along the tokens, and every document lies inside one window of 512 consecutive tokens.
All inputs are finite; a program needn't handle non-finite values.
Results may differ from the reference program's by a relative error of at most 0.012.
Values may be sent and summed in bfloat16 or wider, within the bound.
A program may use at most 128 MiB of HBM per device.

```python
import jax
import jax.numpy as jnp
from jax import lax

MODEL_WIDTH = 4096
QUERY_HEADS = 32
KEY_VALUE_HEADS = 4
HEAD_WIDTH = 128
BLOCK = 128
WINDOW_TOKENS = 512
GROUP_KV_HEADS = 1
TOKEN_TOTAL = 4096
N_TOK = 8


def document_plan(key):
    windows = TOKEN_TOTAL // WINDOW_TOKENS
    half_axis = windows // 2
    window_ids = jnp.arange(windows, dtype=jnp.int32)
    positions = jnp.arange(WINDOW_TOKENS, dtype=jnp.int32)
    sparse_density = jax.random.randint(jax.random.fold_in(key, 11), (windows, 1), 0, 2)
    dense_density = jax.random.randint(jax.random.fold_in(key, 13), (windows, 1), 64, 193)
    density = jnp.where(window_ids[:, None] < half_axis, sparse_density, dense_density)
    rolls = jax.random.randint(jax.random.fold_in(key, 12), (windows, WINDOW_TOKENS), 0, 64 * BLOCK)
    cut_flags = (rolls < density) & (positions[None, :] > 0)
    block_cuts = (positions % BLOCK == 0) & (positions > 0)
    cut_flags = jnp.where(window_ids[:, None] == 0, False, cut_flags)
    cut_flags = jnp.where(window_ids[:, None] == half_axis, block_cuts[None, :], cut_flags)
    local_ids = jnp.cumsum(cut_flags.astype(jnp.int32), axis=1)
    return local_ids + window_ids[:, None] * WINDOW_TOKENS


def draw_segments(key, part):
    return document_plan(key).reshape(TOKEN_TOTAL).astype(jnp.int32)


def levels(stream_key, dims, split, smallest, top_value):
    factor_of, own = 1.0, jax.random.fold_in(stream_key, 6)
    for position, shards_of in split:
        heights = jnp.exp(jax.random.uniform(jax.random.fold_in(own, position), (shards_of,), jnp.float32, smallest / len(split), top_value / len(split)))
        factor_of = factor_of * jnp.repeat(heights, dims[position] // shards_of).reshape([-1 if axis == position else 1 for axis in range(len(dims))])
    return factor_of


def scatter_about(rng, dims, deviation, most, shards=(), held_as=jnp.bfloat16):
    loudness = levels(rng, dims, shards, -0.22, 0.18) if shards else 1.0
    array = jax.random.normal(rng, dims, jnp.float32) * deviation * loudness
    return jnp.minimum(jnp.maximum(array, -most), most).astype(held_as)


def setup_inputs(seed: int = 0) -> dict:
    keys = jax.random.split(jax.random.key(seed), 9)
    return {
        "query_rows": scatter_about(keys[0], (TOKEN_TOTAL, KEY_VALUE_HEADS, QUERY_HEADS // KEY_VALUE_HEADS * HEAD_WIDTH), 1.0, 6.0, ((0, 8), (1, 4))),
        "key_rows": scatter_about(keys[1], (TOKEN_TOTAL, KEY_VALUE_HEADS, HEAD_WIDTH), 1.0, 6.0, ((0, 8), (1, 4))),
        "value_rows": scatter_about(keys[2], (TOKEN_TOTAL, KEY_VALUE_HEADS, HEAD_WIDTH), 1.0, 6.0, ((0, 8), (1, 4))),
        "output_gradient": scatter_about(keys[3], (TOKEN_TOTAL, KEY_VALUE_HEADS, QUERY_HEADS // KEY_VALUE_HEADS * HEAD_WIDTH), 1.0, 6.0, ((0, 8), (1, 4))),
        "row_logsumexp": jnp.clip(3.0 + 4.0 * jax.random.uniform(keys[4], (KEY_VALUE_HEADS, QUERY_HEADS // KEY_VALUE_HEADS, TOKEN_TOTAL), jnp.float32) ** levels(keys[4], (KEY_VALUE_HEADS, QUERY_HEADS // KEY_VALUE_HEADS, TOKEN_TOTAL), ((0, 4), (2, 8)), -0.2, 0.2), 3.0, 7.0).astype(jnp.bfloat16),
        "row_delta_sums": scatter_about(keys[5], (KEY_VALUE_HEADS, QUERY_HEADS // KEY_VALUE_HEADS, TOKEN_TOTAL), 1.0, 5.0, ((0, 4), (2, 8))),
        "segments": draw_segments(jax.random.fold_in(keys[8], 71), 0),
        "query_key_value_weight": scatter_about(keys[7], (MODEL_WIDTH, KEY_VALUE_HEADS, (QUERY_HEADS // KEY_VALUE_HEADS + 2) * HEAD_WIDTH), MODEL_WIDTH ** -0.5, 0.09375, ((0, 8), (1, 4))),
    }


def reference(query_rows, key_rows, value_rows, output_gradient, row_logsumexp, row_delta_sums, segments, query_key_value_weight):
    heads_per_group = QUERY_HEADS // KEY_VALUE_HEADS
    score_scale = HEAD_WIDTH ** -0.5
    offsets = jnp.arange(WINDOW_TOKENS)
    causal = offsets[None, :] <= offsets[:, None]

    def one_window(window_index):
        leading_row = (window_index * WINDOW_TOKENS).astype(jnp.int32)
        query_window_rows = lax.dynamic_slice_in_dim(query_rows, leading_row, WINDOW_TOKENS, 0).astype(jnp.float32).reshape(WINDOW_TOKENS, KEY_VALUE_HEADS, heads_per_group, HEAD_WIDTH)
        output_grad_window = lax.dynamic_slice_in_dim(output_gradient, leading_row, WINDOW_TOKENS, 0).astype(jnp.float32).reshape(WINDOW_TOKENS, KEY_VALUE_HEADS, heads_per_group, HEAD_WIDTH)
        key_win = lax.dynamic_slice_in_dim(key_rows, leading_row, WINDOW_TOKENS, 0).astype(jnp.float32)
        value_win = lax.dynamic_slice_in_dim(value_rows, leading_row, WINDOW_TOKENS, 0).astype(jnp.float32)
        lse_win = lax.dynamic_slice_in_dim(row_logsumexp, leading_row, WINDOW_TOKENS, 2).astype(jnp.float32)
        delta_win = lax.dynamic_slice_in_dim(row_delta_sums, leading_row, WINDOW_TOKENS, 2).astype(jnp.float32)
        seg_win = lax.dynamic_slice_in_dim(segments, leading_row, WINDOW_TOKENS, 0)
        allowed = (seg_win[:, None] == seg_win[None, :]) & causal
        scores = jnp.einsum("agrd,bgd->grab", query_window_rows, key_win) * score_scale
        soft_probs = jnp.where(allowed[None, None], jnp.exp(scores - lse_win[..., None]), 0.0)
        probs_low = lax.optimization_barrier(soft_probs.astype(jnp.bfloat16)).astype(jnp.float32)
        value_gradient = jnp.einsum("grab,agrd->bgd", probs_low, output_grad_window)
        grad_prob = jnp.einsum("agrd,bgd->grab", output_grad_window, value_win)
        grad_score = soft_probs * (grad_prob - delta_win[..., None])
        score_low = lax.optimization_barrier(grad_score.astype(jnp.bfloat16)).astype(jnp.float32)
        query_gradient = jnp.einsum("grab,bgd->agrd", score_low, key_win) * score_scale
        key_gradient = jnp.einsum("grab,agrd->bgd", score_low, query_window_rows) * score_scale
        stacked_gradients = jnp.concatenate([query_gradient.reshape(WINDOW_TOKENS, KEY_VALUE_HEADS, heads_per_group * HEAD_WIDTH), key_gradient, value_gradient], axis=2).astype(jnp.bfloat16)
        running_sum = jnp.zeros((WINDOW_TOKENS, MODEL_WIDTH), jnp.float32)
        for group_of_heads in range(KEY_VALUE_HEADS // GROUP_KV_HEADS):
            first_head = group_of_heads * GROUP_KV_HEADS
            part_rows = stacked_gradients[:, first_head:first_head + GROUP_KV_HEADS, :].reshape(WINDOW_TOKENS, -1)
            part_weights = query_key_value_weight[:, first_head:first_head + GROUP_KV_HEADS, :].reshape(MODEL_WIDTH, -1)
            group_term = jnp.dot(part_rows, part_weights.T, preferred_element_type=jnp.float32)
            running_sum = running_sum + lax.optimization_barrier(group_term.astype(jnp.bfloat16)).astype(jnp.float32)
        return running_sum.astype(jnp.bfloat16)

    return lax.map(one_window, jnp.arange(N_TOK, dtype=jnp.int32)).reshape(TOKEN_TOTAL, MODEL_WIDTH)
```

```python
import functools

import jax
import jax.numpy as jnp
import numpy as np
from jax import lax
from jax.experimental import pallas as pl
from jax.experimental.pallas import tpu as pltpu
from jax.sharding import PartitionSpec as P

BLOCK = 128


def pair_lists(block_count):
    query_list = []
    key_list = []
    for query_block in range(block_count):
        for key_block in range(query_block + 1):
            query_list.append(query_block)
            key_list.append(key_block)
    return (np.array(query_list, np.int32), np.array(key_list, np.int32))


def live_pairs(seg_window, query_list, key_list, tile_rows):
    first_seg = jnp.take(seg_window, query_list * tile_rows)
    last_seg = jnp.take(seg_window, key_list * tile_rows + tile_rows - 1)
    return (first_seg == last_seg) | jnp.asarray(query_list == key_list)


def pair_grads(query_tile, dout_tile, key_tile, value_tile, lse_tile, delta_tile, allowed):
    tile_rows, groups, query_width = query_tile.shape
    head_size = key_tile.shape[2]
    heads_per_group = query_width // head_size
    query_heads = query_tile.reshape(tile_rows, groups, heads_per_group, head_size)
    dout_heads = dout_tile.reshape(tile_rows, groups, heads_per_group, head_size)
    scores = jnp.einsum(
        "agrd,bgd->grab", query_heads, key_tile, preferred_element_type=jnp.float32
    ) * head_size ** (-0.5)
    logits = scores - lse_tile.astype(jnp.float32)[:, :, :, None]
    soft_probs = jnp.where(allowed[None, None], jnp.exp(logits), 0.0)
    probs_low = soft_probs.astype(jnp.bfloat16)
    value_gradient = jnp.einsum(
        "grab,agrd->bgd", probs_low, dout_heads, preferred_element_type=jnp.float32
    )
    grad_prob = jnp.einsum(
        "agrd,bgd->grab", dout_heads, value_tile, preferred_element_type=jnp.float32
    )
    grad_score = (soft_probs * (grad_prob - delta_tile.astype(jnp.float32)[:, :, :, None])).astype(
        jnp.bfloat16
    )
    query_gradient = jnp.einsum(
        "grab,bgd->agrd", grad_score, key_tile, preferred_element_type=jnp.float32
    )
    key_gradient = jnp.einsum(
        "grab,agrd->bgd", grad_score, query_heads, preferred_element_type=jnp.float32
    )
    return (query_gradient.reshape(tile_rows, groups, query_width), key_gradient, value_gradient)


def on_device(
    query_rows,
    key_rows,
    value_rows,
    output_gradient,
    row_logsumexp,
    row_delta_sums,
    segments,
    query_key_value_weight,
):
    window, kv_dev, query_width = query_rows.shape
    head_size = key_rows.shape[2]
    tile_rows = BLOCK
    block_count = window // tile_rows
    query_list, key_list = pair_lists(block_count)
    query_table = jnp.asarray(query_list)
    key_table = jnp.asarray(key_list)
    myself = lax.axis_index("tok")
    own_seg = lax.dynamic_slice_in_dim(segments, myself * window, window)
    own_live = live_pairs(own_seg, query_list, key_list, tile_rows)
    block_ids = jnp.arange(block_count, dtype=jnp.int32)
    query_match = (query_table[:, None] == block_ids[None, :]) & own_live[:, None]
    key_match = key_table[:, None] == block_ids[None, :]
    block_local = jnp.any(query_match[:, :, None] & key_match[:, None, :], axis=0)
    token_local = jnp.repeat(jnp.repeat(block_local, tile_rows, axis=0), tile_rows, axis=1)
    offsets = jnp.arange(window, dtype=jnp.int32)
    allowed_all = (
        (own_seg[:, None] == own_seg[None, :])
        & (offsets[None, :] <= offsets[:, None])
        & token_local
    )
    local_out = pair_grads(
        query_rows,
        output_gradient,
        key_rows,
        value_rows,
        row_logsumexp,
        row_delta_sums,
        allowed_all,
    )
    acc_query = local_out[0].reshape(block_count, tile_rows, kv_dev, query_width)
    acc_key = local_out[1].reshape(block_count, tile_rows, kv_dev, head_size)
    acc_value = local_out[2].reshape(block_count, tile_rows, kv_dev, head_size)
    score_scale = head_size ** (-0.5)
    query_gradient = (acc_query * score_scale).reshape(window, kv_dev, query_width)
    key_gradient = (acc_key * score_scale).reshape(window, kv_dev, head_size)
    value_gradient = acc_value.reshape(window, kv_dev, head_size)
    stacked_gradients = (
        jnp.concatenate([query_gradient, key_gradient, value_gradient], axis=2)
        .astype(jnp.bfloat16)
        .reshape(window, -1)
    )
    weight_piece = lax.all_gather(query_key_value_weight, "tok", axis=0, tiled=True)
    flat_piece = weight_piece.reshape(weight_piece.shape[0], -1)
    partial_sum = lax.dot_general(
        stacked_gradients, flat_piece, (((1,), (1,)), ((), ())), preferred_element_type=jnp.float32
    )
    summed = lax.psum_scatter(
        partial_sum.astype(jnp.bfloat16), "head", scatter_dimension=1, tiled=True
    )
    return summed


MESH = pl.DeviceIdType.MESH
LANES = 128
PIECE = 32


def fused_kernel(
    sides,
    q_hbm,
    k_hbm,
    v_hbm,
    do_hbm,
    lse_ref,
    delta_ref,
    seg_ref,
    w_hbm,
    out_ref,
    q_ref,
    k_ref,
    v_ref,
    do_ref,
    joined,
    w_all,
    keep,
    part_out,
    part_in,
    x_out,
    x_in,
    back_out,
    back_in,
    bias,
    lse32,
    delta32,
    dk_acc,
    dv_acc,
    load_sem,
    own_send,
    own_recv,
    far_send,
    far_recv,
    relay_send,
    relay_recv,
    j_send,
    j_recv,
    part_send,
    part_recv,
    x_send,
    x_recv,
    back_send,
    back_recv,
):
    window, head_size = k_ref.shape
    groups = q_ref.shape[1] // head_size
    rows = w_hbm.shape[0]
    chunks, pieces = rows // LANES, rows // PIECE
    per = LANES // PIECE
    columns = groups + 2
    tok, h = lax.axis_index("tok"), lax.axis_index("head")
    z, y = tok // sides, tok % sides
    x, c = h // sides, h % sides
    yo, xo, co = 1 - y, 1 - x, 1 - c
    odd, upper = z % sides, z // sides
    partner = z + 1 - 2 * odd
    far = z + sides - 2 * sides * upper
    outer = upper == odd
    mine = jnp.where(c == odd, 0, 1)
    final = jnp.where(x == upper, 0, 1)

    def device(dz, dy, dx, dc):
        return (dz * sides + dy, dx * sides + dc)

    y_peer = device(z, yo, x, c)
    far_peer = device(far, y, x, c)
    j_peer = device(partner, y, x, c)
    core_peer = device(z, y, x, co)
    x_peer = device(z, y, xo, c)
    back_peer = device(partner, y, x, co)

    loads = [
        pltpu.make_async_copy(src, dst, load_sem.at[i])
        for i, (src, dst) in enumerate(
            (
                (k_hbm, k_ref),
                (v_hbm, v_ref),
                (q_hbm, q_ref),
                (do_hbm, do_ref),
                (w_hbm, w_all.at[0, y]),
            )
        )
    ]
    for load in loads:
        load.start()

    barrier = pltpu.get_barrier_semaphore()
    peers = (y_peer, far_peer, j_peer, core_peer, x_peer, back_peer)
    for peer in peers:
        pl.semaphore_signal(barrier, inc=1, device_id=peer, device_id_type=MESH)
    pl.semaphore_wait(barrier, len(peers))

    def remote(src, dst, send, recv, peer):
        return pltpu.make_async_remote_copy(
            src_ref=src,
            dst_ref=dst,
            send_sem=send,
            recv_sem=recv,
            device_id=peer,
            device_id_type=MESH,
        )

    def piece_rows(p):
        return pl.ds(pl.multiple_of(p * PIECE, PIECE), PIECE)

    def chunk_rows(k):
        return pl.ds(pl.multiple_of(k * LANES, LANES), LANES)

    def own_copy(p):
        return remote(
            w_hbm.at[piece_rows(p)],
            w_all.at[0, y, piece_rows(p)],
            own_send.at[p],
            own_recv.at[p],
            y_peer,
        )

    def far_copy(p):
        return remote(
            w_hbm.at[piece_rows(p)],
            w_all.at[1, y, piece_rows(p)],
            far_send.at[p],
            far_recv.at[p],
            far_peer,
        )

    def relay_copy(p):
        ref = w_all.at[1, y, piece_rows(p)]
        return remote(ref, ref, relay_send.at[p], relay_recv.at[p], y_peer)

    def arrived_own(p):
        ref = w_all.at[0, yo, piece_rows(p)]
        remote(ref, ref, own_send.at[p], own_recv.at[p], y_peer).wait_recv()

    def arrived_far(p):
        ref = w_all.at[1, y, piece_rows(p)]
        remote(ref, ref, far_send.at[p], far_recv.at[p], far_peer).wait_recv()

    def arrived_relay(p):
        ref = w_all.at[1, yo, piece_rows(p)]
        remote(ref, ref, relay_send.at[p], relay_recv.at[p], y_peer).wait_recv()

    def j_cols(r):
        return pl.ds(pl.multiple_of(r * head_size, head_size), head_size)

    def j_copy(r):
        return remote(
            joined.at[0, :, j_cols(r)],
            joined.at[1, :, j_cols(r)],
            j_send.at[r],
            j_recv.at[r],
            j_peer,
        )

    def each(count, body):
        lax.fori_loop(0, count, lambda i, carry: (body(i), carry)[1], 0)

    first = 2

    each(pieces, lambda p: own_copy(p).start())

    @pl.when(outer)
    def _():
        each(first, lambda p: far_copy(p).start())

    @pl.when(jnp.logical_not(outer))
    def _():
        each(pieces, lambda p: far_copy(p).start())

    lse32[...] = lse_ref[0].astype(jnp.float32)
    delta32[...] = delta_ref[0].astype(jnp.float32)
    seg_row = seg_ref[:, pl.ds(pl.multiple_of(tok * window, LANES), window)].astype(jnp.float32)
    seg_col = jnp.transpose(jnp.broadcast_to(seg_row, (LANES, window)))[:, :1]
    key_id = lax.broadcasted_iota(jnp.int32, (window, window), 0)
    query_id = lax.broadcasted_iota(jnp.int32, (window, window), 1)
    bias[...] = jnp.where((seg_col == seg_row) & (key_id <= query_id), 0.0, -1e30)
    dk_acc[...] = jnp.zeros_like(dk_acc)
    dv_acc[...] = jnp.zeros_like(dv_acc)
    scale = head_size ** (-0.5)
    half = window // 2

    def dot(a, b, da, db):
        return lax.dot_general(a, b, (((da,), (db,)), ((), ())), preferred_element_type=jnp.float32)

    for load in loads[:4]:
        load.wait()

    @pl.loop(0, groups)
    def _(r):
        cols = j_cols(r)
        sums = []
        for start in (0, half):
            keys, queries = slice(start, start + half), slice(start, window)
            q, do = q_ref[queries, cols], do_ref[queries, cols]
            kk, vv = k_ref[keys, :], v_ref[keys, :]
            logits = dot(kk, q, 1, 1) * scale - lse32[pl.ds(r, 1), queries]
            probs = jnp.exp(logits + bias[keys, queries])
            dv_acc[keys, :] += dot(probs.astype(jnp.bfloat16), do, 1, 0)
            grad_prob = dot(vv, do, 1, 1)
            ds = (probs * (grad_prob - delta32[pl.ds(r, 1), queries])).astype(jnp.bfloat16)
            dk_acc[keys, :] += dot(ds, q, 1, 0)
            sums.append(dot(ds, kk, 0, 0))
        low = sums[0]
        joined[0, :half, cols] = (low[:half] * scale).astype(jnp.bfloat16)
        joined[0, half:, cols] = ((low[half:] + sums[1]) * scale).astype(jnp.bfloat16)

        @pl.when(outer)
        def _():
            j_copy(r).start()

    wide = groups * head_size
    joined[0, :, wide : wide + head_size] = (dk_acc[...] * scale).astype(jnp.bfloat16)
    joined[0, :, wide + head_size : wide + 2 * head_size] = dv_acc[...].astype(jnp.bfloat16)
    loads[4].wait()

    def part_copy(slot, yr, k):
        return remote(
            part_out.at[slot, yr, k],
            part_in.at[slot, yr, k],
            part_send.at[slot, yr, k],
            part_recv.at[slot, yr, k],
            core_peer,
        )

    def x_copy(yr, k):
        return remote(
            x_out.at[yr, k], x_in.at[yr, k], x_send.at[yr, k], x_recv.at[yr, k], x_peer
        )

    def back_copy(yr, k):
        return remote(
            back_out.at[yr, k], back_in.at[yr, k], back_send.at[yr, k], back_recv.at[yr, k], back_peer
        )

    def unit(slot, yr, k, side):
        value = dot(joined[side], w_all[slot, yr, chunk_rows(k)], 1, 1)

        @pl.when(mine == side)
        def _():
            keep[slot, yr, k] = value

        @pl.when(mine != side)
        def _():
            part_out[slot, yr, k] = value.astype(jnp.bfloat16)
            part_copy(slot, yr, k).start()

    def core_sum(slot, yr, k):
        part_copy(slot, yr, k).wait_recv()
        value = keep[slot, yr, k] + part_in[slot, yr, k].astype(jnp.float32)

        @pl.when(slot == final)
        def _():
            keep[slot, yr, k] = value

        @pl.when(slot != final)
        def _():
            x_out[yr, k] = value.astype(jnp.bfloat16)
            x_copy(yr, k).start()

    def out_cols(yr, k):
        return pl.ds(pl.multiple_of(yr * rows + k * LANES, LANES), LANES)

    def x_sum(yr, k):
        x_copy(yr, k).wait_recv()
        value = (keep[final, yr, k] + x_in[yr, k].astype(jnp.float32)).astype(jnp.bfloat16)

        @pl.when(mine == 0)
        def _():
            out_ref[:, out_cols(yr, k)] = value

        @pl.when(mine == 1)
        def _():
            back_out[yr, k] = value
            back_copy(yr, k).start()

    def wait_chunk(arrived, k):
        for i in range(per):
            arrived(k * per + i)

    def which(i):
        return jnp.where(i // chunks % 2 == 0, y, yo)

    lag = 2

    @pl.when(outer)
    def _():
        j_copy(groups).start()
        j_copy(groups + 1).start()
        each(pieces - first, lambda p: far_copy(p + first).start())
        steps = 4 * chunks
        share = 2 * pieces // steps

        @pl.loop(0, steps + lag)
        def _(i):
            k = i % chunks

            @pl.when(i < steps // 2)
            def _():
                for j in range(share):
                    arrived_far(i * share + j)
                    relay_copy(i * share + j).start()

            @pl.when((i >= chunks) & (i < 2 * chunks))
            def _():
                wait_chunk(arrived_own, k)

            @pl.when((i >= 3 * chunks) & (i < steps))
            def _():
                wait_chunk(arrived_relay, k)

            @pl.when(i < steps)
            def _():
                unit(i // (2 * chunks), which(i), k, 0)

            @pl.when((i >= lag) & (mine == 0))
            def _():
                core_sum((i - lag) // (2 * chunks), which(i - lag), (i - lag) % chunks)

        @pl.when(mine == 0)
        def _():
            each(2 * chunks, lambda i: x_sum(which(i), i % chunks))

        each(columns, lambda r: j_copy(r).wait_recv())

        @pl.loop(0, chunks + 2)
        def _(k):
            @pl.when(k < chunks)
            def _():
                for slot in (0, 1):
                    for yr in (y, yo):
                        unit(slot, yr, k, 1)

            @pl.when((k >= 1) & (k <= chunks) & (mine == 1))
            def _():
                for slot in (0, 1):
                    for yr in (y, yo):
                        core_sum(slot, yr, k - 1)

            @pl.when((k >= 2) & (mine == 1))
            def _():
                for yr in (y, yo):
                    x_sum(yr, k - 2)

    @pl.when(jnp.logical_not(outer))
    def _():
        @pl.loop(0, 2 * chunks + lag)
        def _(i):
            k = i % chunks

            @pl.when(i == 2 * chunks - 1)
            def _():
                each(columns, lambda r: j_copy(r).start())

            @pl.when((i >= chunks) & (i < 2 * chunks))
            def _():
                wait_chunk(arrived_own, k)

            @pl.when(i < 2 * chunks)
            def _():
                unit(0, which(i), k, 0)

            @pl.when((i >= lag) & (mine == 0))
            def _():
                core_sum(0, which(i - lag), (i - lag) % chunks)

        each(columns, lambda r: j_copy(r).wait_recv())

        @pl.loop(0, 2 * chunks + lag)
        def _(i):
            @pl.when(i < 2 * chunks)
            def _():
                unit(0, which(i), i % chunks, 1)

            @pl.when((i >= lag) & (mine == 1))
            def _():
                core_sum(0, which(i - lag), (i - lag) % chunks)

        @pl.loop(0, chunks + 2)
        def _(k):
            for i in range(per):

                @pl.when(k < chunks)
                def _():
                    arrived_far(k * per + i)
                    relay_copy(k * per + i).start()

                @pl.when((k >= 1) & (k <= chunks))
                def _():
                    if i == 0:
                        unit(1, y, k - 1, 0)
                        unit(1, y, k - 1, 1)
                    if i == 1:
                        wait_chunk(arrived_relay, k - 1)
                        unit(1, yo, k - 1, 0)
                        unit(1, yo, k - 1, 1)
                    if i == 2:
                        core_sum(1, y, k - 1)
                        core_sum(1, yo, k - 1)

                @pl.when(k >= 2)
                def _():
                    if i == 3:
                        x_sum(y, k - 2)
                        x_sum(yo, k - 2)

    @pl.when(mine == 1)
    def _():
        @pl.loop(0, 2 * chunks)
        def _(i):
            k, yr = i // 2, jnp.where(i % 2 == 0, y, yo)
            back_copy(yr, k).wait_recv()
            out_ref[:, out_cols(yr, k)] = back_in[yr, k]
            back_copy(yr, k).wait_send()

    @pl.loop(0, pieces)
    def _(p):
        own_copy(p).wait_send()
        far_copy(p).wait_send()
        relay_copy(p).wait_send()

    each(columns, lambda r: j_copy(r).wait_send())

    @pl.loop(0, 2 * chunks)
    def _(i):
        yr, k = i // chunks, i % chunks
        part_copy(0, yr, k).wait_send()
        part_copy(1, yr, k).wait_send()
        x_copy(yr, k).wait_send()


def fused(sides, q, k, v, do, lse, delta, segments, weight):
    window, _, query_width = q.shape
    head_size = k.shape[2]
    rows, _, width = weight.shape
    chunks, pieces = rows // LANES, rows // PIECE
    columns = width // head_size
    bf16, f32 = jnp.bfloat16, jnp.float32
    dma = pltpu.SemaphoreType.DMA
    vmem = pl.BlockSpec(memory_space=pltpu.VMEM)
    hbm = pl.BlockSpec(memory_space=pl.ANY)
    tile = (window, LANES)
    return pl.pallas_call(
        functools.partial(fused_kernel, sides),
        out_shape=jax.ShapeDtypeStruct((window, 2 * rows), bf16),
        in_specs=[hbm] * 4 + [vmem] * 3 + [hbm],
        out_specs=vmem,
        scratch_shapes=[
            pltpu.VMEM((window, query_width), bf16),
            pltpu.VMEM((window, head_size), bf16),
            pltpu.VMEM((window, head_size), bf16),
            pltpu.VMEM((window, query_width), bf16),
            pltpu.VMEM((2, window, width), bf16),
            pltpu.VMEM((2, 2, rows, width), bf16),
            pltpu.VMEM((2, 2, chunks) + tile, f32),
            pltpu.VMEM((2, 2, chunks) + tile, bf16),
            pltpu.VMEM((2, 2, chunks) + tile, bf16),
            pltpu.VMEM((2, chunks) + tile, bf16),
            pltpu.VMEM((2, chunks) + tile, bf16),
            pltpu.VMEM((2, chunks) + tile, bf16),
            pltpu.VMEM((2, chunks) + tile, bf16),
            pltpu.VMEM((window, window), f32),
            pltpu.VMEM(lse.shape[1:], f32),
            pltpu.VMEM(lse.shape[1:], f32),
            pltpu.VMEM((window, head_size), f32),
            pltpu.VMEM((window, head_size), f32),
            dma((5,)),
            dma((pieces,)),
            dma((pieces,)),
            dma((pieces,)),
            dma((pieces,)),
            dma((pieces,)),
            dma((pieces,)),
            dma((columns,)),
            dma((columns,)),
            dma((2, 2, chunks)),
            dma((2, 2, chunks)),
            dma((2, chunks)),
            dma((2, chunks)),
            dma((2, chunks)),
            dma((2, chunks)),
        ],
        compiler_params=pltpu.CompilerParams(
            collective_id=0, has_side_effects=True, vmem_limit_bytes=60 * 1024 * 1024
        ),
    )(
        q.reshape(window, query_width),
        k.reshape(window, head_size),
        v.reshape(window, head_size),
        do.reshape(window, query_width),
        lse,
        delta,
        segments.reshape(1, -1),
        weight.reshape(rows, width),
    )


def solution(mesh):
    placed = (
        P("tok", "head", None),
        P("tok", "head", None),
        P("tok", "head", None),
        P("tok", "head", None),
        P("head", None, "tok"),
        P("head", None, "tok"),
        P(),
        P("tok", "head", None),
    )
    tok, heads = mesh.shape["tok"], mesh.shape["head"]
    sides = tok // heads

    def step(*args):
        window, kv_dev, _ = args[0].shape
        rows = args[7].shape[0]
        paired = sides == 2 and heads == sides * sides and tok == heads * sides and kv_dev == 1
        if paired and rows % LANES == 0 and window % (2 * LANES) == 0 and args[1].shape[2] == LANES:
            return fused(sides, *args)
        return on_device(*args)

    return jax.shard_map(
        step, mesh=mesh, in_specs=placed, out_specs=P("tok", "head"), check_vma=False
    )
```

```python
import functools

import jax
import jax.numpy as jnp
import numpy as np
from jax import lax
from jax.experimental import pallas as pl
from jax.experimental.pallas import tpu as pltpu
from jax.sharding import PartitionSpec as P

BLOCK = 128


def pair_lists(block_count):
    query_list = []
    key_list = []
    for query_block in range(block_count):
        for key_block in range(query_block + 1):
            query_list.append(query_block)
            key_list.append(key_block)
    return (np.array(query_list, np.int32), np.array(key_list, np.int32))


def live_pairs(seg_window, query_list, key_list, tile_rows):
    first_seg = jnp.take(seg_window, query_list * tile_rows)
    last_seg = jnp.take(seg_window, key_list * tile_rows + tile_rows - 1)
    return (first_seg == last_seg) | jnp.asarray(query_list == key_list)


def pair_grads(query_tile, dout_tile, key_tile, value_tile, lse_tile, delta_tile, allowed):
    tile_rows, groups, query_width = query_tile.shape
    head_size = key_tile.shape[2]
    heads_per_group = query_width // head_size
    query_heads = query_tile.reshape(tile_rows, groups, heads_per_group, head_size)
    dout_heads = dout_tile.reshape(tile_rows, groups, heads_per_group, head_size)
    scores = jnp.einsum(
        "agrd,bgd->grab", query_heads, key_tile, preferred_element_type=jnp.float32
    ) * head_size ** (-0.5)
    logits = scores - lse_tile.astype(jnp.float32)[:, :, :, None]
    soft_probs = jnp.where(allowed[None, None], jnp.exp(logits), 0.0)
    probs_low = soft_probs.astype(jnp.bfloat16)
    value_gradient = jnp.einsum(
        "grab,agrd->bgd", probs_low, dout_heads, preferred_element_type=jnp.float32
    )
    grad_prob = jnp.einsum(
        "agrd,bgd->grab", dout_heads, value_tile, preferred_element_type=jnp.float32
    )
    grad_score = (soft_probs * (grad_prob - delta_tile.astype(jnp.float32)[:, :, :, None])).astype(
        jnp.bfloat16
    )
    query_gradient = jnp.einsum(
        "grab,bgd->agrd", grad_score, key_tile, preferred_element_type=jnp.float32
    )
    key_gradient = jnp.einsum(
        "grab,agrd->bgd", grad_score, query_heads, preferred_element_type=jnp.float32
    )
    return (query_gradient.reshape(tile_rows, groups, query_width), key_gradient, value_gradient)


def on_device(
    query_rows,
    key_rows,
    value_rows,
    output_gradient,
    row_logsumexp,
    row_delta_sums,
    segments,
    query_key_value_weight,
):
    window, kv_dev, query_width = query_rows.shape
    head_size = key_rows.shape[2]
    tile_rows = BLOCK
    block_count = window // tile_rows
    query_list, key_list = pair_lists(block_count)
    query_table = jnp.asarray(query_list)
    key_table = jnp.asarray(key_list)
    myself = lax.axis_index("tok")
    own_seg = lax.dynamic_slice_in_dim(segments, myself * window, window)
    own_live = live_pairs(own_seg, query_list, key_list, tile_rows)
    block_ids = jnp.arange(block_count, dtype=jnp.int32)
    query_match = (query_table[:, None] == block_ids[None, :]) & own_live[:, None]
    key_match = key_table[:, None] == block_ids[None, :]
    block_local = jnp.any(query_match[:, :, None] & key_match[:, None, :], axis=0)
    token_local = jnp.repeat(jnp.repeat(block_local, tile_rows, axis=0), tile_rows, axis=1)
    offsets = jnp.arange(window, dtype=jnp.int32)
    allowed_all = (
        (own_seg[:, None] == own_seg[None, :])
        & (offsets[None, :] <= offsets[:, None])
        & token_local
    )
    local_out = pair_grads(
        query_rows,
        output_gradient,
        key_rows,
        value_rows,
        row_logsumexp,
        row_delta_sums,
        allowed_all,
    )
    acc_query = local_out[0].reshape(block_count, tile_rows, kv_dev, query_width)
    acc_key = local_out[1].reshape(block_count, tile_rows, kv_dev, head_size)
    acc_value = local_out[2].reshape(block_count, tile_rows, kv_dev, head_size)
    score_scale = head_size ** (-0.5)
    query_gradient = (acc_query * score_scale).reshape(window, kv_dev, query_width)
    key_gradient = (acc_key * score_scale).reshape(window, kv_dev, head_size)
    value_gradient = acc_value.reshape(window, kv_dev, head_size)
    stacked_gradients = (
        jnp.concatenate([query_gradient, key_gradient, value_gradient], axis=2)
        .astype(jnp.bfloat16)
        .reshape(window, -1)
    )
    weight_piece = lax.all_gather(query_key_value_weight, "tok", axis=0, tiled=True)
    flat_piece = weight_piece.reshape(weight_piece.shape[0], -1)
    partial_sum = lax.dot_general(
        stacked_gradients, flat_piece, (((1,), (1,)), ((), ())), preferred_element_type=jnp.float32
    )
    summed = lax.psum_scatter(
        partial_sum.astype(jnp.bfloat16), "head", scatter_dimension=1, tiled=True
    )
    return summed


MESH = pl.DeviceIdType.MESH
LANES = 128
PIECE = 32


def fused_kernel(
    sides,
    q_hbm,
    k_hbm,
    v_hbm,
    do_hbm,
    lse_ref,
    delta_ref,
    seg_ref,
    w_hbm,
    out_ref,
    q_ref,
    k_ref,
    v_ref,
    do_ref,
    joined,
    w_all,
    keep,
    part_out,
    part_in,
    x_out,
    x_in,
    back_out,
    bias,
    lse32,
    delta32,
    dk_acc,
    dv_acc,
    load_sem,
    own_send,
    own_recv,
    far_send,
    far_recv,
    relay_send,
    relay_recv,
    j_send,
    j_recv,
    part_send,
    part_recv,
    x_send,
    x_recv,
    back_send,
    back_recv,
):
    window, head_size = k_ref.shape
    groups = q_ref.shape[1] // head_size
    rows = w_hbm.shape[0]
    chunks, pieces = rows // LANES, rows // PIECE
    per = LANES // PIECE
    block = window // chunks
    columns = groups + 2
    tok, h = lax.axis_index("tok"), lax.axis_index("head")
    z, y = tok // sides, tok % sides
    x, c = h // sides, h % sides
    yo, xo, co = 1 - y, 1 - x, 1 - c
    odd, upper = z % sides, z // sides
    partner = z + 1 - 2 * odd
    far = z + sides - 2 * sides * upper
    outer = upper == odd
    mine = jnp.where(c == odd, 0, 1)
    final = jnp.where(x == upper, 0, 1)

    def device(dz, dy, dx, dc):
        return (dz * sides + dy, dx * sides + dc)

    y_peer = device(z, yo, x, c)
    far_peer = device(far, y, x, c)
    j_peer = device(partner, y, x, c)
    core_peer = device(z, y, x, co)
    x_peer = device(z, y, xo, c)
    back_peer = device(partner, y, x, co)

    loads = [
        pltpu.make_async_copy(src, dst, load_sem.at[i])
        for i, (src, dst) in enumerate(
            (
                (k_hbm, k_ref),
                (v_hbm, v_ref),
                (q_hbm, q_ref),
                (do_hbm, do_ref),
                (w_hbm, w_all.at[0, y]),
            )
        )
    ]
    for load in loads:
        load.start()

    barrier = pltpu.get_barrier_semaphore()
    peers = (y_peer, far_peer, j_peer, core_peer, x_peer, back_peer)
    for peer in peers:
        pl.semaphore_signal(barrier, inc=1, device_id=peer, device_id_type=MESH)
    pl.semaphore_wait(barrier, len(peers))

    def remote(src, dst, send, recv, peer):
        return pltpu.make_async_remote_copy(
            src_ref=src,
            dst_ref=dst,
            send_sem=send,
            recv_sem=recv,
            device_id=peer,
            device_id_type=MESH,
        )

    def piece_rows(p):
        return pl.ds(pl.multiple_of(p * PIECE, PIECE), PIECE)

    def chunk_rows(k):
        return pl.ds(pl.multiple_of(k * LANES, LANES), LANES)

    def block_rows(i):
        return pl.ds(pl.multiple_of(i * block, block), block)

    def own_copy(p):
        return remote(
            w_hbm.at[piece_rows(p)],
            w_all.at[0, y, piece_rows(p)],
            own_send.at[p],
            own_recv.at[p],
            y_peer,
        )

    def far_copy(p):
        return remote(
            w_hbm.at[piece_rows(p)],
            w_all.at[1, y, piece_rows(p)],
            far_send.at[p],
            far_recv.at[p],
            far_peer,
        )

    def relay_copy(p):
        ref = w_all.at[1, y, piece_rows(p)]
        return remote(ref, ref, relay_send.at[p], relay_recv.at[p], y_peer)

    def arrived_own(p):
        ref = w_all.at[0, yo, piece_rows(p)]
        remote(ref, ref, own_send.at[p], own_recv.at[p], y_peer).wait_recv()

    def arrived_far(p):
        ref = w_all.at[1, y, piece_rows(p)]
        remote(ref, ref, far_send.at[p], far_recv.at[p], far_peer).wait_recv()

    def arrived_relay(p):
        ref = w_all.at[1, yo, piece_rows(p)]
        remote(ref, ref, relay_send.at[p], relay_recv.at[p], y_peer).wait_recv()

    def j_cols(r):
        return pl.ds(pl.multiple_of(r * head_size, head_size), head_size)

    def j_copy(r):
        return remote(
            joined.at[0, :, j_cols(r)],
            joined.at[1, :, j_cols(r)],
            j_send.at[r],
            j_recv.at[r],
            j_peer,
        )

    def j_block(i):
        return remote(
            joined.at[0, block_rows(i)],
            joined.at[1, block_rows(i)],
            j_send.at[i],
            j_recv.at[i],
            j_peer,
        )

    def each(count, body):
        lax.fori_loop(0, count, lambda i, carry: (body(i), carry)[1], 0)

    first = 2

    each(pieces, lambda p: own_copy(p).start())

    @pl.when(outer)
    def _():
        each(first, lambda p: far_copy(p).start())

    @pl.when(jnp.logical_not(outer))
    def _():
        each(pieces, lambda p: far_copy(p).start())

    lse32[...] = lse_ref[0].astype(jnp.float32)
    delta32[...] = delta_ref[0].astype(jnp.float32)
    seg_row = seg_ref[:, pl.ds(pl.multiple_of(tok * window, LANES), window)].astype(jnp.float32)
    seg_col = jnp.transpose(jnp.broadcast_to(seg_row, (LANES, window)))[:, :1]
    key_id = lax.broadcasted_iota(jnp.int32, (window, window), 0)
    query_id = lax.broadcasted_iota(jnp.int32, (window, window), 1)
    bias[...] = jnp.where((seg_col == seg_row) & (key_id <= query_id), 0.0, -1e30)
    dk_acc[...] = jnp.zeros_like(dk_acc)
    dv_acc[...] = jnp.zeros_like(dv_acc)
    scale = head_size ** (-0.5)
    half = window // 2

    def dot(a, b, da, db):
        return lax.dot_general(a, b, (((da,), (db,)), ((), ())), preferred_element_type=jnp.float32)

    for load in loads[:4]:
        load.wait()

    @pl.loop(0, groups)
    def _(r):
        cols = j_cols(r)
        sums = []
        for start in (0, half):
            keys, queries = slice(start, start + half), slice(start, window)
            q, do = q_ref[queries, cols], do_ref[queries, cols]
            kk, vv = k_ref[keys, :], v_ref[keys, :]
            logits = dot(kk, q, 1, 1) * scale - lse32[pl.ds(r, 1), queries]
            probs = jnp.exp(logits + bias[keys, queries])
            dv_acc[keys, :] += dot(probs.astype(jnp.bfloat16), do, 1, 0)
            grad_prob = dot(vv, do, 1, 1)
            ds = (probs * (grad_prob - delta32[pl.ds(r, 1), queries])).astype(jnp.bfloat16)
            dk_acc[keys, :] += dot(ds, q, 1, 0)
            sums.append(dot(ds, kk, 0, 0))
        low = sums[0]
        joined[0, :half, cols] = (low[:half] * scale).astype(jnp.bfloat16)
        joined[0, half:, cols] = ((low[half:] + sums[1]) * scale).astype(jnp.bfloat16)

        @pl.when(outer)
        def _():
            j_copy(r).start()

    wide = groups * head_size
    joined[0, :, wide : wide + head_size] = (dk_acc[...] * scale).astype(jnp.bfloat16)
    joined[0, :, wide + head_size : wide + 2 * head_size] = dv_acc[...].astype(jnp.bfloat16)
    loads[4].wait()

    def tile(ref, lead, i, by_token):
        return ref.at[(*lead, slice(None), block_rows(i))] if by_token else ref.at[(*lead, i)]

    def part_copy(slot, yr, i, by_token):
        return remote(
            tile(part_out, (slot, yr), i, by_token),
            tile(part_in, (slot, yr), i, by_token),
            part_send.at[slot, yr, i],
            part_recv.at[slot, yr, i],
            core_peer,
        )

    def x_copy(yr, i, by_token):
        return remote(
            tile(x_out, (yr,), i, by_token),
            tile(x_in, (yr,), i, by_token),
            x_send.at[yr, i],
            x_recv.at[yr, i],
            x_peer,
        )

    def out_cols(yr, k):
        return pl.ds(pl.multiple_of(yr * rows + k * LANES, LANES), LANES)

    def out_tile(ref, yr, i, by_token):
        if by_token:
            return ref.at[block_rows(i), pl.ds(pl.multiple_of(yr * rows, LANES), rows)]
        return ref.at[:, out_cols(yr, i)]

    def back_copy(yr, i, by_token):
        return remote(
            out_tile(back_out, yr, i, by_token),
            out_tile(out_ref, yr, i, by_token),
            back_send.at[yr, i],
            back_recv.at[yr, i],
            back_peer,
        )

    def unit(slot, yr, k, side):
        value = dot(joined[side], w_all[slot, yr, chunk_rows(k)], 1, 1)

        @pl.when(mine == side)
        def _():
            keep[slot, yr, k] = value

        @pl.when(mine != side)
        def _():
            part_out[slot, yr, k] = value.astype(jnp.bfloat16)
            part_copy(slot, yr, k, False).start()

    def block_unit(slot, yr, i):
        value = dot(joined[1, block_rows(i)], w_all[slot, yr], 1, 1)

        @pl.when(mine == 1)
        def _():
            for k in range(chunks):
                keep[slot, yr, k, block_rows(i)] = value[:, k * LANES : (k + 1) * LANES]

        @pl.when(mine == 0)
        def _():
            low = value.astype(jnp.bfloat16)
            for k in range(chunks):
                part_out[slot, yr, k, block_rows(i)] = low[:, k * LANES : (k + 1) * LANES]
            part_copy(slot, yr, i, True).start()

    def core_sum(slot, yr, i, by_token):
        part_copy(slot, yr, i, by_token).wait_recv()
        kept = tile(keep, (slot, yr), i, by_token)
        value = kept[...] + tile(part_in, (slot, yr), i, by_token)[...].astype(jnp.float32)

        @pl.when(slot == final)
        def _():
            kept[...] = value

        @pl.when(slot != final)
        def _():
            tile(x_out, (yr,), i, by_token)[...] = value.astype(jnp.bfloat16)
            x_copy(yr, i, by_token).start()

    def x_sum(yr, i, by_token):
        x_copy(yr, i, by_token).wait_recv()
        value = tile(keep, (final, yr), i, by_token)[...]
        value += tile(x_in, (yr,), i, by_token)[...].astype(jnp.float32)
        value = value.astype(jnp.bfloat16)

        def put(ref):
            if by_token:
                for k in range(chunks):
                    ref[block_rows(i), out_cols(yr, k)] = value[k]
            else:
                ref[:, out_cols(yr, i)] = value

        if by_token:
            put(back_out)
            back_copy(yr, i, True).start()
        else:

            @pl.when(mine == 0)
            def _():
                put(out_ref)

            @pl.when(mine == 1)
            def _():
                put(back_out)
                back_copy(yr, i, False).start()

    def wait_chunk(arrived, k):
        for i in range(per):
            arrived(k * per + i)

    def which(i):
        return jnp.where(i // chunks % 2 == 0, y, yo)

    lag = 2

    @pl.when(outer)
    def _():
        j_copy(groups).start()
        j_copy(groups + 1).start()
        each(pieces - first, lambda p: far_copy(p + first).start())
        steps = 3 * chunks
        share = pieces // (2 * chunks)

        @pl.loop(0, steps + lag)
        def _(i):
            k = i % chunks

            @pl.when(i < 2 * chunks)
            def _():
                for j in range(share):
                    arrived_far(i * share + j)
                    relay_copy(i * share + j).start()

            @pl.when((i >= chunks) & (i < 2 * chunks))
            def _():
                wait_chunk(arrived_own, k)

            @pl.when(i < steps)
            def _():
                unit(i // (2 * chunks), which(i), k, 0)

            @pl.when((i >= lag) & (mine == 0))
            def _():
                core_sum((i - lag) // (2 * chunks), which(i - lag), (i - lag) % chunks, False)

        @pl.loop(0, chunks + 2)
        def _(i):
            @pl.when(i < chunks)
            def _():
                wait_chunk(arrived_relay, i)
                unit(1, yo, i, 0)
                j_block(i).wait_recv()
                block_unit(0, y, i)
                block_unit(0, yo, i)
                block_unit(1, y, i)

            @pl.when(i == chunks)
            def _():
                each(chunks, lambda j: block_unit(1, yo, j))

            @pl.when(mine == 0)
            def _():
                @pl.when((i >= 1) & (i <= chunks))
                def _():
                    core_sum(1, yo, i - 1, False)
                    x_sum(y, i - 1, False)

                @pl.when(i >= 2)
                def _():
                    x_sum(yo, i - 2, False)

            @pl.when(mine == 1)
            def _():
                @pl.when((i >= 1) & (i <= chunks))
                def _():
                    for slot, yr in ((0, y), (0, yo), (1, y)):
                        core_sum(slot, yr, i - 1, True)

                @pl.when(i == chunks + 1)
                def _():
                    each(chunks, lambda j: core_sum(1, yo, j, True))

                @pl.when(i >= 2)
                def _():
                    x_sum(y, i - 2, True)

                @pl.when((i >= 2) & (final == 0))
                def _():
                    x_sum(yo, i - 2, True)

        @pl.when((mine == 1) & (final == 1))
        def _():
            each(chunks, lambda j: x_sum(yo, j, True))

    @pl.when(jnp.logical_not(outer))
    def _():
        @pl.loop(0, 2 * chunks + lag)
        def _(i):
            k = i % chunks

            @pl.when(i == 2 * chunks - 1)
            def _():
                each(chunks, lambda j: j_block(j).start())

            @pl.when((i >= chunks) & (i < 2 * chunks))
            def _():
                wait_chunk(arrived_own, k)

            @pl.when(i < 2 * chunks)
            def _():
                unit(0, which(i), k, 0)

            @pl.when((i >= lag) & (mine == 0))
            def _():
                core_sum(0, which(i - lag), (i - lag) % chunks, False)

        each(columns, lambda r: j_copy(r).wait_recv())

        @pl.loop(0, chunks + 2)
        def _(k):
            for i in range(per):

                @pl.when(k < chunks)
                def _():
                    arrived_far(k * per + i)
                    relay_copy(k * per + i).start()

                @pl.when(k == 0)
                def _():
                    for j in range(i * 2 * chunks // per, (i + 1) * 2 * chunks // per):
                        unit(0, which(j), j % chunks, 1)

                @pl.when((k == 1) & (mine == 1))
                def _():
                    for j in range(i * 2 * chunks // per, (i + 1) * 2 * chunks // per):
                        core_sum(0, which(j), j % chunks, False)

                @pl.when((k >= 1) & (k <= chunks))
                def _():
                    if i == 0:
                        unit(1, y, k - 1, 0)
                    if i == 1:
                        unit(1, y, k - 1, 1)
                    if i == 2:
                        wait_chunk(arrived_relay, k - 1)
                        unit(1, yo, k - 1, 0)
                        core_sum(1, y, k - 1, False)
                    if i == 3:
                        unit(1, yo, k - 1, 1)

                @pl.when(k >= 2)
                def _():
                    if i == 0:
                        core_sum(1, yo, k - 2, False)
                    if i == 1:
                        x_sum(y, k - 2, False)
                    if i == 3:
                        x_sum(yo, k - 2, False)

    @pl.when(mine == 1)
    def _():
        @pl.loop(0, 2 * chunks)
        def _(i):
            back_copy(i // chunks, i % chunks, False).wait_recv()
            back_copy(i // chunks, i % chunks, False).wait_send()

    @pl.loop(0, pieces)
    def _(p):
        own_copy(p).wait_send()
        far_copy(p).wait_send()
        relay_copy(p).wait_send()

    @pl.when(outer)
    def _():
        each(columns, lambda r: j_copy(r).wait_send())

    @pl.when(jnp.logical_not(outer))
    def _():
        each(chunks, lambda i: j_block(i).wait_send())

    @pl.loop(0, 2 * chunks)
    def _(i):
        yr, k = i // chunks, i % chunks
        part_copy(0, yr, k, False).wait_send()
        part_copy(1, yr, k, False).wait_send()
        x_copy(yr, k, False).wait_send()


def fused(sides, q, k, v, do, lse, delta, segments, weight):
    window, _, query_width = q.shape
    head_size = k.shape[2]
    rows, _, width = weight.shape
    chunks, pieces = rows // LANES, rows // PIECE
    columns = width // head_size
    bf16, f32 = jnp.bfloat16, jnp.float32
    dma = pltpu.SemaphoreType.DMA
    vmem = pl.BlockSpec(memory_space=pltpu.VMEM)
    hbm = pl.BlockSpec(memory_space=pl.ANY)
    tile = (window, LANES)
    return pl.pallas_call(
        functools.partial(fused_kernel, sides),
        out_shape=jax.ShapeDtypeStruct((window, 2 * rows), bf16),
        in_specs=[hbm] * 4 + [vmem] * 3 + [hbm],
        out_specs=vmem,
        scratch_shapes=[
            pltpu.VMEM((window, query_width), bf16),
            pltpu.VMEM((window, head_size), bf16),
            pltpu.VMEM((window, head_size), bf16),
            pltpu.VMEM((window, query_width), bf16),
            pltpu.VMEM((2, window, width), bf16),
            pltpu.VMEM((2, 2, rows, width), bf16),
            pltpu.VMEM((2, 2, chunks) + tile, f32),
            pltpu.VMEM((2, 2, chunks) + tile, bf16),
            pltpu.VMEM((2, 2, chunks) + tile, bf16),
            pltpu.VMEM((2, chunks) + tile, bf16),
            pltpu.VMEM((2, chunks) + tile, bf16),
            pltpu.VMEM((window, 2 * rows), bf16),
            pltpu.VMEM((window, window), f32),
            pltpu.VMEM(lse.shape[1:], f32),
            pltpu.VMEM(lse.shape[1:], f32),
            pltpu.VMEM((window, head_size), f32),
            pltpu.VMEM((window, head_size), f32),
            dma((5,)),
            dma((pieces,)),
            dma((pieces,)),
            dma((pieces,)),
            dma((pieces,)),
            dma((pieces,)),
            dma((pieces,)),
            dma((columns,)),
            dma((columns,)),
            dma((2, 2, chunks)),
            dma((2, 2, chunks)),
            dma((2, chunks)),
            dma((2, chunks)),
            dma((2, chunks)),
            dma((2, chunks)),
        ],
        compiler_params=pltpu.CompilerParams(
            collective_id=0, has_side_effects=True, vmem_limit_bytes=60 * 1024 * 1024
        ),
    )(
        q.reshape(window, query_width),
        k.reshape(window, head_size),
        v.reshape(window, head_size),
        do.reshape(window, query_width),
        lse,
        delta,
        segments.reshape(1, -1),
        weight.reshape(rows, width),
    )


def solution(mesh):
    placed = (
        P("tok", "head", None),
        P("tok", "head", None),
        P("tok", "head", None),
        P("tok", "head", None),
        P("head", None, "tok"),
        P("head", None, "tok"),
        P(),
        P("tok", "head", None),
    )
    tok, heads = mesh.shape["tok"], mesh.shape["head"]
    sides = tok // heads

    def step(*args):
        window, kv_dev, _ = args[0].shape
        rows = args[7].shape[0]
        paired = sides == 2 and heads == sides * sides and tok == heads * sides and kv_dev == 1
        if paired and rows % LANES == 0 and window % (2 * LANES) == 0 and args[1].shape[2] == LANES:
            return fused(sides, *args)
        return on_device(*args)

    return jax.shard_map(
        step, mesh=mesh, in_specs=placed, out_specs=P("tok", "head"), check_vma=False
    )
```

```python
import functools

import jax
import jax.numpy as jnp
import numpy as np
from jax import lax
from jax.experimental import pallas as pl
from jax.experimental.pallas import tpu as pltpu
from jax.sharding import PartitionSpec as P

BLOCK = 128


def pair_lists(block_count):
    query_list = []
    key_list = []
    for query_block in range(block_count):
        for key_block in range(query_block + 1):
            query_list.append(query_block)
            key_list.append(key_block)
    return (np.array(query_list, np.int32), np.array(key_list, np.int32))


def live_pairs(seg_window, query_list, key_list, tile_rows):
    first_seg = jnp.take(seg_window, query_list * tile_rows)
    last_seg = jnp.take(seg_window, key_list * tile_rows + tile_rows - 1)
    return (first_seg == last_seg) | jnp.asarray(query_list == key_list)


def pair_grads(query_tile, dout_tile, key_tile, value_tile, lse_tile, delta_tile, allowed):
    tile_rows, groups, query_width = query_tile.shape
    head_size = key_tile.shape[2]
    heads_per_group = query_width // head_size
    query_heads = query_tile.reshape(tile_rows, groups, heads_per_group, head_size)
    dout_heads = dout_tile.reshape(tile_rows, groups, heads_per_group, head_size)
    scores = jnp.einsum(
        "agrd,bgd->grab", query_heads, key_tile, preferred_element_type=jnp.float32
    ) * head_size ** (-0.5)
    logits = scores - lse_tile.astype(jnp.float32)[:, :, :, None]
    soft_probs = jnp.where(allowed[None, None], jnp.exp(logits), 0.0)
    probs_low = soft_probs.astype(jnp.bfloat16)
    value_gradient = jnp.einsum(
        "grab,agrd->bgd", probs_low, dout_heads, preferred_element_type=jnp.float32
    )
    grad_prob = jnp.einsum(
        "agrd,bgd->grab", dout_heads, value_tile, preferred_element_type=jnp.float32
    )
    grad_score = (soft_probs * (grad_prob - delta_tile.astype(jnp.float32)[:, :, :, None])).astype(
        jnp.bfloat16
    )
    query_gradient = jnp.einsum(
        "grab,bgd->agrd", grad_score, key_tile, preferred_element_type=jnp.float32
    )
    key_gradient = jnp.einsum(
        "grab,agrd->bgd", grad_score, query_heads, preferred_element_type=jnp.float32
    )
    return (query_gradient.reshape(tile_rows, groups, query_width), key_gradient, value_gradient)


def on_device(
    query_rows,
    key_rows,
    value_rows,
    output_gradient,
    row_logsumexp,
    row_delta_sums,
    segments,
    query_key_value_weight,
):
    window, kv_dev, query_width = query_rows.shape
    head_size = key_rows.shape[2]
    tile_rows = BLOCK
    block_count = window // tile_rows
    query_list, key_list = pair_lists(block_count)
    query_table = jnp.asarray(query_list)
    key_table = jnp.asarray(key_list)
    myself = lax.axis_index("tok")
    own_seg = lax.dynamic_slice_in_dim(segments, myself * window, window)
    own_live = live_pairs(own_seg, query_list, key_list, tile_rows)
    block_ids = jnp.arange(block_count, dtype=jnp.int32)
    query_match = (query_table[:, None] == block_ids[None, :]) & own_live[:, None]
    key_match = key_table[:, None] == block_ids[None, :]
    block_local = jnp.any(query_match[:, :, None] & key_match[:, None, :], axis=0)
    token_local = jnp.repeat(jnp.repeat(block_local, tile_rows, axis=0), tile_rows, axis=1)
    offsets = jnp.arange(window, dtype=jnp.int32)
    allowed_all = (
        (own_seg[:, None] == own_seg[None, :])
        & (offsets[None, :] <= offsets[:, None])
        & token_local
    )
    local_out = pair_grads(
        query_rows,
        output_gradient,
        key_rows,
        value_rows,
        row_logsumexp,
        row_delta_sums,
        allowed_all,
    )
    acc_query = local_out[0].reshape(block_count, tile_rows, kv_dev, query_width)
    acc_key = local_out[1].reshape(block_count, tile_rows, kv_dev, head_size)
    acc_value = local_out[2].reshape(block_count, tile_rows, kv_dev, head_size)
    score_scale = head_size ** (-0.5)
    query_gradient = (acc_query * score_scale).reshape(window, kv_dev, query_width)
    key_gradient = (acc_key * score_scale).reshape(window, kv_dev, head_size)
    value_gradient = acc_value.reshape(window, kv_dev, head_size)
    stacked_gradients = (
        jnp.concatenate([query_gradient, key_gradient, value_gradient], axis=2)
        .astype(jnp.bfloat16)
        .reshape(window, -1)
    )
    weight_piece = lax.all_gather(query_key_value_weight, "tok", axis=0, tiled=True)
    flat_piece = weight_piece.reshape(weight_piece.shape[0], -1)
    partial_sum = lax.dot_general(
        stacked_gradients, flat_piece, (((1,), (1,)), ((), ())), preferred_element_type=jnp.float32
    )
    summed = lax.psum_scatter(
        partial_sum.astype(jnp.bfloat16), "head", scatter_dimension=1, tiled=True
    )
    return summed


MESH = pl.DeviceIdType.MESH
LANES = 128
PIECE = 32


def fused_kernel(
    sides,
    q_hbm,
    k_hbm,
    v_hbm,
    do_hbm,
    lse_hbm,
    delta_hbm,
    seg_hbm,
    w_hbm,
    out_ref,
    q_ref,
    k_ref,
    v_ref,
    do_ref,
    lse_ref,
    delta_ref,
    seg_ref,
    joined,
    w_all,
    keep,
    part_out,
    part_in,
    x_out,
    x_in,
    back_out,
    bias,
    lse32,
    delta32,
    dk_acc,
    dv_acc,
    load_sem,
    own_send,
    own_recv,
    far_send,
    far_recv,
    relay_send,
    relay_recv,
    j_send,
    j_recv,
    part_send,
    part_recv,
    x_send,
    x_recv,
    back_send,
    back_recv,
):
    window, head_size = k_ref.shape
    groups = q_ref.shape[1] // head_size
    rows = w_hbm.shape[0]
    chunks, pieces = rows // LANES, rows // PIECE
    per = LANES // PIECE
    block = window // chunks
    columns = groups + 2
    tok, h = lax.axis_index("tok"), lax.axis_index("head")
    z, y = tok // sides, tok % sides
    x, c = h // sides, h % sides
    yo, xo, co = 1 - y, 1 - x, 1 - c
    odd, upper = z % sides, z // sides
    partner = z + 1 - 2 * odd
    far = z + sides - 2 * sides * upper
    outer = upper == odd
    mine = jnp.where(c == odd, 0, 1)
    final = jnp.where(x == upper, 0, 1)

    def device(dz, dy, dx, dc):
        return (dz * sides + dy, dx * sides + dc)

    y_peer = device(z, yo, x, c)
    far_peer = device(far, y, x, c)
    j_peer = device(partner, y, x, c)
    core_peer = device(z, y, x, co)
    x_peer = device(z, y, xo, c)
    back_peer = device(partner, y, x, co)

    loads = [
        pltpu.make_async_copy(src, dst, load_sem.at[i])
        for i, (src, dst) in enumerate(
            (
                (seg_hbm, seg_ref),
                (lse_hbm, lse_ref),
                (delta_hbm, delta_ref),
                (k_hbm, k_ref),
                (v_hbm, v_ref),
                (q_hbm, q_ref),
                (do_hbm, do_ref),
                (w_hbm, w_all.at[0, y]),
            )
        )
    ]
    for load in loads:
        load.start()

    barrier = pltpu.get_barrier_semaphore()
    peers = (y_peer, far_peer, j_peer, core_peer, x_peer, back_peer)
    for peer in peers:
        pl.semaphore_signal(barrier, inc=1, device_id=peer, device_id_type=MESH)
    pl.semaphore_wait(barrier, len(peers))

    def remote(src, dst, send, recv, peer):
        return pltpu.make_async_remote_copy(
            src_ref=src,
            dst_ref=dst,
            send_sem=send,
            recv_sem=recv,
            device_id=peer,
            device_id_type=MESH,
        )

    def piece_rows(p):
        return pl.ds(pl.multiple_of(p * PIECE, PIECE), PIECE)

    def chunk_rows(k):
        return pl.ds(pl.multiple_of(k * LANES, LANES), LANES)

    def block_rows(i):
        return pl.ds(pl.multiple_of(i * block, block), block)

    def own_copy(p):
        return remote(
            w_hbm.at[piece_rows(p)],
            w_all.at[0, y, piece_rows(p)],
            own_send.at[p],
            own_recv.at[p],
            y_peer,
        )

    def far_copy(p):
        return remote(
            w_hbm.at[piece_rows(p)],
            w_all.at[1, y, piece_rows(p)],
            far_send.at[p],
            far_recv.at[p],
            far_peer,
        )

    def relay_copy(p):
        ref = w_all.at[1, y, piece_rows(p)]
        return remote(ref, ref, relay_send.at[p], relay_recv.at[p], y_peer)

    def arrived_own(p):
        ref = w_all.at[0, yo, piece_rows(p)]
        remote(ref, ref, own_send.at[p], own_recv.at[p], y_peer).wait_recv()

    def arrived_far(p):
        ref = w_all.at[1, y, piece_rows(p)]
        remote(ref, ref, far_send.at[p], far_recv.at[p], far_peer).wait_recv()

    def arrived_relay(p):
        ref = w_all.at[1, yo, piece_rows(p)]
        remote(ref, ref, relay_send.at[p], relay_recv.at[p], y_peer).wait_recv()

    def j_cols(r):
        return pl.ds(pl.multiple_of(r * head_size, head_size), head_size)

    def j_copy(r):
        return remote(
            joined.at[0, :, j_cols(r)],
            joined.at[1, :, j_cols(r)],
            j_send.at[r],
            j_recv.at[r],
            j_peer,
        )

    def j_block(i):
        return remote(
            joined.at[0, block_rows(i)],
            joined.at[1, block_rows(i)],
            j_send.at[i],
            j_recv.at[i],
            j_peer,
        )

    def each(count, body):
        lax.fori_loop(0, count, lambda i, carry: (body(i), carry)[1], 0)

    first = 2

    each(pieces, lambda p: own_copy(p).start())

    @pl.when(outer)
    def _():
        each(first, lambda p: far_copy(p).start())

    @pl.when(jnp.logical_not(outer))
    def _():
        each(pieces, lambda p: far_copy(p).start())

    for load in loads[:3]:
        load.wait()
    lse32[...] = lse_ref[...].astype(jnp.float32)
    delta32[...] = delta_ref[...].astype(jnp.float32)
    seg_row = seg_ref[:, pl.ds(pl.multiple_of(tok * window, LANES), window)].astype(jnp.float32)
    seg_col = jnp.transpose(jnp.broadcast_to(seg_row, (LANES, window)))[:, :1]
    key_id = lax.broadcasted_iota(jnp.int32, (window, window), 0)
    query_id = lax.broadcasted_iota(jnp.int32, (window, window), 1)
    bias[...] = jnp.where((seg_col == seg_row) & (key_id <= query_id), 0.0, -1e30)
    dk_acc[...] = jnp.zeros_like(dk_acc)
    dv_acc[...] = jnp.zeros_like(dv_acc)
    scale = head_size ** (-0.5)
    half = window // 2

    def dot(a, b, da, db):
        return lax.dot_general(a, b, (((da,), (db,)), ((), ())), preferred_element_type=jnp.float32)

    for load in loads[3:7]:
        load.wait()

    @pl.loop(0, groups)
    def _(r):
        cols = j_cols(r)
        sums = []
        for start in (0, half):
            keys, queries = slice(start, start + half), slice(start, window)
            q, do = q_ref[queries, cols], do_ref[queries, cols]
            kk, vv = k_ref[keys, :], v_ref[keys, :]
            logits = dot(kk, q, 1, 1) * scale - lse32[pl.ds(r, 1), queries]
            probs = jnp.exp(logits + bias[keys, queries])
            dv_acc[keys, :] += dot(probs.astype(jnp.bfloat16), do, 1, 0)
            grad_prob = dot(vv, do, 1, 1)
            ds = (probs * (grad_prob - delta32[pl.ds(r, 1), queries])).astype(jnp.bfloat16)
            dk_acc[keys, :] += dot(ds, q, 1, 0)
            sums.append(dot(ds, kk, 0, 0))
        low = sums[0]
        joined[0, :half, cols] = (low[:half] * scale).astype(jnp.bfloat16)
        joined[0, half:, cols] = ((low[half:] + sums[1]) * scale).astype(jnp.bfloat16)

        @pl.when(outer)
        def _():
            j_copy(r).start()

    wide = groups * head_size
    joined[0, :, wide : wide + head_size] = (dk_acc[...] * scale).astype(jnp.bfloat16)
    joined[0, :, wide + head_size : wide + 2 * head_size] = dv_acc[...].astype(jnp.bfloat16)
    loads[7].wait()

    def tile(ref, lead, i, by_token):
        return ref.at[(*lead, slice(None), block_rows(i))] if by_token else ref.at[(*lead, i)]

    def part_copy(slot, yr, i, by_token):
        return remote(
            tile(part_out, (slot, yr), i, by_token),
            tile(part_in, (slot, yr), i, by_token),
            part_send.at[slot, yr, i],
            part_recv.at[slot, yr, i],
            core_peer,
        )

    def x_copy(yr, i, by_token):
        return remote(
            tile(x_out, (yr,), i, by_token),
            tile(x_in, (yr,), i, by_token),
            x_send.at[yr, i],
            x_recv.at[yr, i],
            x_peer,
        )

    def out_cols(yr, k):
        return pl.ds(pl.multiple_of(yr * rows + k * LANES, LANES), LANES)

    def out_tile(ref, yr, i, by_token):
        if by_token:
            return ref.at[block_rows(i), pl.ds(pl.multiple_of(yr * rows, LANES), rows)]
        return ref.at[:, out_cols(yr, i)]

    def back_copy(yr, i, by_token):
        return remote(
            out_tile(back_out, yr, i, by_token),
            out_tile(out_ref, yr, i, by_token),
            back_send.at[yr, i],
            back_recv.at[yr, i],
            back_peer,
        )

    def unit(slot, yr, k, side):
        value = dot(joined[side], w_all[slot, yr, chunk_rows(k)], 1, 1)

        @pl.when(mine == side)
        def _():
            keep[slot, yr, k] = value

        @pl.when(mine != side)
        def _():
            part_out[slot, yr, k] = value.astype(jnp.bfloat16)
            part_copy(slot, yr, k, False).start()

    def block_unit(slot, yr, i):
        value = dot(joined[1, block_rows(i)], w_all[slot, yr], 1, 1)

        @pl.when(mine == 1)
        def _():
            for k in range(chunks):
                keep[slot, yr, k, block_rows(i)] = value[:, k * LANES : (k + 1) * LANES]

        @pl.when(mine == 0)
        def _():
            low = value.astype(jnp.bfloat16)
            for k in range(chunks):
                part_out[slot, yr, k, block_rows(i)] = low[:, k * LANES : (k + 1) * LANES]
            part_copy(slot, yr, i, True).start()

    def core_sum(slot, yr, i, by_token):
        part_copy(slot, yr, i, by_token).wait_recv()
        kept = tile(keep, (slot, yr), i, by_token)
        value = kept[...] + tile(part_in, (slot, yr), i, by_token)[...].astype(jnp.float32)

        @pl.when(slot == final)
        def _():
            kept[...] = value

        @pl.when(slot != final)
        def _():
            tile(x_out, (yr,), i, by_token)[...] = value.astype(jnp.bfloat16)
            x_copy(yr, i, by_token).start()

    def x_sum(yr, i, by_token):
        x_copy(yr, i, by_token).wait_recv()
        value = tile(keep, (final, yr), i, by_token)[...]
        value += tile(x_in, (yr,), i, by_token)[...].astype(jnp.float32)
        value = value.astype(jnp.bfloat16)

        def put(ref):
            if by_token:
                for k in range(chunks):
                    ref[block_rows(i), out_cols(yr, k)] = value[k]
            else:
                ref[:, out_cols(yr, i)] = value

        if by_token:
            put(back_out)
            back_copy(yr, i, True).start()
        else:

            @pl.when(mine == 0)
            def _():
                put(out_ref)

            @pl.when(mine == 1)
            def _():
                put(back_out)
                back_copy(yr, i, False).start()

    def wait_chunk(arrived, k):
        for i in range(per):
            arrived(k * per + i)

    def which(i):
        return jnp.where(i // chunks % 2 == 0, y, yo)

    lag = 2

    @pl.when(outer)
    def _():
        j_copy(groups).start()
        j_copy(groups + 1).start()
        each(pieces - first, lambda p: far_copy(p + first).start())
        steps = 3 * chunks
        share = pieces // (2 * chunks)

        @pl.loop(0, steps + lag)
        def _(i):
            k = i % chunks

            @pl.when(i < 2 * chunks)
            def _():
                for j in range(share):
                    arrived_far(i * share + j)
                    relay_copy(i * share + j).start()

            @pl.when((i >= chunks) & (i < 2 * chunks))
            def _():
                wait_chunk(arrived_own, k)

            @pl.when(i < steps)
            def _():
                unit(i // (2 * chunks), which(i), k, 0)

            @pl.when((i >= lag) & (mine == 0))
            def _():
                core_sum((i - lag) // (2 * chunks), which(i - lag), (i - lag) % chunks, False)

        @pl.loop(0, chunks + 1)
        def _(i):
            @pl.when(i < chunks)
            def _():
                wait_chunk(arrived_relay, i)
                unit(1, yo, i, 0)
                j_block(i).wait_recv()
                block_unit(0, y, i)
                block_unit(0, yo, i)
                block_unit(1, y, i)

            @pl.when(i == chunks - 1)
            def _():
                each(chunks, lambda j: block_unit(1, yo, j))

            @pl.when(mine == 0)
            def _():
                @pl.when(i < chunks)
                def _():
                    core_sum(1, yo, i, False)
                    x_sum(y, i, False)

                @pl.when(i >= 1)
                def _():
                    x_sum(yo, i - 1, False)

            @pl.when(mine == 1)
            def _():
                @pl.when(i < chunks)
                def _():
                    for slot, yr in ((0, y), (0, yo), (1, y)):
                        core_sum(slot, yr, i, True)

                @pl.when(i == chunks - 1)
                def _():
                    each(chunks, lambda j: core_sum(1, yo, j, True))

                @pl.when(i >= 1)
                def _():
                    x_sum(y, i - 1, True)

                @pl.when((i >= 1) & (final == 0))
                def _():
                    x_sum(yo, i - 1, True)

        @pl.when((mine == 1) & (final == 1))
        def _():
            each(chunks, lambda j: x_sum(yo, j, True))

    @pl.when(jnp.logical_not(outer))
    def _():
        @pl.loop(0, 2 * chunks + lag)
        def _(i):
            k = i % chunks

            @pl.when(i == 2 * chunks - 1)
            def _():
                each(chunks, lambda j: j_block(j).start())

            @pl.when((i >= chunks) & (i < 2 * chunks))
            def _():
                wait_chunk(arrived_own, k)

            @pl.when(i < 2 * chunks)
            def _():
                unit(0, which(i), k, 0)

            @pl.when((i >= lag) & (mine == 0))
            def _():
                core_sum(0, which(i - lag), (i - lag) % chunks, False)

        each(columns, lambda r: j_copy(r).wait_recv())

        @pl.loop(0, chunks + 2)
        def _(k):
            for i in range(per):

                @pl.when(k < chunks)
                def _():
                    arrived_far(k * per + i)
                    relay_copy(k * per + i).start()

                @pl.when(k == 0)
                def _():
                    for j in range(i * 2 * chunks // per, (i + 1) * 2 * chunks // per):
                        unit(0, which(j), j % chunks, 1)

                @pl.when((k == 1) & (mine == 1))
                def _():
                    for j in range(i * 2 * chunks // per, (i + 1) * 2 * chunks // per):
                        core_sum(0, which(j), j % chunks, False)

                @pl.when((k >= 1) & (k <= chunks))
                def _():
                    if i == 0:
                        unit(1, y, k - 1, 0)
                    if i == 1:
                        unit(1, y, k - 1, 1)
                    if i == 2:
                        wait_chunk(arrived_relay, k - 1)
                        unit(1, yo, k - 1, 0)
                        core_sum(1, y, k - 1, False)
                    if i == 3:
                        unit(1, yo, k - 1, 1)

                @pl.when(k >= 2)
                def _():
                    if i == 0:
                        core_sum(1, yo, k - 2, False)

                    @pl.when(final == 1)
                    def _():
                        if i == 1:
                            x_sum(y, k - 2, False)
                        if i == 3:
                            x_sum(yo, k - 2, False)

                    @pl.when((final == 0) & (k < 4))
                    def _():
                        j = 2 * k - 4 + i // 2
                        x_sum(y if i % 2 == 0 else yo, j, False)

    @pl.when(mine == 1)
    def _():
        @pl.loop(0, 2 * chunks)
        def _(i):
            back_copy(i // chunks, i % chunks, False).wait_recv()
            back_copy(i // chunks, i % chunks, False).wait_send()

    @pl.loop(0, pieces)
    def _(p):
        own_copy(p).wait_send()
        far_copy(p).wait_send()
        relay_copy(p).wait_send()

    @pl.when(outer)
    def _():
        each(columns, lambda r: j_copy(r).wait_send())

    @pl.when(jnp.logical_not(outer))
    def _():
        each(chunks, lambda i: j_block(i).wait_send())

    @pl.loop(0, 2 * chunks)
    def _(i):
        yr, k = i // chunks, i % chunks
        part_copy(0, yr, k, False).wait_send()
        part_copy(1, yr, k, False).wait_send()
        x_copy(yr, k, False).wait_send()


def fused(sides, q, k, v, do, lse, delta, segments, weight):
    window, _, query_width = q.shape
    head_size = k.shape[2]
    rows, _, width = weight.shape
    chunks, pieces = rows // LANES, rows // PIECE
    columns = width // head_size
    bf16, f32 = jnp.bfloat16, jnp.float32
    dma = pltpu.SemaphoreType.DMA
    vmem = pl.BlockSpec(memory_space=pltpu.VMEM)
    hbm = pl.BlockSpec(memory_space=pl.ANY)
    tile = (window, LANES)
    return pl.pallas_call(
        functools.partial(fused_kernel, sides),
        out_shape=jax.ShapeDtypeStruct((window, 2 * rows), bf16),
        in_specs=[hbm] * 8,
        out_specs=vmem,
        scratch_shapes=[
            pltpu.VMEM((window, query_width), bf16),
            pltpu.VMEM((window, head_size), bf16),
            pltpu.VMEM((window, head_size), bf16),
            pltpu.VMEM((window, query_width), bf16),
            pltpu.VMEM(lse.shape[1:], bf16),
            pltpu.VMEM(lse.shape[1:], bf16),
            pltpu.VMEM((1,) + segments.shape, segments.dtype),
            pltpu.VMEM((2, window, width), bf16),
            pltpu.VMEM((2, 2, rows, width), bf16),
            pltpu.VMEM((2, 2, chunks) + tile, f32),
            pltpu.VMEM((2, 2, chunks) + tile, bf16),
            pltpu.VMEM((2, 2, chunks) + tile, bf16),
            pltpu.VMEM((2, chunks) + tile, bf16),
            pltpu.VMEM((2, chunks) + tile, bf16),
            pltpu.VMEM((window, 2 * rows), bf16),
            pltpu.VMEM((window, window), f32),
            pltpu.VMEM(lse.shape[1:], f32),
            pltpu.VMEM(lse.shape[1:], f32),
            pltpu.VMEM((window, head_size), f32),
            pltpu.VMEM((window, head_size), f32),
            dma((8,)),
            dma((pieces,)),
            dma((pieces,)),
            dma((pieces,)),
            dma((pieces,)),
            dma((pieces,)),
            dma((pieces,)),
            dma((columns,)),
            dma((columns,)),
            dma((2, 2, chunks)),
            dma((2, 2, chunks)),
            dma((2, chunks)),
            dma((2, chunks)),
            dma((2, chunks)),
            dma((2, chunks)),
        ],
        compiler_params=pltpu.CompilerParams(
            collective_id=0, has_side_effects=True, vmem_limit_bytes=40 * 1024 * 1024
        ),
    )(
        *(
            pltpu.with_memory_space_constraint(array, pltpu.HBM)
            for array in (
                q.reshape(window, query_width),
                k.reshape(window, head_size),
                v.reshape(window, head_size),
                do.reshape(window, query_width),
                lse.reshape(lse.shape[1:]),
                delta.reshape(delta.shape[1:]),
                segments.reshape(1, -1),
                weight.reshape(rows, width),
            )
        )
    )


def solution(mesh):
    placed = (
        P("tok", "head", None),
        P("tok", "head", None),
        P("tok", "head", None),
        P("tok", "head", None),
        P("head", None, "tok"),
        P("head", None, "tok"),
        P(),
        P("tok", "head", None),
    )
    tok, heads = mesh.shape["tok"], mesh.shape["head"]
    sides = tok // heads

    def step(*args):
        window, kv_dev, _ = args[0].shape
        rows = args[7].shape[0]
        paired = sides == 2 and heads == sides * sides and tok == heads * sides and kv_dev == 1
        if paired and rows % LANES == 0 and window % (2 * LANES) == 0 and args[1].shape[2] == LANES:
            return fused(sides, *args)
        return on_device(*args)

    return jax.shard_map(
        step, mesh=mesh, in_specs=placed, out_specs=P("tok", "head"), check_vma=False
    )
```

```python
import functools

import jax
import jax.numpy as jnp
import numpy as np
from jax import lax
from jax.experimental import pallas as pl
from jax.experimental.pallas import tpu as pltpu
from jax.sharding import PartitionSpec as P

BLOCK = 128


def pair_lists(block_count):
    query_list = []
    key_list = []
    for query_block in range(block_count):
        for key_block in range(query_block + 1):
            query_list.append(query_block)
            key_list.append(key_block)
    return (np.array(query_list, np.int32), np.array(key_list, np.int32))


def live_pairs(seg_window, query_list, key_list, tile_rows):
    first_seg = jnp.take(seg_window, query_list * tile_rows)
    last_seg = jnp.take(seg_window, key_list * tile_rows + tile_rows - 1)
    return (first_seg == last_seg) | jnp.asarray(query_list == key_list)


def pair_grads(query_tile, dout_tile, key_tile, value_tile, lse_tile, delta_tile, allowed):
    tile_rows, groups, query_width = query_tile.shape
    head_size = key_tile.shape[2]
    heads_per_group = query_width // head_size
    query_heads = query_tile.reshape(tile_rows, groups, heads_per_group, head_size)
    dout_heads = dout_tile.reshape(tile_rows, groups, heads_per_group, head_size)
    scores = jnp.einsum(
        "agrd,bgd->grab", query_heads, key_tile, preferred_element_type=jnp.float32
    ) * head_size ** (-0.5)
    logits = scores - lse_tile.astype(jnp.float32)[:, :, :, None]
    soft_probs = jnp.where(allowed[None, None], jnp.exp(logits), 0.0)
    probs_low = soft_probs.astype(jnp.bfloat16)
    value_gradient = jnp.einsum(
        "grab,agrd->bgd", probs_low, dout_heads, preferred_element_type=jnp.float32
    )
    grad_prob = jnp.einsum(
        "agrd,bgd->grab", dout_heads, value_tile, preferred_element_type=jnp.float32
    )
    grad_score = (soft_probs * (grad_prob - delta_tile.astype(jnp.float32)[:, :, :, None])).astype(
        jnp.bfloat16
    )
    query_gradient = jnp.einsum(
        "grab,bgd->agrd", grad_score, key_tile, preferred_element_type=jnp.float32
    )
    key_gradient = jnp.einsum(
        "grab,agrd->bgd", grad_score, query_heads, preferred_element_type=jnp.float32
    )
    return (query_gradient.reshape(tile_rows, groups, query_width), key_gradient, value_gradient)


def on_device(
    query_rows,
    key_rows,
    value_rows,
    output_gradient,
    row_logsumexp,
    row_delta_sums,
    segments,
    query_key_value_weight,
):
    window, kv_dev, query_width = query_rows.shape
    head_size = key_rows.shape[2]
    tile_rows = BLOCK
    block_count = window // tile_rows
    query_list, key_list = pair_lists(block_count)
    query_table = jnp.asarray(query_list)
    key_table = jnp.asarray(key_list)
    myself = lax.axis_index("tok")
    own_seg = lax.dynamic_slice_in_dim(segments, myself * window, window)
    own_live = live_pairs(own_seg, query_list, key_list, tile_rows)
    block_ids = jnp.arange(block_count, dtype=jnp.int32)
    query_match = (query_table[:, None] == block_ids[None, :]) & own_live[:, None]
    key_match = key_table[:, None] == block_ids[None, :]
    block_local = jnp.any(query_match[:, :, None] & key_match[:, None, :], axis=0)
    token_local = jnp.repeat(jnp.repeat(block_local, tile_rows, axis=0), tile_rows, axis=1)
    offsets = jnp.arange(window, dtype=jnp.int32)
    allowed_all = (
        (own_seg[:, None] == own_seg[None, :])
        & (offsets[None, :] <= offsets[:, None])
        & token_local
    )
    local_out = pair_grads(
        query_rows,
        output_gradient,
        key_rows,
        value_rows,
        row_logsumexp,
        row_delta_sums,
        allowed_all,
    )
    acc_query = local_out[0].reshape(block_count, tile_rows, kv_dev, query_width)
    acc_key = local_out[1].reshape(block_count, tile_rows, kv_dev, head_size)
    acc_value = local_out[2].reshape(block_count, tile_rows, kv_dev, head_size)
    score_scale = head_size ** (-0.5)
    query_gradient = (acc_query * score_scale).reshape(window, kv_dev, query_width)
    key_gradient = (acc_key * score_scale).reshape(window, kv_dev, head_size)
    value_gradient = acc_value.reshape(window, kv_dev, head_size)
    stacked_gradients = (
        jnp.concatenate([query_gradient, key_gradient, value_gradient], axis=2)
        .astype(jnp.bfloat16)
        .reshape(window, -1)
    )
    weight_piece = lax.all_gather(query_key_value_weight, "tok", axis=0, tiled=True)
    flat_piece = weight_piece.reshape(weight_piece.shape[0], -1)
    partial_sum = lax.dot_general(
        stacked_gradients, flat_piece, (((1,), (1,)), ((), ())), preferred_element_type=jnp.float32
    )
    summed = lax.psum_scatter(
        partial_sum.astype(jnp.bfloat16), "head", scatter_dimension=1, tiled=True
    )
    return summed


MESH = pl.DeviceIdType.MESH
LANES = 128
PIECE = 32


def fused_kernel(
    sides,
    q_hbm,
    k_hbm,
    v_hbm,
    do_hbm,
    lse_hbm,
    delta_hbm,
    seg_hbm,
    w_hbm,
    out_ref,
    q_ref,
    k_ref,
    v_ref,
    do_ref,
    lse_ref,
    delta_ref,
    seg_ref,
    joined,
    w_all,
    keep,
    part_out,
    part_in,
    x_out,
    x_in,
    back_out,
    bias,
    lse32,
    delta32,
    dk_acc,
    dv_acc,
    load_sem,
    own_send,
    own_recv,
    far_send,
    far_recv,
    relay_send,
    relay_recv,
    j_send,
    j_recv,
    part_send,
    part_recv,
    x_send,
    x_recv,
    back_send,
    back_recv,
    small_part_send,
    small_part_recv,
    small_x_send,
    small_x_recv,
    small_back_send,
    small_back_recv,
):
    window, head_size = k_ref.shape
    groups = q_ref.shape[1] // head_size
    rows = w_hbm.shape[0]
    chunks, pieces = rows // LANES, rows // PIECE
    per = LANES // PIECE
    block = window // chunks
    columns = groups + 2
    tok, h = lax.axis_index("tok"), lax.axis_index("head")
    z, y = tok // sides, tok % sides
    x, c = h // sides, h % sides
    yo, xo, co = 1 - y, 1 - x, 1 - c
    odd, upper = z % sides, z // sides
    partner = z + 1 - 2 * odd
    far = z + sides - 2 * sides * upper
    outer = upper == odd
    mine = jnp.where(c == odd, 0, 1)
    final = jnp.where(x == upper, 0, 1)

    def device(dz, dy, dx, dc):
        return (dz * sides + dy, dx * sides + dc)

    y_peer = device(z, yo, x, c)
    far_peer = device(far, y, x, c)
    j_peer = device(partner, y, x, c)
    core_peer = device(z, y, x, co)
    x_peer = device(z, y, xo, c)
    back_peer = device(partner, y, x, co)

    loads = [
        pltpu.make_async_copy(src, dst, load_sem.at[i])
        for i, (src, dst) in enumerate(
            (
                (seg_hbm, seg_ref),
                (lse_hbm, lse_ref),
                (delta_hbm, delta_ref),
                (k_hbm, k_ref),
                (v_hbm, v_ref),
                (q_hbm, q_ref),
                (do_hbm, do_ref),
                (w_hbm, w_all.at[0, y]),
            )
        )
    ]
    for load in loads:
        load.start()

    barrier = pltpu.get_barrier_semaphore()
    peers = (y_peer, far_peer, j_peer, core_peer, x_peer, back_peer)
    for peer in peers:
        pl.semaphore_signal(barrier, inc=1, device_id=peer, device_id_type=MESH)
    pl.semaphore_wait(barrier, len(peers))

    def remote(src, dst, send, recv, peer):
        return pltpu.make_async_remote_copy(
            src_ref=src,
            dst_ref=dst,
            send_sem=send,
            recv_sem=recv,
            device_id=peer,
            device_id_type=MESH,
        )

    def piece_rows(p):
        return pl.ds(pl.multiple_of(p * PIECE, PIECE), PIECE)

    def chunk_rows(k):
        return pl.ds(pl.multiple_of(k * LANES, LANES), LANES)

    def block_rows(i):
        return pl.ds(pl.multiple_of(i * block, block), block)

    def own_copy(p):
        return remote(
            w_hbm.at[piece_rows(p)],
            w_all.at[0, y, piece_rows(p)],
            own_send.at[p],
            own_recv.at[p],
            y_peer,
        )

    def far_copy(p):
        return remote(
            w_hbm.at[piece_rows(p)],
            w_all.at[1, y, piece_rows(p)],
            far_send.at[p],
            far_recv.at[p],
            far_peer,
        )

    def relay_copy(p):
        ref = w_all.at[1, y, piece_rows(p)]
        return remote(ref, ref, relay_send.at[p], relay_recv.at[p], y_peer)

    def arrived_own(p):
        ref = w_all.at[0, yo, piece_rows(p)]
        remote(ref, ref, own_send.at[p], own_recv.at[p], y_peer).wait_recv()

    def arrived_far(p):
        ref = w_all.at[1, y, piece_rows(p)]
        remote(ref, ref, far_send.at[p], far_recv.at[p], far_peer).wait_recv()

    def arrived_relay(p):
        ref = w_all.at[1, yo, piece_rows(p)]
        remote(ref, ref, relay_send.at[p], relay_recv.at[p], y_peer).wait_recv()

    def j_cols(r):
        return pl.ds(pl.multiple_of(r * head_size, head_size), head_size)

    def j_copy(r):
        return remote(
            joined.at[0, :, j_cols(r)],
            joined.at[1, :, j_cols(r)],
            j_send.at[r],
            j_recv.at[r],
            j_peer,
        )

    def j_block(i):
        return remote(
            joined.at[0, block_rows(i)],
            joined.at[1, block_rows(i)],
            j_send.at[i],
            j_recv.at[i],
            j_peer,
        )

    def each(count, body):
        lax.fori_loop(0, count, lambda i, carry: (body(i), carry)[1], 0)

    first = LANES // PIECE // 4

    each(pieces, lambda p: own_copy(p).start())

    @pl.when(outer)
    def _():
        each(first, lambda p: far_copy(p).start())

    @pl.when(jnp.logical_not(outer))
    def _():
        each(pieces, lambda p: far_copy(p).start())

    for load in loads[:3]:
        load.wait()
    lse32[...] = lse_ref[...].astype(jnp.float32)
    delta32[...] = delta_ref[...].astype(jnp.float32)
    seg_row = seg_ref[:, pl.ds(pl.multiple_of(tok * window, LANES), window)].astype(jnp.float32)
    seg_col = jnp.transpose(jnp.broadcast_to(seg_row, (LANES, window)))[:, :1]
    key_id = lax.broadcasted_iota(jnp.int32, (window, window), 0)
    query_id = lax.broadcasted_iota(jnp.int32, (window, window), 1)
    bias[...] = jnp.where((seg_col == seg_row) & (key_id <= query_id), 0.0, -1e30)
    dk_acc[...] = jnp.zeros_like(dk_acc)
    dv_acc[...] = jnp.zeros_like(dv_acc)
    scale = head_size ** (-0.5)
    half = window // 2

    def dot(a, b, da, db):
        return lax.dot_general(a, b, (((da,), (db,)), ((), ())), preferred_element_type=jnp.float32)

    for load in loads[3:7]:
        load.wait()

    @pl.loop(0, groups)
    def _(r):
        cols = j_cols(r)
        sums = []
        for start in (0, half):
            keys, queries = slice(start, start + half), slice(start, window)
            q, do = q_ref[queries, cols], do_ref[queries, cols]
            kk, vv = k_ref[keys, :], v_ref[keys, :]
            logits = dot(kk, q, 1, 1) * scale - lse32[pl.ds(r, 1), queries]
            probs = jnp.exp(logits + bias[keys, queries])
            dv_acc[keys, :] += dot(probs.astype(jnp.bfloat16), do, 1, 0)
            grad_prob = dot(vv, do, 1, 1)
            ds = (probs * (grad_prob - delta32[pl.ds(r, 1), queries])).astype(jnp.bfloat16)
            dk_acc[keys, :] += dot(ds, q, 1, 0)
            sums.append(dot(ds, kk, 0, 0))
        low = sums[0]
        joined[0, :half, cols] = (low[:half] * scale).astype(jnp.bfloat16)
        joined[0, half:, cols] = ((low[half:] + sums[1]) * scale).astype(jnp.bfloat16)

        @pl.when(outer)
        def _():
            j_copy(r).start()

    wide = groups * head_size
    joined[0, :, wide : wide + head_size] = (dk_acc[...] * scale).astype(jnp.bfloat16)
    joined[0, :, wide + head_size : wide + 2 * head_size] = dv_acc[...].astype(jnp.bfloat16)
    loads[7].wait()

    def tile(ref, lead, i, by_token):
        return ref.at[(*lead, slice(None), block_rows(i))] if by_token else ref.at[(*lead, i)]

    def part_copy(slot, yr, i, by_token):
        return remote(
            tile(part_out, (slot, yr), i, by_token),
            tile(part_in, (slot, yr), i, by_token),
            part_send.at[slot, yr, i],
            part_recv.at[slot, yr, i],
            core_peer,
        )

    def x_copy(yr, i, by_token):
        return remote(
            tile(x_out, (yr,), i, by_token),
            tile(x_in, (yr,), i, by_token),
            x_send.at[yr, i],
            x_recv.at[yr, i],
            x_peer,
        )

    def out_cols(yr, k):
        return pl.ds(pl.multiple_of(yr * rows + k * LANES, LANES), LANES)

    def out_tile(ref, yr, i, by_token):
        if by_token:
            return ref.at[block_rows(i), pl.ds(pl.multiple_of(yr * rows, LANES), rows)]
        return ref.at[:, out_cols(yr, i)]

    def back_copy(yr, i, by_token):
        return remote(
            out_tile(back_out, yr, i, by_token),
            out_tile(out_ref, yr, i, by_token),
            back_send.at[yr, i],
            back_recv.at[yr, i],
            back_peer,
        )

    def unit(slot, yr, k, side):
        value = dot(joined[side], w_all[slot, yr, chunk_rows(k)], 1, 1)

        @pl.when(mine == side)
        def _():
            keep[slot, yr, k] = value

        @pl.when(mine != side)
        def _():
            part_out[slot, yr, k] = value.astype(jnp.bfloat16)
            part_copy(slot, yr, k, False).start()

    def block_unit(slot, yr, i):
        value = dot(joined[1, block_rows(i)], w_all[slot, yr], 1, 1)

        @pl.when(mine == 1)
        def _():
            for k in range(chunks):
                keep[slot, yr, k, block_rows(i)] = value[:, k * LANES : (k + 1) * LANES]

        @pl.when(mine == 0)
        def _():
            low = value.astype(jnp.bfloat16)
            for k in range(chunks):
                part_out[slot, yr, k, block_rows(i)] = low[:, k * LANES : (k + 1) * LANES]
            part_copy(slot, yr, i, True).start()

    def small(ref, lead, a, b):
        return ref.at[(*lead, b, block_rows(a))]

    def small_part(a, b):
        return remote(
            small(part_out, (1, yo), a, b),
            small(part_in, (1, yo), a, b),
            small_part_send.at[a, b],
            small_part_recv.at[a, b],
            core_peer,
        )

    def small_x(a, b):
        return remote(
            small(x_out, (yo,), a, b),
            small(x_in, (yo,), a, b),
            small_x_send.at[a, b],
            small_x_recv.at[a, b],
            x_peer,
        )

    def small_back(a, b):
        return remote(
            back_out.at[block_rows(a), out_cols(yo, b)],
            out_ref.at[block_rows(a), out_cols(yo, b)],
            small_back_send.at[a, b],
            small_back_recv.at[a, b],
            back_peer,
        )

    def small_unit(a, b):
        value = dot(joined[1, block_rows(a)], w_all[1, yo, chunk_rows(b)], 1, 1)

        @pl.when(mine == 1)
        def _():
            keep[1, yo, b, block_rows(a)] = value

        @pl.when(mine == 0)
        def _():
            part_out[1, yo, b, block_rows(a)] = value.astype(jnp.bfloat16)
            small_part(a, b).start()

    def small_core_sum(a, b):
        small_part(a, b).wait_recv()
        kept = small(keep, (1, yo), a, b)
        value = kept[...] + small(part_in, (1, yo), a, b)[...].astype(jnp.float32)

        @pl.when(final == 1)
        def _():
            kept[...] = value

        @pl.when(final == 0)
        def _():
            small(x_out, (yo,), a, b)[...] = value.astype(jnp.bfloat16)
            small_x(a, b).start()

    def small_x_sum(a, b):
        small_x(a, b).wait_recv()
        value = small(keep, (1, yo), a, b)[...] + small(x_in, (yo,), a, b)[...].astype(jnp.float32)
        back_out[block_rows(a), out_cols(yo, b)] = value.astype(jnp.bfloat16)
        small_back(a, b).start()

    def added(step, body):
        def one(j):
            body(jnp.minimum(j, step), jnp.where(j <= step, step, j - step - 1))

        each(2 * step + 1, one)

    def all_small(body):
        each(chunks * chunks, lambda j: body(j // chunks, j % chunks))

    def core_sum(slot, yr, i, by_token):
        part_copy(slot, yr, i, by_token).wait_recv()
        kept = tile(keep, (slot, yr), i, by_token)
        value = kept[...] + tile(part_in, (slot, yr), i, by_token)[...].astype(jnp.float32)

        @pl.when(slot == final)
        def _():
            kept[...] = value

        @pl.when(slot != final)
        def _():
            tile(x_out, (yr,), i, by_token)[...] = value.astype(jnp.bfloat16)
            x_copy(yr, i, by_token).start()

    def x_sum(yr, i, by_token):
        x_copy(yr, i, by_token).wait_recv()
        value = tile(keep, (final, yr), i, by_token)[...]
        value += tile(x_in, (yr,), i, by_token)[...].astype(jnp.float32)
        value = value.astype(jnp.bfloat16)

        def put(ref):
            if by_token:
                for k in range(chunks):
                    ref[block_rows(i), out_cols(yr, k)] = value[k]
            else:
                ref[:, out_cols(yr, i)] = value

        if by_token:
            put(back_out)
            back_copy(yr, i, True).start()
        else:

            @pl.when(mine == 0)
            def _():
                put(out_ref)

            @pl.when(mine == 1)
            def _():
                put(back_out)
                back_copy(yr, i, False).start()

    def wait_chunk(arrived, k):
        for i in range(per):
            arrived(k * per + i)

    def which(i):
        return jnp.where(i // chunks % 2 == 0, y, yo)

    lag, turns = 2, 4

    @pl.when(outer)
    def _():
        j_copy(groups).start()
        j_copy(groups + 1).start()
        each(pieces - first, lambda p: far_copy(p + first).start())
        steps = 3 * chunks
        share = pieces // (2 * chunks)

        @pl.loop(0, steps + lag)
        def _(i):
            k = i % chunks

            @pl.when(i < 2 * chunks)
            def _():
                for j in range(share):
                    arrived_far(i * share + j)
                    relay_copy(i * share + j).start()

            @pl.when((i >= chunks) & (i < 2 * chunks))
            def _():
                wait_chunk(arrived_own, k)

            @pl.when(i < steps)
            def _():
                unit(i // (2 * chunks), which(i), k, 0)

            @pl.when((i >= lag) & (mine == 0))
            def _():
                core_sum((i - lag) // (2 * chunks), which(i - lag), (i - lag) % chunks, False)

        @pl.loop(0, chunks + 1)
        def _(i):
            @pl.when(i < chunks)
            def _():
                wait_chunk(arrived_relay, i)
                unit(1, yo, i, 0)
                j_block(i).wait_recv()
                block_unit(0, y, i)
                block_unit(0, yo, i)
                block_unit(1, y, i)
                added(i, small_unit)

            @pl.when(mine == 0)
            def _():
                @pl.when(i < chunks)
                def _():
                    core_sum(1, yo, i, False)
                    x_sum(y, i, False)

                @pl.when(i >= 1)
                def _():
                    x_sum(yo, i - 1, False)

            @pl.when(mine == 1)
            def _():
                @pl.when(i < chunks)
                def _():
                    for slot, yr in ((0, y), (0, yo), (1, y)):
                        core_sum(slot, yr, i, True)
                    added(i, small_core_sum)

                @pl.when(i >= 1)
                def _():
                    x_sum(y, i - 1, True)

                @pl.when((i >= 1) & (final == 0))
                def _():
                    x_sum(yo, i - 1, True)

                @pl.when((i >= 1) & (final == 1))
                def _():
                    added(i - 1, small_x_sum)

    @pl.when(jnp.logical_not(outer))
    def _():
        @pl.loop(0, 2 * chunks + lag)
        def _(i):
            k = i % chunks

            @pl.when((i >= chunks) & (i < 2 * chunks))
            def _():
                for j in range(per):
                    if j == per * 3 // 4:

                        @pl.when(i == 2 * chunks - 1)
                        def _():
                            each(chunks, lambda b: j_block(b).start())

                    arrived_own(k * per + j)

            @pl.when(i < 2 * chunks)
            def _():
                unit(0, which(i), k, 0)

            @pl.when((i >= lag) & (mine == 0))
            def _():
                core_sum(0, which(i - lag), (i - lag) % chunks, False)

        each(columns, lambda r: j_copy(r).wait_recv())

        @pl.loop(0, chunks + 2)
        def _(k):
            for i in range(turns):

                @pl.when(k < chunks)
                def _():
                    for j in range(per // turns):
                        p = k * per + i * (per // turns) + j
                        arrived_far(p)
                        relay_copy(p).start()

                @pl.when(k == 0)
                def _():
                    for j in range(i * 2 * chunks // turns, (i + 1) * 2 * chunks // turns):
                        unit(0, which(j), j % chunks, 1)

                @pl.when((k == 1) & (mine == 1))
                def _():
                    for j in range(i * 2 * chunks // turns, (i + 1) * 2 * chunks // turns):
                        core_sum(0, which(j), j % chunks, False)

                @pl.when((k >= 1) & (k <= chunks))
                def _():
                    if i == 0:
                        unit(1, y, k - 1, 0)
                    if i == 1:
                        unit(1, y, k - 1, 1)
                    if i == 2:
                        wait_chunk(arrived_relay, k - 1)
                        unit(1, yo, k - 1, 0)
                        core_sum(1, y, k - 1, False)
                    if i == 3:
                        unit(1, yo, k - 1, 1)

                @pl.when(k >= 2)
                def _():
                    if i == 0:
                        core_sum(1, yo, k - 2, False)

                    @pl.when(final == 1)
                    def _():
                        if i == 1:
                            x_sum(y, k - 2, False)
                        if i == 3:
                            x_sum(yo, k - 2, False)

                    @pl.when((final == 0) & (k < chunks))
                    def _():
                        if i < 2:
                            x_sum((y, yo)[i], 2 * k - 4, False)
                            x_sum((y, yo)[i], 2 * k - 3, False)

    inner = jnp.logical_not(outer)

    def tiles(condition, copies, wait):
        @pl.when(condition)
        def _():
            each(chunks, lambda i: wait(copies(i)))

    def smalls(condition, copies, wait):
        @pl.when(condition)
        def _():
            all_small(lambda a, b: wait(copies(a, b)))

    def received(copy):
        copy.wait_recv()

    def sent(copy):
        copy.wait_send()

    back = mine == 1
    tiles(back, lambda i: back_copy(y, i, False), received)
    tiles(back & (outer | (final == 0)), lambda i: back_copy(yo, i, False), received)
    smalls(back & inner & (final == 1), small_back, received)
    tiles(back, lambda i: back_copy(y, i, False), sent)
    tiles(back & (inner | (final == 0)), lambda i: back_copy(yo, i, False), sent)
    smalls(back & outer & (final == 1), small_back, sent)
    by_small = outer & (final == 0) & (mine == 1)
    tiles(jnp.logical_not(by_small), lambda i: x_copy(yo, i, False), sent)
    smalls(by_small, small_x, sent)
    by_small = outer & (mine == 0)
    tiles(jnp.logical_not(by_small), lambda i: part_copy(1, yo, i, False), sent)
    smalls(by_small, small_part, sent)

    @pl.loop(0, chunks)
    def _(i):
        x_copy(y, i, False).wait_send()
        part_copy(0, y, i, False).wait_send()
        part_copy(0, yo, i, False).wait_send()
        part_copy(1, y, i, False).wait_send()

    @pl.loop(0, pieces)
    def _(p):
        own_copy(p).wait_send()
        far_copy(p).wait_send()
        relay_copy(p).wait_send()

    @pl.when(outer)
    def _():
        each(columns, lambda r: j_copy(r).wait_send())

    @pl.when(jnp.logical_not(outer))
    def _():
        each(chunks, lambda i: j_block(i).wait_send())


def fused(sides, q, k, v, do, lse, delta, segments, weight):
    window, _, query_width = q.shape
    head_size = k.shape[2]
    rows, _, width = weight.shape
    chunks, pieces = rows // LANES, rows // PIECE
    columns = width // head_size
    bf16, f32 = jnp.bfloat16, jnp.float32
    dma = pltpu.SemaphoreType.DMA
    vmem = pl.BlockSpec(memory_space=pltpu.VMEM)
    hbm = pl.BlockSpec(memory_space=pl.ANY)
    tile = (window, LANES)
    return pl.pallas_call(
        functools.partial(fused_kernel, sides),
        out_shape=jax.ShapeDtypeStruct((window, 2 * rows), bf16),
        in_specs=[hbm] * 8,
        out_specs=vmem,
        scratch_shapes=[
            pltpu.VMEM((window, query_width), bf16),
            pltpu.VMEM((window, head_size), bf16),
            pltpu.VMEM((window, head_size), bf16),
            pltpu.VMEM((window, query_width), bf16),
            pltpu.VMEM(lse.shape[1:], bf16),
            pltpu.VMEM(lse.shape[1:], bf16),
            pltpu.VMEM((1,) + segments.shape, segments.dtype),
            pltpu.VMEM((2, window, width), bf16),
            pltpu.VMEM((2, 2, rows, width), bf16),
            pltpu.VMEM((2, 2, chunks) + tile, f32),
            pltpu.VMEM((2, 2, chunks) + tile, bf16),
            pltpu.VMEM((2, 2, chunks) + tile, bf16),
            pltpu.VMEM((2, chunks) + tile, bf16),
            pltpu.VMEM((2, chunks) + tile, bf16),
            pltpu.VMEM((window, 2 * rows), bf16),
            pltpu.VMEM((window, window), f32),
            pltpu.VMEM(lse.shape[1:], f32),
            pltpu.VMEM(lse.shape[1:], f32),
            pltpu.VMEM((window, head_size), f32),
            pltpu.VMEM((window, head_size), f32),
            dma((8,)),
            dma((pieces,)),
            dma((pieces,)),
            dma((pieces,)),
            dma((pieces,)),
            dma((pieces,)),
            dma((pieces,)),
            dma((columns,)),
            dma((columns,)),
            dma((2, 2, chunks)),
            dma((2, 2, chunks)),
            dma((2, chunks)),
            dma((2, chunks)),
            dma((2, chunks)),
            dma((2, chunks)),
            *[dma((chunks, chunks))] * 6,
        ],
        compiler_params=pltpu.CompilerParams(
            collective_id=0, has_side_effects=True, vmem_limit_bytes=40 * 1024 * 1024
        ),
    )(
        *(
            pltpu.with_memory_space_constraint(array, pltpu.HBM)
            for array in (
                q.reshape(window, query_width),
                k.reshape(window, head_size),
                v.reshape(window, head_size),
                do.reshape(window, query_width),
                lse.reshape(lse.shape[1:]),
                delta.reshape(delta.shape[1:]),
                segments.reshape(1, -1),
                weight.reshape(rows, width),
            )
        )
    )


def solution(mesh):
    placed = (
        P("tok", "head", None),
        P("tok", "head", None),
        P("tok", "head", None),
        P("tok", "head", None),
        P("head", None, "tok"),
        P("head", None, "tok"),
        P(),
        P("tok", "head", None),
    )
    tok, heads = mesh.shape["tok"], mesh.shape["head"]
    sides = tok // heads

    def step(*args):
        window, kv_dev, _ = args[0].shape
        rows = args[7].shape[0]
        paired = sides == 2 and heads == sides * sides and tok == heads * sides and kv_dev == 1
        if paired and rows % LANES == 0 and window % (2 * LANES) == 0 and args[1].shape[2] == LANES:
            return fused(sides, *args)
        return on_device(*args)

    return jax.shard_map(
        step, mesh=mesh, in_specs=placed, out_specs=P("tok", "head"), check_vma=False
    )
```

```python
import functools

import jax
import jax.numpy as jnp
import numpy as np
from jax import lax
from jax.experimental import pallas as pl
from jax.experimental.pallas import tpu as pltpu
from jax.sharding import PartitionSpec as P

BLOCK = 128


def pair_lists(block_count):
    query_list = []
    key_list = []
    for query_block in range(block_count):
        for key_block in range(query_block + 1):
            query_list.append(query_block)
            key_list.append(key_block)
    return (np.array(query_list, np.int32), np.array(key_list, np.int32))


def live_pairs(seg_window, query_list, key_list, tile_rows):
    first_seg = jnp.take(seg_window, query_list * tile_rows)
    last_seg = jnp.take(seg_window, key_list * tile_rows + tile_rows - 1)
    return (first_seg == last_seg) | jnp.asarray(query_list == key_list)


def pair_grads(query_tile, dout_tile, key_tile, value_tile, lse_tile, delta_tile, allowed):
    tile_rows, groups, query_width = query_tile.shape
    head_size = key_tile.shape[2]
    heads_per_group = query_width // head_size
    query_heads = query_tile.reshape(tile_rows, groups, heads_per_group, head_size)
    dout_heads = dout_tile.reshape(tile_rows, groups, heads_per_group, head_size)
    scores = jnp.einsum(
        "agrd,bgd->grab", query_heads, key_tile, preferred_element_type=jnp.float32
    ) * head_size ** (-0.5)
    logits = scores - lse_tile.astype(jnp.float32)[:, :, :, None]
    soft_probs = jnp.where(allowed[None, None], jnp.exp(logits), 0.0)
    probs_low = soft_probs.astype(jnp.bfloat16)
    value_gradient = jnp.einsum(
        "grab,agrd->bgd", probs_low, dout_heads, preferred_element_type=jnp.float32
    )
    grad_prob = jnp.einsum(
        "agrd,bgd->grab", dout_heads, value_tile, preferred_element_type=jnp.float32
    )
    grad_score = (soft_probs * (grad_prob - delta_tile.astype(jnp.float32)[:, :, :, None])).astype(
        jnp.bfloat16
    )
    query_gradient = jnp.einsum(
        "grab,bgd->agrd", grad_score, key_tile, preferred_element_type=jnp.float32
    )
    key_gradient = jnp.einsum(
        "grab,agrd->bgd", grad_score, query_heads, preferred_element_type=jnp.float32
    )
    return (query_gradient.reshape(tile_rows, groups, query_width), key_gradient, value_gradient)


def on_device(
    query_rows,
    key_rows,
    value_rows,
    output_gradient,
    row_logsumexp,
    row_delta_sums,
    segments,
    query_key_value_weight,
):
    window, kv_dev, query_width = query_rows.shape
    head_size = key_rows.shape[2]
    tile_rows = BLOCK
    block_count = window // tile_rows
    query_list, key_list = pair_lists(block_count)
    query_table = jnp.asarray(query_list)
    key_table = jnp.asarray(key_list)
    myself = lax.axis_index("tok")
    own_seg = lax.dynamic_slice_in_dim(segments, myself * window, window)
    own_live = live_pairs(own_seg, query_list, key_list, tile_rows)
    block_ids = jnp.arange(block_count, dtype=jnp.int32)
    query_match = (query_table[:, None] == block_ids[None, :]) & own_live[:, None]
    key_match = key_table[:, None] == block_ids[None, :]
    block_local = jnp.any(query_match[:, :, None] & key_match[:, None, :], axis=0)
    token_local = jnp.repeat(jnp.repeat(block_local, tile_rows, axis=0), tile_rows, axis=1)
    offsets = jnp.arange(window, dtype=jnp.int32)
    allowed_all = (
        (own_seg[:, None] == own_seg[None, :])
        & (offsets[None, :] <= offsets[:, None])
        & token_local
    )
    local_out = pair_grads(
        query_rows,
        output_gradient,
        key_rows,
        value_rows,
        row_logsumexp,
        row_delta_sums,
        allowed_all,
    )
    acc_query = local_out[0].reshape(block_count, tile_rows, kv_dev, query_width)
    acc_key = local_out[1].reshape(block_count, tile_rows, kv_dev, head_size)
    acc_value = local_out[2].reshape(block_count, tile_rows, kv_dev, head_size)
    score_scale = head_size ** (-0.5)
    query_gradient = (acc_query * score_scale).reshape(window, kv_dev, query_width)
    key_gradient = (acc_key * score_scale).reshape(window, kv_dev, head_size)
    value_gradient = acc_value.reshape(window, kv_dev, head_size)
    stacked_gradients = (
        jnp.concatenate([query_gradient, key_gradient, value_gradient], axis=2)
        .astype(jnp.bfloat16)
        .reshape(window, -1)
    )
    weight_piece = lax.all_gather(query_key_value_weight, "tok", axis=0, tiled=True)
    flat_piece = weight_piece.reshape(weight_piece.shape[0], -1)
    partial_sum = lax.dot_general(
        stacked_gradients, flat_piece, (((1,), (1,)), ((), ())), preferred_element_type=jnp.float32
    )
    summed = lax.psum_scatter(
        partial_sum.astype(jnp.bfloat16), "head", scatter_dimension=1, tiled=True
    )
    return summed


MESH = pl.DeviceIdType.MESH
LANES = 128
PIECE = 32


def fused_kernel(
    sides,
    q_hbm,
    k_hbm,
    v_hbm,
    do_hbm,
    lse_hbm,
    delta_hbm,
    seg_hbm,
    w_hbm,
    out_ref,
    q_ref,
    k_ref,
    v_ref,
    do_ref,
    lse_ref,
    delta_ref,
    seg_ref,
    joined,
    w_all,
    keep,
    part_out,
    part_in,
    x_out,
    x_in,
    back_out,
    bias,
    lse32,
    delta32,
    dk_acc,
    dv_acc,
    load_sem,
    own_send,
    own_recv,
    far_send,
    far_recv,
    relay_send,
    relay_recv,
    j_send,
    j_recv,
    part_send,
    part_recv,
    x_send,
    x_recv,
    back_send,
    back_recv,
    small_part_send,
    small_part_recv,
    small_x_send,
    small_x_recv,
    small_back_send,
    small_back_recv,
):
    window, head_size = k_ref.shape
    groups = q_ref.shape[1] // head_size
    rows = w_hbm.shape[0]
    chunks, pieces = rows // LANES, rows // PIECE
    per = LANES // PIECE
    block = window // chunks
    columns = groups + 2
    tok, h = lax.axis_index("tok"), lax.axis_index("head")
    z, y = tok // sides, tok % sides
    x, c = h // sides, h % sides
    yo, xo, co = 1 - y, 1 - x, 1 - c
    odd, upper = z % sides, z // sides
    partner = z + 1 - 2 * odd
    far = z + sides - 2 * sides * upper
    outer = upper != odd
    mine = jnp.where(c == odd, 0, 1)
    final = jnp.where(x == upper, 0, 1)

    def device(dz, dy, dx, dc):
        return (dz * sides + dy, dx * sides + dc)

    y_peer = device(z, yo, x, c)
    far_peer = device(far, y, x, c)
    j_peer = device(partner, y, x, c)
    core_peer = device(z, y, x, co)
    x_peer = device(z, y, xo, c)
    back_peer = device(partner, y, x, co)

    loads = [
        pltpu.make_async_copy(src, dst, load_sem.at[i])
        for i, (src, dst) in enumerate(
            (
                (seg_hbm, seg_ref),
                (lse_hbm, lse_ref),
                (delta_hbm, delta_ref),
                (k_hbm, k_ref),
                (v_hbm, v_ref),
                (q_hbm.at[:, :head_size], q_ref.at[:, :head_size]),
                (do_hbm.at[:, :head_size], do_ref.at[:, :head_size]),
                (q_hbm.at[:, head_size:], q_ref.at[:, head_size:]),
                (do_hbm.at[:, head_size:], do_ref.at[:, head_size:]),
                (w_hbm, w_all.at[0, y]),
            )
        )
    ]
    barrier = pltpu.get_barrier_semaphore()
    peers = (y_peer, far_peer, j_peer, core_peer, x_peer, back_peer)
    for peer in peers:
        pl.semaphore_signal(barrier, inc=1, device_id=peer, device_id_type=MESH)
    for load in loads:
        load.start()
    for load in loads[:3]:
        load.wait()
    lse32[...] = lse_ref[...].astype(jnp.float32)
    delta32[...] = delta_ref[...].astype(jnp.float32)
    seg_row = seg_ref[:, pl.ds(pl.multiple_of(tok * window, LANES), window)].astype(jnp.float32)
    seg_col = jnp.transpose(jnp.broadcast_to(seg_row, (LANES, window)))[:, :1]
    key_id = lax.broadcasted_iota(jnp.int32, (window, window), 0)
    query_id = lax.broadcasted_iota(jnp.int32, (window, window), 1)
    bias[...] = jnp.where((seg_col == seg_row) & (key_id <= query_id), 0.0, -1e30)
    def j_cols(r):
        return pl.ds(pl.multiple_of(r * head_size, head_size), head_size)

    scale = head_size ** (-0.5)
    half = window // 2

    def dot(a, b, da, db):
        return lax.dot_general(a, b, (((da,), (db,)), ((), ())), preferred_element_type=jnp.float32)

    def head(r):
        cols = j_cols(r)
        sums = []
        for start in (0, half):
            keys, queries = slice(start, start + half), slice(start, window)
            q, do = q_ref[queries, cols], do_ref[queries, cols]
            kk, vv = k_ref[keys, :], v_ref[keys, :]
            logits = dot(kk, q, 1, 1) * scale - lse32[pl.ds(r, 1), queries]
            probs = jnp.exp(logits + bias[keys, queries])
            dv_acc[keys, :] += dot(probs.astype(jnp.bfloat16), do, 1, 0)
            grad_prob = dot(vv, do, 1, 1)
            ds = (probs * (grad_prob - delta32[pl.ds(r, 1), queries])).astype(jnp.bfloat16)
            dk_acc[keys, :] += dot(ds, q, 1, 0)
            sums.append(dot(ds, kk, 0, 0))
        low = sums[0]
        joined[0, :half, cols] = (low[:half] * scale).astype(jnp.bfloat16)
        joined[0, half:, cols] = ((low[half:] + sums[1]) * scale).astype(jnp.bfloat16)

    dk_acc[...] = jnp.zeros_like(dk_acc)
    dv_acc[...] = jnp.zeros_like(dv_acc)
    for load in loads[3:7]:
        load.wait()

    @pl.when(outer)
    def _():
        head(0)

    pl.semaphore_wait(barrier, len(peers))

    def remote(src, dst, send, recv, peer):
        return pltpu.make_async_remote_copy(
            src_ref=src,
            dst_ref=dst,
            send_sem=send,
            recv_sem=recv,
            device_id=peer,
            device_id_type=MESH,
        )

    def piece_rows(p):
        return pl.ds(pl.multiple_of(p * PIECE, PIECE), PIECE)

    def chunk_rows(k):
        return pl.ds(pl.multiple_of(k * LANES, LANES), LANES)

    def block_rows(i):
        return pl.ds(pl.multiple_of(i * block, block), block)

    def own_copy(k):
        return remote(
            w_hbm.at[chunk_rows(k)],
            w_all.at[0, y, chunk_rows(k)],
            own_send.at[k],
            own_recv.at[k],
            y_peer,
        )

    def arrived_own(k):
        ref = w_all.at[0, yo, chunk_rows(k)]
        remote(ref, ref, own_send.at[k], own_recv.at[k], y_peer).wait_recv()

    def far_copy(p, part):
        return remote(
            w_hbm.at[part(p)],
            w_all.at[1, y, part(p)],
            far_send.at[p],
            far_recv.at[p],
            far_peer,
        )

    def relay_copy(p, part):
        ref = w_all.at[1, y, part(p)]
        return remote(ref, ref, relay_send.at[p], relay_recv.at[p], y_peer)

    def arrived_far(p, part):
        ref = w_all.at[1, y, part(p)]
        remote(ref, ref, far_send.at[p], far_recv.at[p], far_peer).wait_recv()

    def arrived_relay(p, part):
        ref = w_all.at[1, yo, part(p)]
        remote(ref, ref, relay_send.at[p], relay_recv.at[p], y_peer).wait_recv()

    def j_copy(r):
        return remote(
            joined.at[0, :, j_cols(r)],
            joined.at[1, :, j_cols(r)],
            j_send.at[r],
            j_recv.at[r],
            j_peer,
        )

    def j_block(i):
        return remote(
            joined.at[0, block_rows(i)],
            joined.at[1, block_rows(i)],
            j_send.at[i],
            j_recv.at[i],
            j_peer,
        )

    def each(count, body):
        lax.fori_loop(0, count, lambda i, carry: (body(i), carry)[1], 0)

    @pl.when(outer)
    def _():
        j_copy(0).start()
        each(chunks, lambda k: own_copy(k).start())

    @pl.when(jnp.logical_not(outer))
    def _():
        def both(k):
            far_copy(k, chunk_rows).start()
            own_copy(k).start()

        each(chunks, both)

    for load in loads[7:9]:
        load.wait()

    @pl.loop(jnp.where(outer, 1, 0), groups)
    def _(r):
        head(r)

        @pl.when(outer)
        def _():
            j_copy(r).start()

    wide = groups * head_size
    joined[0, :, wide : wide + head_size] = (dk_acc[...] * scale).astype(jnp.bfloat16)
    joined[0, :, wide + head_size : wide + 2 * head_size] = dv_acc[...].astype(jnp.bfloat16)
    loads[9].wait()

    def tile(ref, lead, i, by_token):
        return ref.at[(*lead, slice(None), block_rows(i))] if by_token else ref.at[(*lead, i)]

    def part_copy(slot, yr, i, by_token):
        return remote(
            tile(part_out, (slot, yr), i, by_token),
            tile(part_in, (slot, yr), i, by_token),
            part_send.at[slot, yr, i],
            part_recv.at[slot, yr, i],
            core_peer,
        )

    def x_copy(yr, i, by_token):
        return remote(
            tile(x_out, (yr,), i, by_token),
            tile(x_in, (yr,), i, by_token),
            x_send.at[yr, i],
            x_recv.at[yr, i],
            x_peer,
        )

    def out_cols(yr, k):
        return pl.ds(pl.multiple_of(yr * rows + k * LANES, LANES), LANES)

    def out_tile(ref, yr, i, by_token):
        if by_token:
            return ref.at[block_rows(i), pl.ds(pl.multiple_of(yr * rows, LANES), rows)]
        return ref.at[:, out_cols(yr, i)]

    def back_copy(yr, i, by_token):
        return remote(
            out_tile(back_out, yr, i, by_token),
            out_tile(out_ref, yr, i, by_token),
            back_send.at[yr, i],
            back_recv.at[yr, i],
            back_peer,
        )

    def unit(slot, yr, k, side):
        value = dot(joined[side], w_all[slot, yr, chunk_rows(k)], 1, 1)

        @pl.when(mine == side)
        def _():
            keep[slot, yr, k] = value

        @pl.when(mine != side)
        def _():
            part_out[slot, yr, k] = value.astype(jnp.bfloat16)
            part_copy(slot, yr, k, False).start()

    def block_unit(slot, yr, i):
        value = dot(joined[1, block_rows(i)], w_all[slot, yr], 1, 1)

        @pl.when(mine == 1)
        def _():
            for k in range(chunks):
                keep[slot, yr, k, block_rows(i)] = value[:, k * LANES : (k + 1) * LANES]

        @pl.when(mine == 0)
        def _():
            low = value.astype(jnp.bfloat16)
            for k in range(chunks):
                part_out[slot, yr, k, block_rows(i)] = low[:, k * LANES : (k + 1) * LANES]
            part_copy(slot, yr, i, True).start()

    def small(ref, lead, a, b):
        return ref.at[(*lead, b, block_rows(a))]

    def small_part(a, b):
        return remote(
            small(part_out, (1, yo), a, b),
            small(part_in, (1, yo), a, b),
            small_part_send.at[a, b],
            small_part_recv.at[a, b],
            core_peer,
        )

    def small_x(a, b):
        return remote(
            small(x_out, (yo,), a, b),
            small(x_in, (yo,), a, b),
            small_x_send.at[a, b],
            small_x_recv.at[a, b],
            x_peer,
        )

    def small_back(a, b):
        return remote(
            back_out.at[block_rows(a), out_cols(yo, b)],
            out_ref.at[block_rows(a), out_cols(yo, b)],
            small_back_send.at[a, b],
            small_back_recv.at[a, b],
            back_peer,
        )

    def small_unit(a, b):
        value = dot(joined[1, block_rows(a)], w_all[1, yo, chunk_rows(b)], 1, 1)

        @pl.when(mine == 1)
        def _():
            keep[1, yo, b, block_rows(a)] = value

        @pl.when(mine == 0)
        def _():
            part_out[1, yo, b, block_rows(a)] = value.astype(jnp.bfloat16)
            small_part(a, b).start()

    def small_core_sum(a, b):
        small_part(a, b).wait_recv()
        kept = small(keep, (1, yo), a, b)
        value = kept[...] + small(part_in, (1, yo), a, b)[...].astype(jnp.float32)

        @pl.when(final == 1)
        def _():
            kept[...] = value

        @pl.when(final == 0)
        def _():
            small(x_out, (yo,), a, b)[...] = value.astype(jnp.bfloat16)
            small_x(a, b).start()

    def small_x_sum(a, b):
        small_x(a, b).wait_recv()
        value = small(keep, (1, yo), a, b)[...] + small(x_in, (yo,), a, b)[...].astype(jnp.float32)
        back_out[block_rows(a), out_cols(yo, b)] = value.astype(jnp.bfloat16)
        small_back(a, b).start()

    def added(step, body):
        def one(j):
            body(jnp.minimum(j, step), jnp.where(j <= step, step, j - step - 1))

        each(2 * step + 1, one)

    def all_small(body):
        each(chunks * chunks, lambda j: body(j // chunks, j % chunks))

    def core_sum(slot, yr, i, by_token):
        part_copy(slot, yr, i, by_token).wait_recv()
        kept = tile(keep, (slot, yr), i, by_token)
        value = kept[...] + tile(part_in, (slot, yr), i, by_token)[...].astype(jnp.float32)

        @pl.when(slot == final)
        def _():
            kept[...] = value

        @pl.when(slot != final)
        def _():
            tile(x_out, (yr,), i, by_token)[...] = value.astype(jnp.bfloat16)
            x_copy(yr, i, by_token).start()

    def x_sum(yr, i, by_token):
        x_copy(yr, i, by_token).wait_recv()
        value = tile(keep, (final, yr), i, by_token)[...]
        value += tile(x_in, (yr,), i, by_token)[...].astype(jnp.float32)
        value = value.astype(jnp.bfloat16)

        def put(ref):
            if by_token:
                for k in range(chunks):
                    ref[block_rows(i), out_cols(yr, k)] = value[k]
            else:
                ref[:, out_cols(yr, i)] = value

        if by_token:
            put(back_out)
            back_copy(yr, i, True).start()
        else:

            @pl.when(mine == 0)
            def _():
                put(out_ref)

            @pl.when(mine == 1)
            def _():
                put(back_out)
                back_copy(yr, i, False).start()

    def which(i):
        return jnp.where(i // chunks % 2 == 0, y, yo)

    lag, turns = 2, 4

    @pl.when(outer)
    def _():
        j_copy(groups).start()
        j_copy(groups + 1).start()
        each(pieces, lambda p: far_copy(p, piece_rows).start())
        steps = 3 * chunks

        @pl.loop(0, steps + lag)
        def _(i):
            k = i % chunks

            @pl.when((i >= chunks) & (i < 2 * chunks))
            def _():
                arrived_far(k, chunk_rows)
                relay_copy(k, chunk_rows).start()
                arrived_own(k)

            @pl.when(i < steps)
            def _():
                unit(i // (2 * chunks), which(i), k, 0)

            @pl.when((i >= lag) & (mine == 0))
            def _():
                core_sum((i - lag) // (2 * chunks), which(i - lag), (i - lag) % chunks, False)

        @pl.loop(0, chunks + 1)
        def _(i):
            live = i < chunks

            def partner_sum(slot, yr):
                @pl.when(live & (mine == 1))
                def _():
                    core_sum(slot, yr, i, True)

            @pl.when(live)
            def _():
                arrived_relay(i, chunk_rows)

            @pl.when(live)
            def _():
                unit(1, yo, i, 0)

            @pl.when(live)
            def _():
                j_block(i).wait_recv()

            @pl.when(live)
            def _():
                block_unit(1, y, i)

            @pl.when(live)
            def _():
                block_unit(0, y, i)

            partner_sum(1, y)
            @pl.when(live)
            def _():
                block_unit(0, yo, i)

            partner_sum(0, y)
            @pl.when(live)
            def _():
                added(i, small_unit)

            partner_sum(0, yo)
            @pl.when((i >= 1) & (mine == 1))
            def _():
                x_sum(y, i - 1, True)

                @pl.when(final == 0)
                def _():
                    x_sum(yo, i - 1, True)

                @pl.when(final == 1)
                def _():
                    added(i - 1, small_x_sum)

            @pl.when(live & (mine == 1))
            def _():
                added(i, small_core_sum)

            @pl.when(mine == 0)
            def _():
                @pl.when(i >= 1)
                def _():
                    x_sum(yo, i - 1, False)

                @pl.when(live)
                def _():
                    core_sum(1, yo, i, False)
                    x_sum(y, i, False)

    @pl.when(jnp.logical_not(outer))
    def _():
        each(chunks, lambda b: j_block(b).start())

        @pl.loop(0, 2 * chunks + lag)
        def _(i):
            k = i % chunks

            @pl.when((i >= chunks) & (i < 2 * chunks))
            def _():
                arrived_own(k)


            @pl.when(i < 2 * chunks)
            def _():
                unit(0, which(i), k, 0)

            @pl.when((i >= lag) & (mine == 0))
            def _():
                core_sum(0, which(i - lag), (i - lag) % chunks, False)

        each(columns, lambda r: j_copy(r).wait_recv())

        @pl.loop(0, chunks + 2)
        def _(k):
            for i in range(turns):

                @pl.when(k < chunks)
                def _():
                    for j in range(per // turns):
                        p = k * per + i * (per // turns) + j
                        arrived_far(p, piece_rows)
                        relay_copy(p, piece_rows).start()

                @pl.when(k == 0)
                def _():
                    for j in range(i * 2 * chunks // turns, (i + 1) * 2 * chunks // turns):
                        unit(0, which(j), j % chunks, 1)

                @pl.when((k == 1) & (mine == 1))
                def _():
                    for j in range(i * 2 * chunks // turns, (i + 1) * 2 * chunks // turns):
                        core_sum(0, which(j), j % chunks, False)

                @pl.when((k >= 1) & (k <= chunks))
                def _():
                    if i == 0:
                        unit(1, y, k - 1, 0)
                        unit(1, y, k - 1, 1)
                    if i == 1:
                        core_sum(1, y, k - 1, False)
                    if i == 2:
                        for j in range(per):
                            arrived_relay((k - 1) * per + j, piece_rows)
                        unit(1, yo, k - 1, 0)
                        unit(1, yo, k - 1, 1)
                    if i == 3:
                        core_sum(1, yo, k - 1, False)

                        @pl.when(final == 1)
                        def _():
                            x_sum(y, k - 1, False)

                @pl.when(k >= 2)
                def _():
                    if i == 0:

                        @pl.when(final == 1)
                        def _():
                            x_sum(yo, k - 2, False)

                    @pl.when((final == 0) & (k < chunks))
                    def _():
                        if i < 2:
                            x_sum((y, yo)[i], 2 * k - 4, False)
                            x_sum((y, yo)[i], 2 * k - 3, False)

    inner = jnp.logical_not(outer)

    def tiles(condition, copies, wait):
        @pl.when(condition)
        def _():
            each(chunks, lambda i: wait(copies(i)))

    def smalls(condition, copies, wait):
        @pl.when(condition)
        def _():
            all_small(lambda a, b: wait(copies(a, b)))

    def received(copy):
        copy.wait_recv()

    def sent(copy):
        copy.wait_send()

    back = mine == 1
    tiles(back, lambda i: back_copy(y, i, False), received)
    tiles(back & (outer | (final == 0)), lambda i: back_copy(yo, i, False), received)
    smalls(back & inner & (final == 1), small_back, received)
    tiles(back, lambda i: back_copy(y, i, False), sent)
    tiles(back & (inner | (final == 0)), lambda i: back_copy(yo, i, False), sent)
    smalls(back & outer & (final == 1), small_back, sent)
    by_small = outer & (final == 0) & (mine == 1)
    tiles(jnp.logical_not(by_small), lambda i: x_copy(yo, i, False), sent)
    smalls(by_small, small_x, sent)
    by_small = outer & (mine == 0)
    tiles(jnp.logical_not(by_small), lambda i: part_copy(1, yo, i, False), sent)
    smalls(by_small, small_part, sent)

    @pl.loop(0, chunks)
    def _(i):
        x_copy(y, i, False).wait_send()
        part_copy(0, y, i, False).wait_send()
        part_copy(0, yo, i, False).wait_send()
        part_copy(1, y, i, False).wait_send()

    each(chunks, lambda k: own_copy(k).wait_send())

    @pl.when(outer)
    def _():
        each(pieces, lambda p: far_copy(p, piece_rows).wait_send())
        each(chunks, lambda k: relay_copy(k, chunk_rows).wait_send())

    @pl.when(inner)
    def _():
        each(chunks, lambda k: far_copy(k, chunk_rows).wait_send())
        each(pieces, lambda p: relay_copy(p, piece_rows).wait_send())

    @pl.when(outer)
    def _():
        each(columns, lambda r: j_copy(r).wait_send())

    @pl.when(jnp.logical_not(outer))
    def _():
        each(chunks, lambda i: j_block(i).wait_send())


def fused(sides, q, k, v, do, lse, delta, segments, weight):
    window, _, query_width = q.shape
    head_size = k.shape[2]
    rows, _, width = weight.shape
    chunks, pieces = rows // LANES, rows // PIECE
    columns = width // head_size
    bf16, f32 = jnp.bfloat16, jnp.float32
    dma = pltpu.SemaphoreType.DMA
    vmem = pl.BlockSpec(memory_space=pltpu.VMEM)
    hbm = pl.BlockSpec(memory_space=pl.ANY)
    tile = (window, LANES)
    return pl.pallas_call(
        functools.partial(fused_kernel, sides),
        out_shape=jax.ShapeDtypeStruct((window, 2 * rows), bf16),
        in_specs=[hbm] * 8,
        out_specs=vmem,
        scratch_shapes=[
            pltpu.VMEM((window, query_width), bf16),
            pltpu.VMEM((window, head_size), bf16),
            pltpu.VMEM((window, head_size), bf16),
            pltpu.VMEM((window, query_width), bf16),
            pltpu.VMEM(lse.shape[1:], bf16),
            pltpu.VMEM(lse.shape[1:], bf16),
            pltpu.VMEM((1,) + segments.shape, segments.dtype),
            pltpu.VMEM((2, window, width), bf16),
            pltpu.VMEM((2, 2, rows, width), bf16),
            pltpu.VMEM((2, 2, chunks) + tile, f32),
            pltpu.VMEM((2, 2, chunks) + tile, bf16),
            pltpu.VMEM((2, 2, chunks) + tile, bf16),
            pltpu.VMEM((2, chunks) + tile, bf16),
            pltpu.VMEM((2, chunks) + tile, bf16),
            pltpu.VMEM((window, 2 * rows), bf16),
            pltpu.VMEM((window, window), f32),
            pltpu.VMEM(lse.shape[1:], f32),
            pltpu.VMEM(lse.shape[1:], f32),
            pltpu.VMEM((window, head_size), f32),
            pltpu.VMEM((window, head_size), f32),
            dma((10,)),
            dma((pieces,)),
            dma((pieces,)),
            dma((pieces,)),
            dma((pieces,)),
            dma((pieces,)),
            dma((pieces,)),
            dma((columns,)),
            dma((columns,)),
            dma((2, 2, chunks)),
            dma((2, 2, chunks)),
            dma((2, chunks)),
            dma((2, chunks)),
            dma((2, chunks)),
            dma((2, chunks)),
            *[dma((chunks, chunks))] * 6,
        ],
        compiler_params=pltpu.CompilerParams(
            collective_id=0, has_side_effects=True, vmem_limit_bytes=40 * 1024 * 1024
        ),
    )(
        *(
            pltpu.with_memory_space_constraint(array, pltpu.HBM)
            for array in (
                q.reshape(window, query_width),
                k.reshape(window, head_size),
                v.reshape(window, head_size),
                do.reshape(window, query_width),
                lse.reshape(lse.shape[1:]),
                delta.reshape(delta.shape[1:]),
                segments.reshape(1, -1),
                weight.reshape(rows, width),
            )
        )
    )


def solution(mesh):
    placed = (
        P("tok", "head", None),
        P("tok", "head", None),
        P("tok", "head", None),
        P("tok", "head", None),
        P("head", None, "tok"),
        P("head", None, "tok"),
        P(),
        P("tok", "head", None),
    )
    tok, heads = mesh.shape["tok"], mesh.shape["head"]
    sides = tok // heads

    def step(*args):
        window, kv_dev, _ = args[0].shape
        rows = args[7].shape[0]
        paired = sides == 2 and heads == sides * sides and tok == heads * sides and kv_dev == 1
        if paired and rows % LANES == 0 and window % (2 * LANES) == 0 and args[1].shape[2] == LANES:
            return fused(sides, *args)
        return on_device(*args)

    return jax.shard_map(
        step, mesh=mesh, in_specs=placed, out_specs=P("tok", "head"), check_vma=False
    )
```

```python
import functools

import jax
import jax.numpy as jnp
import numpy as np
from jax import lax
from jax.experimental import pallas as pl
from jax.experimental.pallas import tpu as pltpu
from jax.sharding import PartitionSpec as P

BLOCK = 128


def pair_lists(block_count):
    query_list = []
    key_list = []
    for query_block in range(block_count):
        for key_block in range(query_block + 1):
            query_list.append(query_block)
            key_list.append(key_block)
    return (np.array(query_list, np.int32), np.array(key_list, np.int32))


def live_pairs(seg_window, query_list, key_list, tile_rows):
    first_seg = jnp.take(seg_window, query_list * tile_rows)
    last_seg = jnp.take(seg_window, key_list * tile_rows + tile_rows - 1)
    return (first_seg == last_seg) | jnp.asarray(query_list == key_list)


def pair_grads(query_tile, dout_tile, key_tile, value_tile, lse_tile, delta_tile, allowed):
    tile_rows, groups, query_width = query_tile.shape
    head_size = key_tile.shape[2]
    heads_per_group = query_width // head_size
    query_heads = query_tile.reshape(tile_rows, groups, heads_per_group, head_size)
    dout_heads = dout_tile.reshape(tile_rows, groups, heads_per_group, head_size)
    scores = jnp.einsum(
        "agrd,bgd->grab", query_heads, key_tile, preferred_element_type=jnp.float32
    ) * head_size ** (-0.5)
    logits = scores - lse_tile.astype(jnp.float32)[:, :, :, None]
    soft_probs = jnp.where(allowed[None, None], jnp.exp(logits), 0.0)
    probs_low = soft_probs.astype(jnp.bfloat16)
    value_gradient = jnp.einsum(
        "grab,agrd->bgd", probs_low, dout_heads, preferred_element_type=jnp.float32
    )
    grad_prob = jnp.einsum(
        "agrd,bgd->grab", dout_heads, value_tile, preferred_element_type=jnp.float32
    )
    grad_score = (soft_probs * (grad_prob - delta_tile.astype(jnp.float32)[:, :, :, None])).astype(
        jnp.bfloat16
    )
    query_gradient = jnp.einsum(
        "grab,bgd->agrd", grad_score, key_tile, preferred_element_type=jnp.float32
    )
    key_gradient = jnp.einsum(
        "grab,agrd->bgd", grad_score, query_heads, preferred_element_type=jnp.float32
    )
    return (query_gradient.reshape(tile_rows, groups, query_width), key_gradient, value_gradient)


def on_device(
    query_rows,
    key_rows,
    value_rows,
    output_gradient,
    row_logsumexp,
    row_delta_sums,
    segments,
    query_key_value_weight,
):
    window, kv_dev, query_width = query_rows.shape
    head_size = key_rows.shape[2]
    tile_rows = BLOCK
    block_count = window // tile_rows
    query_list, key_list = pair_lists(block_count)
    query_table = jnp.asarray(query_list)
    key_table = jnp.asarray(key_list)
    myself = lax.axis_index("tok")
    own_seg = lax.dynamic_slice_in_dim(segments, myself * window, window)
    own_live = live_pairs(own_seg, query_list, key_list, tile_rows)
    block_ids = jnp.arange(block_count, dtype=jnp.int32)
    query_match = (query_table[:, None] == block_ids[None, :]) & own_live[:, None]
    key_match = key_table[:, None] == block_ids[None, :]
    block_local = jnp.any(query_match[:, :, None] & key_match[:, None, :], axis=0)
    token_local = jnp.repeat(jnp.repeat(block_local, tile_rows, axis=0), tile_rows, axis=1)
    offsets = jnp.arange(window, dtype=jnp.int32)
    allowed_all = (
        (own_seg[:, None] == own_seg[None, :])
        & (offsets[None, :] <= offsets[:, None])
        & token_local
    )
    local_out = pair_grads(
        query_rows,
        output_gradient,
        key_rows,
        value_rows,
        row_logsumexp,
        row_delta_sums,
        allowed_all,
    )
    acc_query = local_out[0].reshape(block_count, tile_rows, kv_dev, query_width)
    acc_key = local_out[1].reshape(block_count, tile_rows, kv_dev, head_size)
    acc_value = local_out[2].reshape(block_count, tile_rows, kv_dev, head_size)
    score_scale = head_size ** (-0.5)
    query_gradient = (acc_query * score_scale).reshape(window, kv_dev, query_width)
    key_gradient = (acc_key * score_scale).reshape(window, kv_dev, head_size)
    value_gradient = acc_value.reshape(window, kv_dev, head_size)
    stacked_gradients = (
        jnp.concatenate([query_gradient, key_gradient, value_gradient], axis=2)
        .astype(jnp.bfloat16)
        .reshape(window, -1)
    )
    weight_piece = lax.all_gather(query_key_value_weight, "tok", axis=0, tiled=True)
    flat_piece = weight_piece.reshape(weight_piece.shape[0], -1)
    partial_sum = lax.dot_general(
        stacked_gradients, flat_piece, (((1,), (1,)), ((), ())), preferred_element_type=jnp.float32
    )
    summed = lax.psum_scatter(
        partial_sum.astype(jnp.bfloat16), "head", scatter_dimension=1, tiled=True
    )
    return summed


MESH = pl.DeviceIdType.MESH
LANES = 128
PIECE = 32


def fused_kernel(
    sides,
    q_hbm,
    k_hbm,
    v_hbm,
    do_hbm,
    lse_hbm,
    delta_hbm,
    seg_hbm,
    w_hbm,
    out_ref,
    q_ref,
    k_ref,
    v_ref,
    do_ref,
    lse_ref,
    delta_ref,
    seg_ref,
    joined,
    w_all,
    keep,
    part_out,
    part_in,
    x_out,
    x_in,
    back_out,
    direct_out,
    direct_in,
    bias,
    lse32,
    delta32,
    dk_acc,
    dv_acc,
    load_sem,
    own_send,
    own_recv,
    far_send,
    far_recv,
    relay_send,
    relay_recv,
    j_send,
    j_recv,
    part_send,
    part_recv,
    x_send,
    x_recv,
    back_send,
    back_recv,
    small_part_send,
    small_part_recv,
    small_x_send,
    small_x_recv,
    small_back_send,
    small_back_recv,
    direct_send,
    direct_recv,
):
    window, head_size = k_ref.shape
    groups = q_ref.shape[1] // head_size
    rows = w_hbm.shape[0]
    chunks, pieces = rows // LANES, rows // PIECE
    per = LANES // PIECE
    block = window // chunks
    columns = groups + 2
    tok, h = lax.axis_index("tok"), lax.axis_index("head")
    z, y = tok // sides, tok % sides
    x, c = h // sides, h % sides
    yo, xo, co = 1 - y, 1 - x, 1 - c
    odd, upper = z % sides, z // sides
    partner = z + 1 - 2 * odd
    far = z + sides - 2 * sides * upper
    middle = upper != odd
    ends = jnp.logical_not(middle)
    mine = jnp.where(c == odd, 0, 1)
    final = jnp.where(x == upper, 0, 1)

    def device(dz, dy, dx, dc):
        return (dz * sides + dy, dx * sides + dc)

    y_peer = device(z, yo, x, c)
    far_peer = device(far, y, x, c)
    j_peer = device(partner, y, x, c)
    core_peer = device(z, y, x, co)
    x_peer = device(z, y, xo, c)
    back_peer = device(partner, y, x, co)

    loads = [
        pltpu.make_async_copy(src, dst, load_sem.at[i])
        for i, (src, dst) in enumerate(
            (
                (seg_hbm, seg_ref),
                (lse_hbm, lse_ref),
                (delta_hbm, delta_ref),
                (k_hbm, k_ref),
                (v_hbm, v_ref),
                (q_hbm.at[:, :head_size], q_ref.at[:, :head_size]),
                (do_hbm.at[:, :head_size], do_ref.at[:, :head_size]),
                (q_hbm.at[:, head_size:], q_ref.at[:, head_size:]),
                (do_hbm.at[:, head_size:], do_ref.at[:, head_size:]),
                (w_hbm, w_all.at[0, y]),
            )
        )
    ]
    barrier = pltpu.get_barrier_semaphore()
    cross_peer = device(partner, y, xo, co)
    peers = (y_peer, far_peer, j_peer, core_peer, x_peer, back_peer, cross_peer)
    for peer in peers:
        pl.semaphore_signal(barrier, inc=1, device_id=peer, device_id_type=MESH)
    for load in loads:
        load.start()

    def j_cols(r):
        return pl.ds(pl.multiple_of(r * head_size, head_size), head_size)

    scale = head_size ** (-0.5)
    half = window // 2

    def dot(a, b, da, db):
        return lax.dot_general(a, b, (((da,), (db,)), ((), ())), preferred_element_type=jnp.float32)

    def head(r):
        cols = j_cols(r)
        sums = []
        for start in (0, half):
            keys, queries = slice(start, start + half), slice(start, window)
            q, do = q_ref[queries, cols], do_ref[queries, cols]
            kk, vv = k_ref[keys, :], v_ref[keys, :]
            logits = dot(kk, q, 1, 1) * scale - lse32[pl.ds(r, 1), queries]
            probs = jnp.exp(logits + bias[keys, queries])
            dv_acc[keys, :] += dot(probs.astype(jnp.bfloat16), do, 1, 0)
            grad_prob = dot(vv, do, 1, 1)
            ds = (probs * (grad_prob - delta32[pl.ds(r, 1), queries])).astype(jnp.bfloat16)
            dk_acc[keys, :] += dot(ds, q, 1, 0)
            sums.append(dot(ds, kk, 0, 0))
        low = sums[0]
        joined[0, :half, cols] = (low[:half] * scale).astype(jnp.bfloat16)
        joined[0, half:, cols] = ((low[half:] + sums[1]) * scale).astype(jnp.bfloat16)

    def remote(src, dst, send, recv, peer):
        return pltpu.make_async_remote_copy(
            src_ref=src,
            dst_ref=dst,
            send_sem=send,
            recv_sem=recv,
            device_id=peer,
            device_id_type=MESH,
        )

    def piece_rows(p):
        return pl.ds(pl.multiple_of(p * PIECE, PIECE), PIECE)

    def chunk_rows(k):
        return pl.ds(pl.multiple_of(k * LANES, LANES), LANES)

    def block_rows(i):
        return pl.ds(pl.multiple_of(i * block, block), block)

    def own_copy(k):
        return remote(
            w_hbm.at[chunk_rows(k)],
            w_all.at[0, y, chunk_rows(k)],
            own_send.at[k],
            own_recv.at[k],
            y_peer,
        )

    def arrived_own(k):
        ref = w_all.at[0, yo, chunk_rows(k)]
        remote(ref, ref, own_send.at[k], own_recv.at[k], y_peer).wait_recv()

    def far_copy(p, part):
        return remote(
            w_hbm.at[part(p)],
            w_all.at[1, y, part(p)],
            far_send.at[p],
            far_recv.at[p],
            far_peer,
        )

    def relay_copy(p, part):
        ref = w_all.at[1, y, part(p)]
        return remote(ref, ref, relay_send.at[p], relay_recv.at[p], y_peer)

    def arrived_far(p, part):
        ref = w_all.at[1, y, part(p)]
        remote(ref, ref, far_send.at[p], far_recv.at[p], far_peer).wait_recv()

    def arrived_relay(p, part):
        ref = w_all.at[1, yo, part(p)]
        remote(ref, ref, relay_send.at[p], relay_recv.at[p], y_peer).wait_recv()

    def j_copy(r):
        return remote(
            joined.at[0, :, j_cols(r)],
            joined.at[1, :, j_cols(r)],
            j_send.at[r],
            j_recv.at[r],
            j_peer,
        )

    def j_block(i):
        return remote(
            joined.at[0, block_rows(i)],
            joined.at[1, block_rows(i)],
            j_send.at[i],
            j_recv.at[i],
            j_peer,
        )

    def each(count, body):
        lax.fori_loop(0, count, lambda i, carry: (body(i), carry)[1], 0)

    def enter():
        pl.semaphore_wait(barrier, len(peers))

    @pl.when(ends)
    def _():
        enter()

        def both(k):
            far_copy(k, chunk_rows).start()
            own_copy(k).start()

        each(chunks, both)

    for load in loads[:3]:
        load.wait()
    lse32[...] = lse_ref[...].astype(jnp.float32)
    delta32[...] = delta_ref[...].astype(jnp.float32)
    seg_row = seg_ref[:, pl.ds(pl.multiple_of(tok * window, LANES), window)].astype(jnp.float32)
    seg_col = jnp.transpose(jnp.broadcast_to(seg_row, (LANES, window)))[:, :1]
    key_id = lax.broadcasted_iota(jnp.int32, (window, window), 0)
    query_id = lax.broadcasted_iota(jnp.int32, (window, window), 1)
    bias[...] = jnp.where((seg_col == seg_row) & (key_id <= query_id), 0.0, -1e30)
    dk_acc[...] = jnp.zeros_like(dk_acc)
    dv_acc[...] = jnp.zeros_like(dv_acc)
    for load in loads[3:7]:
        load.wait()

    @pl.when(middle)
    def _():
        head(0)
        enter()
        j_copy(0).start()
        each(chunks, lambda k: own_copy(k).start())

    for load in loads[7:9]:
        load.wait()

    @pl.loop(jnp.where(middle, 1, 0), groups)
    def _(r):
        head(r)

        @pl.when(middle)
        def _():
            j_copy(r).start()

    wide = groups * head_size
    joined[0, :, wide : wide + head_size] = (dk_acc[...] * scale).astype(jnp.bfloat16)
    joined[0, :, wide + head_size : wide + 2 * head_size] = dv_acc[...].astype(jnp.bfloat16)
    loads[9].wait()

    def tile(ref, lead, i, by_token):
        return ref.at[(*lead, slice(None), block_rows(i))] if by_token else ref.at[(*lead, i)]

    def part_copy(slot, yr, i, by_token):
        return remote(
            tile(part_out, (slot, yr), i, by_token),
            tile(part_in, (slot, yr), i, by_token),
            part_send.at[slot, yr, i],
            part_recv.at[slot, yr, i],
            core_peer,
        )

    def x_copy(yr, i, by_token):
        return remote(
            tile(x_out, (yr,), i, by_token),
            tile(x_in, (yr,), i, by_token),
            x_send.at[yr, i],
            x_recv.at[yr, i],
            x_peer,
        )

    def out_cols(yr, k):
        return pl.ds(pl.multiple_of(yr * rows + k * LANES, LANES), LANES)

    def out_tile(ref, yr, i, by_token):
        if by_token:
            return ref.at[block_rows(i), pl.ds(pl.multiple_of(yr * rows, LANES), rows)]
        return ref.at[:, out_cols(yr, i)]

    def back_copy(yr, i, by_token):
        return remote(
            out_tile(back_out, yr, i, by_token),
            out_tile(out_ref, yr, i, by_token),
            back_send.at[yr, i],
            back_recv.at[yr, i],
            back_peer,
        )

    def unit(slot, yr, k, side):
        value = dot(joined[side], w_all[slot, yr, chunk_rows(k)], 1, 1)

        @pl.when(mine == side)
        def _():
            keep[slot, yr, k] = value

        @pl.when(mine != side)
        def _():
            part_out[slot, yr, k] = value.astype(jnp.bfloat16)
            part_copy(slot, yr, k, False).start()

    def block_unit(slot, yr, i):
        value = dot(joined[1, block_rows(i)], w_all[slot, yr], 1, 1)

        @pl.when(mine == 1)
        def _():
            for k in range(chunks):
                keep[slot, yr, k, block_rows(i)] = value[:, k * LANES : (k + 1) * LANES]

        @pl.when(mine == 0)
        def _():
            low = value.astype(jnp.bfloat16)
            for k in range(chunks):
                part_out[slot, yr, k, block_rows(i)] = low[:, k * LANES : (k + 1) * LANES]
            part_copy(slot, yr, i, True).start()

    def small(ref, lead, a, b):
        return ref.at[(*lead, b, block_rows(a))]

    def small_part(a, b):
        return remote(
            small(part_out, (1, yo), a, b),
            small(part_in, (1, yo), a, b),
            small_part_send.at[a, b],
            small_part_recv.at[a, b],
            core_peer,
        )

    def small_x(a, b):
        return remote(
            small(x_out, (yo,), a, b),
            small(x_in, (yo,), a, b),
            small_x_send.at[a, b],
            small_x_recv.at[a, b],
            x_peer,
        )

    def small_back(a, b):
        return remote(
            back_out.at[block_rows(a), out_cols(yo, b)],
            out_ref.at[block_rows(a), out_cols(yo, b)],
            small_back_send.at[a, b],
            small_back_recv.at[a, b],
            back_peer,
        )

    def small_unit(a, b):
        value = dot(joined[1, block_rows(a)], w_all[1, yo, chunk_rows(b)], 1, 1)

        @pl.when(mine == 1)
        def _():
            keep[1, yo, b, block_rows(a)] = value

        @pl.when(mine == 0)
        def _():
            part_out[1, yo, b, block_rows(a)] = value.astype(jnp.bfloat16)
            small_part(a, b).start()

    def small_core_sum(a, b):
        small_part(a, b).wait_recv()
        kept = small(keep, (1, yo), a, b)
        value = kept[...] + small(part_in, (1, yo), a, b)[...].astype(jnp.float32)

        @pl.when(final == 1)
        def _():
            kept[...] = value

        @pl.when(final == 0)
        def _():
            small(x_out, (yo,), a, b)[...] = value.astype(jnp.bfloat16)
            small_x(a, b).start()

    def small_x_sum(a, b):
        small_x(a, b).wait_recv()
        value = small(keep, (1, yo), a, b)[...] + small(x_in, (yo,), a, b)[...].astype(jnp.float32)
        back_out[block_rows(a), out_cols(yo, b)] = value.astype(jnp.bfloat16)
        small_back(a, b).start()

    end = chunks - 1

    def direct_copy(yr, source, peer):
        return remote(
            direct_out.at[yr],
            direct_in.at[source, yr],
            direct_send.at[yr],
            direct_recv.at[source, yr],
            peer,
        )

    def direct_sum(yr):
        part_copy(1, yr, end, False).wait_recv()
        value = keep[1, yr, end] + part_in[1, yr, end].astype(jnp.float32)
        direct_out[yr] = value.astype(jnp.bfloat16)

        @pl.when(final == 1)
        def _():
            direct_copy(yr, 0, back_peer).start()

        @pl.when(final == 0)
        def _():
            direct_copy(yr, 1, cross_peer).start()

    def far_sum(yr, k):
        whole = (k == end) & (mine == 1)

        @pl.when(whole)
        def _():
            direct_sum(yr)

        @pl.when(jnp.logical_not(whole))
        def _():
            core_sum(1, yr, k, False)

    def far_x_sum(yr, k):
        @pl.when((final == 1) & ((k < end) | (mine == 0)))
        def _():
            x_sum(yr, k, False)

    def added(step, body):
        def one(j):
            body(jnp.minimum(j, step), jnp.where(j <= step, step, j - step - 1))

        each(2 * step + 1, one)

    def all_small(body):
        each(chunks * chunks, lambda j: body(j // chunks, j % chunks))

    def core_sum(slot, yr, i, by_token):
        part_copy(slot, yr, i, by_token).wait_recv()
        kept = tile(keep, (slot, yr), i, by_token)
        value = kept[...] + tile(part_in, (slot, yr), i, by_token)[...].astype(jnp.float32)

        @pl.when(slot == final)
        def _():
            kept[...] = value

        @pl.when(slot != final)
        def _():
            tile(x_out, (yr,), i, by_token)[...] = value.astype(jnp.bfloat16)
            x_copy(yr, i, by_token).start()

    def x_sum(yr, i, by_token):
        x_copy(yr, i, by_token).wait_recv()
        value = tile(keep, (final, yr), i, by_token)[...]
        value += tile(x_in, (yr,), i, by_token)[...].astype(jnp.float32)
        value = value.astype(jnp.bfloat16)

        def put(ref):
            if by_token:
                for k in range(chunks):
                    ref[block_rows(i), out_cols(yr, k)] = value[k]
            else:
                ref[:, out_cols(yr, i)] = value

        if by_token:
            put(back_out)
            back_copy(yr, i, True).start()
        else:

            @pl.when(mine == 0)
            def _():
                put(out_ref)

            @pl.when(mine == 1)
            def _():
                put(back_out)
                back_copy(yr, i, False).start()

    def which(i):
        return jnp.where(i // chunks % 2 == 0, y, yo)

    lag, turns = 2, 4

    @pl.when(middle)
    def _():
        j_copy(groups).start()
        j_copy(groups + 1).start()
        each(pieces, lambda p: far_copy(p, piece_rows).start())
        steps = 3 * chunks

        @pl.loop(0, steps + lag)
        def _(i):
            k = i % chunks

            @pl.when((i >= chunks) & (i < 2 * chunks))
            def _():
                arrived_far(k, chunk_rows)
                relay_copy(k, chunk_rows).start()
                arrived_own(k)

            @pl.when(i < steps)
            def _():
                unit(i // (2 * chunks), which(i), k, 0)

            @pl.when((i >= lag) & (mine == 0))
            def _():
                core_sum((i - lag) // (2 * chunks), which(i - lag), (i - lag) % chunks, False)

        @pl.loop(0, chunks + 1)
        def _(i):
            live = i < chunks

            def partner_sum(slot, yr):
                @pl.when(live & (mine == 1))
                def _():
                    core_sum(slot, yr, i, True)

            @pl.when(live)
            def _():
                j_block(i).wait_recv()

            @pl.when(live)
            def _():
                block_unit(1, y, i)

            @pl.when(live)
            def _():
                block_unit(0, y, i)

            @pl.when(live)
            def _():
                block_unit(0, yo, i)

            partner_sum(1, y)
            partner_sum(0, y)
            @pl.when((i >= 1) & (mine == 1))
            def _():
                x_sum(y, i - 1, True)

                @pl.when(final == 0)
                def _():
                    x_sum(yo, i - 1, True)

                @pl.when(final == 1)
                def _():
                    added(i - 1, small_x_sum)

            partner_sum(0, yo)
            @pl.when(live)
            def _():
                arrived_relay(i, chunk_rows)

            @pl.when(live)
            def _():
                added(i, small_unit)

            @pl.when(live & (mine == 1))
            def _():
                added(i, small_core_sum)

            @pl.when(live)
            def _():
                unit(1, yo, i, 0)

            @pl.when(mine == 0)
            def _():
                @pl.when(i >= 1)
                def _():
                    x_sum(yo, i - 1, False)

                @pl.when(live)
                def _():
                    core_sum(1, yo, i, False)
                    x_sum(y, i, False)

    @pl.when(ends)
    def _():
        each(chunks, lambda b: j_block(b).start())

        @pl.loop(0, 2 * chunks + lag)
        def _(i):
            k = i % chunks

            @pl.when((i >= chunks) & (i < 2 * chunks))
            def _():
                arrived_own(k)


            @pl.when(i < 2 * chunks)
            def _():
                unit(0, which(i), k, 0)

            @pl.when((i >= lag) & (mine == 0))
            def _():
                core_sum(0, which(i - lag), (i - lag) % chunks, False)

        each(columns, lambda r: j_copy(r).wait_recv())

        @pl.loop(0, chunks + 2)
        def _(k):
            for i in range(turns):

                @pl.when(k < chunks)
                def _():
                    for j in range(per // turns):
                        p = k * per + i * (per // turns) + j
                        arrived_far(p, piece_rows)
                        relay_copy(p, piece_rows).start()

                @pl.when(k == 0)
                def _():
                    for j in range(i * 2 * chunks // turns, (i + 1) * 2 * chunks // turns):
                        unit(0, which(j), j % chunks, 1)

                @pl.when((k == 1) & (mine == 1))
                def _():
                    for j in range(i * 2 * chunks // turns, (i + 1) * 2 * chunks // turns):
                        core_sum(0, which(j), j % chunks, False)

                @pl.when((k >= 1) & (k <= chunks))
                def _():
                    if i == 0:
                        unit(1, y, k - 1, 1)
                        unit(1, y, k - 1, 0)
                    if i == 1:
                        far_sum(y, k - 1)
                    if i == 2:
                        for j in range(per):
                            arrived_relay((k - 1) * per + j, piece_rows)
                        unit(1, yo, k - 1, 1)
                        unit(1, yo, k - 1, 0)
                    if i == 3:
                        far_sum(yo, k - 1)
                        far_x_sum(y, k - 1)

                @pl.when(k >= 2)
                def _():
                    if i == 0:
                        far_x_sum(yo, k - 2)

                    @pl.when((final == 0) & (k < chunks))
                    def _():
                        if i < 2:
                            x_sum((y, yo)[i], 2 * k - 4, False)
                            x_sum((y, yo)[i], 2 * k - 3, False)


    def tiles(condition, copies, wait, count=chunks):
        @pl.when(condition)
        def _():
            each(count, lambda i: wait(copies(i)))

    def smalls(condition, copies, wait):
        @pl.when(condition)
        def _():
            all_small(lambda a, b: wait(copies(a, b)))

    def received(copy):
        copy.wait_recv()

    def sent(copy):
        copy.wait_send()

    back = mine == 1
    count_in = jnp.where(middle & (final == 1), end, chunks)
    count_out = jnp.where(ends & (final == 1), end, chunks)
    count_x = jnp.where(ends & back & (final == 0), end, chunks)
    tiles(back, lambda i: back_copy(y, i, False), received, count_in)
    tiles(back & (middle | (final == 0)), lambda i: back_copy(yo, i, False), received, count_in)
    smalls(back & ends & (final == 1), small_back, received)

    @pl.when(back & middle & (final == 1))
    def _():
        for yr in (y, yo):
            direct_copy(yr, 0, back_peer).wait_recv()
            direct_copy(yr, 1, back_peer).wait_recv()
            value = direct_in[0, yr].astype(jnp.float32) + direct_in[1, yr].astype(jnp.float32)
            out_ref[:, out_cols(yr, end)] = value.astype(jnp.bfloat16)

    @pl.when(back & ends)
    def _():
        direct_copy(y, 0, back_peer).wait_send()
        direct_copy(yo, 0, back_peer).wait_send()

    tiles(back, lambda i: back_copy(y, i, False), sent, count_out)
    tiles(back & (ends | (final == 0)), lambda i: back_copy(yo, i, False), sent, count_out)
    smalls(back & middle & (final == 1), small_back, sent)
    by_small = middle & (final == 0) & (mine == 1)
    tiles(jnp.logical_not(by_small), lambda i: x_copy(yo, i, False), sent, count_x)
    tiles(True, lambda i: x_copy(y, i, False), sent, count_x)
    smalls(by_small, small_x, sent)
    by_small = middle & (mine == 0)
    tiles(jnp.logical_not(by_small), lambda i: part_copy(1, yo, i, False), sent)
    smalls(by_small, small_part, sent)

    @pl.loop(0, chunks)
    def _(i):
        part_copy(0, y, i, False).wait_send()
        part_copy(0, yo, i, False).wait_send()
        part_copy(1, y, i, False).wait_send()

    each(chunks, lambda k: own_copy(k).wait_send())

    @pl.when(middle)
    def _():
        each(pieces, lambda p: far_copy(p, piece_rows).wait_send())
        each(chunks, lambda k: relay_copy(k, chunk_rows).wait_send())

    @pl.when(ends)
    def _():
        each(chunks, lambda k: far_copy(k, chunk_rows).wait_send())
        each(pieces, lambda p: relay_copy(p, piece_rows).wait_send())

    @pl.when(middle)
    def _():
        each(columns, lambda r: j_copy(r).wait_send())

    @pl.when(ends)
    def _():
        each(chunks, lambda i: j_block(i).wait_send())


def fused(sides, q, k, v, do, lse, delta, segments, weight):
    window, _, query_width = q.shape
    head_size = k.shape[2]
    rows, _, width = weight.shape
    chunks, pieces = rows // LANES, rows // PIECE
    columns = width // head_size
    bf16, f32 = jnp.bfloat16, jnp.float32
    dma = pltpu.SemaphoreType.DMA
    vmem = pl.BlockSpec(memory_space=pltpu.VMEM)
    hbm = pl.BlockSpec(memory_space=pl.ANY)
    tile = (window, LANES)
    return pl.pallas_call(
        functools.partial(fused_kernel, sides),
        out_shape=jax.ShapeDtypeStruct((window, 2 * rows), bf16),
        in_specs=[hbm] * 8,
        out_specs=vmem,
        scratch_shapes=[
            pltpu.VMEM((window, query_width), bf16),
            pltpu.VMEM((window, head_size), bf16),
            pltpu.VMEM((window, head_size), bf16),
            pltpu.VMEM((window, query_width), bf16),
            pltpu.VMEM(lse.shape[1:], bf16),
            pltpu.VMEM(lse.shape[1:], bf16),
            pltpu.VMEM((1,) + segments.shape, segments.dtype),
            pltpu.VMEM((2, window, width), bf16),
            pltpu.VMEM((2, 2, rows, width), bf16),
            pltpu.VMEM((2, 2, chunks) + tile, f32),
            pltpu.VMEM((2, 2, chunks) + tile, bf16),
            pltpu.VMEM((2, 2, chunks) + tile, bf16),
            pltpu.VMEM((2, chunks) + tile, bf16),
            pltpu.VMEM((2, chunks) + tile, bf16),
            pltpu.VMEM((window, 2 * rows), bf16),
            pltpu.VMEM((2,) + tile, bf16),
            pltpu.VMEM((2, 2) + tile, bf16),
            pltpu.VMEM((window, window), f32),
            pltpu.VMEM(lse.shape[1:], f32),
            pltpu.VMEM(lse.shape[1:], f32),
            pltpu.VMEM((window, head_size), f32),
            pltpu.VMEM((window, head_size), f32),
            dma((10,)),
            dma((pieces,)),
            dma((pieces,)),
            dma((pieces,)),
            dma((pieces,)),
            dma((pieces,)),
            dma((pieces,)),
            dma((columns,)),
            dma((columns,)),
            dma((2, 2, chunks)),
            dma((2, 2, chunks)),
            dma((2, chunks)),
            dma((2, chunks)),
            dma((2, chunks)),
            dma((2, chunks)),
            *[dma((chunks, chunks))] * 6,
            dma((2,)),
            dma((2, 2)),
        ],
        compiler_params=pltpu.CompilerParams(
            collective_id=0, has_side_effects=True, vmem_limit_bytes=40 * 1024 * 1024
        ),
    )(
        *(
            pltpu.with_memory_space_constraint(array, pltpu.HBM)
            for array in (
                q.reshape(window, query_width),
                k.reshape(window, head_size),
                v.reshape(window, head_size),
                do.reshape(window, query_width),
                lse.reshape(lse.shape[1:]),
                delta.reshape(delta.shape[1:]),
                segments.reshape(1, -1),
                weight.reshape(rows, width),
            )
        )
    )


def solution(mesh):
    placed = (
        P("tok", "head", None),
        P("tok", "head", None),
        P("tok", "head", None),
        P("tok", "head", None),
        P("head", None, "tok"),
        P("head", None, "tok"),
        P(),
        P("tok", "head", None),
    )
    tok, heads = mesh.shape["tok"], mesh.shape["head"]
    sides = tok // heads

    def step(*args):
        window, kv_dev, _ = args[0].shape
        rows = args[7].shape[0]
        paired = sides == 2 and heads == sides * sides and tok == heads * sides and kv_dev == 1
        if paired and rows % LANES == 0 and window % (2 * LANES) == 0 and args[1].shape[2] == LANES:
            return fused(sides, *args)
        return on_device(*args)

    return jax.shard_map(
        step, mesh=mesh, in_specs=placed, out_specs=P("tok", "head"), check_vma=False
    )
```

```python
import functools

import jax
import jax.numpy as jnp
import numpy as np
from jax import lax
from jax.experimental import pallas as pl
from jax.experimental.pallas import tpu as pltpu
from jax.sharding import PartitionSpec as P

BLOCK = 128


def pair_lists(block_count):
    query_list = []
    key_list = []
    for query_block in range(block_count):
        for key_block in range(query_block + 1):
            query_list.append(query_block)
            key_list.append(key_block)
    return (np.array(query_list, np.int32), np.array(key_list, np.int32))


def live_pairs(seg_window, query_list, key_list, tile_rows):
    first_seg = jnp.take(seg_window, query_list * tile_rows)
    last_seg = jnp.take(seg_window, key_list * tile_rows + tile_rows - 1)
    return (first_seg == last_seg) | jnp.asarray(query_list == key_list)


def pair_grads(query_tile, dout_tile, key_tile, value_tile, lse_tile, delta_tile, allowed):
    tile_rows, groups, query_width = query_tile.shape
    head_size = key_tile.shape[2]
    heads_per_group = query_width // head_size
    query_heads = query_tile.reshape(tile_rows, groups, heads_per_group, head_size)
    dout_heads = dout_tile.reshape(tile_rows, groups, heads_per_group, head_size)
    scores = jnp.einsum(
        "agrd,bgd->grab", query_heads, key_tile, preferred_element_type=jnp.float32
    ) * head_size ** (-0.5)
    logits = scores - lse_tile.astype(jnp.float32)[:, :, :, None]
    soft_probs = jnp.where(allowed[None, None], jnp.exp(logits), 0.0)
    probs_low = soft_probs.astype(jnp.bfloat16)
    value_gradient = jnp.einsum(
        "grab,agrd->bgd", probs_low, dout_heads, preferred_element_type=jnp.float32
    )
    grad_prob = jnp.einsum(
        "agrd,bgd->grab", dout_heads, value_tile, preferred_element_type=jnp.float32
    )
    grad_score = (soft_probs * (grad_prob - delta_tile.astype(jnp.float32)[:, :, :, None])).astype(
        jnp.bfloat16
    )
    query_gradient = jnp.einsum(
        "grab,bgd->agrd", grad_score, key_tile, preferred_element_type=jnp.float32
    )
    key_gradient = jnp.einsum(
        "grab,agrd->bgd", grad_score, query_heads, preferred_element_type=jnp.float32
    )
    return (query_gradient.reshape(tile_rows, groups, query_width), key_gradient, value_gradient)


def on_device(
    query_rows,
    key_rows,
    value_rows,
    output_gradient,
    row_logsumexp,
    row_delta_sums,
    segments,
    query_key_value_weight,
):
    window, kv_dev, query_width = query_rows.shape
    head_size = key_rows.shape[2]
    tile_rows = BLOCK
    block_count = window // tile_rows
    query_list, key_list = pair_lists(block_count)
    query_table = jnp.asarray(query_list)
    key_table = jnp.asarray(key_list)
    myself = lax.axis_index("tok")
    own_seg = lax.dynamic_slice_in_dim(segments, myself * window, window)
    own_live = live_pairs(own_seg, query_list, key_list, tile_rows)
    block_ids = jnp.arange(block_count, dtype=jnp.int32)
    query_match = (query_table[:, None] == block_ids[None, :]) & own_live[:, None]
    key_match = key_table[:, None] == block_ids[None, :]
    block_local = jnp.any(query_match[:, :, None] & key_match[:, None, :], axis=0)
    token_local = jnp.repeat(jnp.repeat(block_local, tile_rows, axis=0), tile_rows, axis=1)
    offsets = jnp.arange(window, dtype=jnp.int32)
    allowed_all = (
        (own_seg[:, None] == own_seg[None, :])
        & (offsets[None, :] <= offsets[:, None])
        & token_local
    )
    local_out = pair_grads(
        query_rows,
        output_gradient,
        key_rows,
        value_rows,
        row_logsumexp,
        row_delta_sums,
        allowed_all,
    )
    acc_query = local_out[0].reshape(block_count, tile_rows, kv_dev, query_width)
    acc_key = local_out[1].reshape(block_count, tile_rows, kv_dev, head_size)
    acc_value = local_out[2].reshape(block_count, tile_rows, kv_dev, head_size)
    score_scale = head_size ** (-0.5)
    query_gradient = (acc_query * score_scale).reshape(window, kv_dev, query_width)
    key_gradient = (acc_key * score_scale).reshape(window, kv_dev, head_size)
    value_gradient = acc_value.reshape(window, kv_dev, head_size)
    stacked_gradients = (
        jnp.concatenate([query_gradient, key_gradient, value_gradient], axis=2)
        .astype(jnp.bfloat16)
        .reshape(window, -1)
    )
    weight_piece = lax.all_gather(query_key_value_weight, "tok", axis=0, tiled=True)
    flat_piece = weight_piece.reshape(weight_piece.shape[0], -1)
    partial_sum = lax.dot_general(
        stacked_gradients, flat_piece, (((1,), (1,)), ((), ())), preferred_element_type=jnp.float32
    )
    summed = lax.psum_scatter(
        partial_sum.astype(jnp.bfloat16), "head", scatter_dimension=1, tiled=True
    )
    return summed


MESH = pl.DeviceIdType.MESH
LANES = 128
PIECE = 32


def fused_kernel(
    sides,
    q_hbm,
    k_hbm,
    v_hbm,
    do_hbm,
    lse_hbm,
    delta_hbm,
    seg_hbm,
    w_hbm,
    out_ref,
    q_ref,
    k_ref,
    v_ref,
    do_ref,
    lse_ref,
    delta_ref,
    seg_ref,
    joined,
    w_all,
    keep,
    part_out,
    part_in,
    x_out,
    x_in,
    back_out,
    direct_out,
    direct_in,
    bias,
    lse32,
    delta32,
    dk_acc,
    dv_acc,
    load_sem,
    own_send,
    own_recv,
    far_send,
    far_recv,
    relay_send,
    relay_recv,
    j_send,
    j_recv,
    part_send,
    part_recv,
    x_send,
    x_recv,
    back_send,
    back_recv,
    small_part_send,
    small_part_recv,
    small_x_send,
    small_x_recv,
    small_back_send,
    small_back_recv,
    direct_send,
    direct_recv,
):
    window, head_size = k_ref.shape
    groups = q_ref.shape[1] // head_size
    rows = w_hbm.shape[0]
    chunks, pieces = rows // LANES, rows // PIECE
    per = LANES // PIECE
    block = window // chunks
    columns = groups + 2
    tok, h = lax.axis_index("tok"), lax.axis_index("head")
    z, y = tok // sides, tok % sides
    x, c = h // sides, h % sides
    yo, xo, co = 1 - y, 1 - x, 1 - c
    odd, upper = z % sides, z // sides
    partner = z + 1 - 2 * odd
    far = z + sides - 2 * sides * upper
    middle = upper != odd
    ends = jnp.logical_not(middle)
    mine = jnp.where(c == odd, 0, 1)
    final = jnp.where(x == upper, 0, 1)

    def device(dz, dy, dx, dc):
        return (dz * sides + dy, dx * sides + dc)

    y_peer = device(z, yo, x, c)
    far_peer = device(far, y, x, c)
    j_peer = device(partner, y, x, c)
    core_peer = device(z, y, x, co)
    x_peer = device(z, y, xo, c)
    back_peer = device(partner, y, x, co)

    loads = [
        pltpu.make_async_copy(src, dst, load_sem.at[i])
        for i, (src, dst) in enumerate(
            (
                (seg_hbm, seg_ref),
                (lse_hbm, lse_ref),
                (delta_hbm, delta_ref),
                (k_hbm, k_ref),
                (v_hbm, v_ref),
                (q_hbm.at[:, :head_size], q_ref.at[:, :head_size]),
                (do_hbm.at[:, :head_size], do_ref.at[:, :head_size]),
                (q_hbm.at[:, head_size:], q_ref.at[:, head_size:]),
                (do_hbm.at[:, head_size:], do_ref.at[:, head_size:]),
                (w_hbm, w_all.at[0, y]),
            )
        )
    ]
    barrier = pltpu.get_barrier_semaphore()
    cross_peer = device(partner, y, xo, co)
    peers = (y_peer, far_peer, j_peer, core_peer, x_peer, back_peer, cross_peer)
    for peer in peers:
        pl.semaphore_signal(barrier, inc=1, device_id=peer, device_id_type=MESH)

    def j_cols(r):
        return pl.ds(pl.multiple_of(r * head_size, head_size), head_size)

    scale = head_size ** (-0.5)
    half = window // 2

    def dot(a, b, da, db):
        return lax.dot_general(a, b, (((da,), (db,)), ((), ())), preferred_element_type=jnp.float32)

    def head(r):
        cols = j_cols(r)
        sums = []
        for start in (0, half):
            keys, queries = slice(start, start + half), slice(start, window)
            q, do = q_ref[queries, cols], do_ref[queries, cols]
            kk, vv = k_ref[keys, :], v_ref[keys, :]
            logits = dot(kk, q, 1, 1) * scale - lse32[pl.ds(r, 1), queries]
            probs = jnp.exp(logits + bias[keys, queries])
            dv_acc[keys, :] += dot(probs.astype(jnp.bfloat16), do, 1, 0)
            grad_prob = dot(vv, do, 1, 1)
            ds = (probs * (grad_prob - delta32[pl.ds(r, 1), queries])).astype(jnp.bfloat16)
            dk_acc[keys, :] += dot(ds, q, 1, 0)
            sums.append(dot(ds, kk, 0, 0))
        low = sums[0]
        joined[0, :half, cols] = (low[:half] * scale).astype(jnp.bfloat16)
        joined[0, half:, cols] = ((low[half:] + sums[1]) * scale).astype(jnp.bfloat16)

    def remote(src, dst, send, recv, peer):
        return pltpu.make_async_remote_copy(
            src_ref=src,
            dst_ref=dst,
            send_sem=send,
            recv_sem=recv,
            device_id=peer,
            device_id_type=MESH,
        )

    def piece_rows(p):
        return pl.ds(pl.multiple_of(p * PIECE, PIECE), PIECE)

    def chunk_rows(k):
        return pl.ds(pl.multiple_of(k * LANES, LANES), LANES)

    def block_rows(i):
        return pl.ds(pl.multiple_of(i * block, block), block)

    def own_copy(k):
        return remote(
            w_hbm.at[chunk_rows(k)],
            w_all.at[0, y, chunk_rows(k)],
            own_send.at[k],
            own_recv.at[k],
            y_peer,
        )

    def arrived_own(k):
        ref = w_all.at[0, yo, chunk_rows(k)]
        remote(ref, ref, own_send.at[k], own_recv.at[k], y_peer).wait_recv()

    def far_copy(p, part):
        return remote(
            w_hbm.at[part(p)],
            w_all.at[1, y, part(p)],
            far_send.at[p],
            far_recv.at[p],
            far_peer,
        )

    def relay_copy(p, part):
        ref = w_all.at[1, y, part(p)]
        return remote(ref, ref, relay_send.at[p], relay_recv.at[p], y_peer)

    def arrived_far(p, part):
        ref = w_all.at[1, y, part(p)]
        remote(ref, ref, far_send.at[p], far_recv.at[p], far_peer).wait_recv()

    def arrived_relay(p, part):
        ref = w_all.at[1, yo, part(p)]
        remote(ref, ref, relay_send.at[p], relay_recv.at[p], y_peer).wait_recv()

    def j_copy(r):
        return remote(
            joined.at[0, :, j_cols(r)],
            joined.at[1, :, j_cols(r)],
            j_send.at[r],
            j_recv.at[r],
            j_peer,
        )

    def j_block(i):
        return remote(
            joined.at[0, block_rows(i)],
            joined.at[1, block_rows(i)],
            j_send.at[i],
            j_recv.at[i],
            j_peer,
        )

    def each(count, body):
        lax.fori_loop(0, count, lambda i, carry: (body(i), carry)[1], 0)

    def enter():
        pl.semaphore_wait(barrier, len(peers))

    def load_all():
        for load in loads:
            load.start()

    @pl.when(middle)
    def _():
        load_all()

    @pl.when(ends)
    def _():
        enter()

        def both(k):
            far_copy(k, chunk_rows).start()
            own_copy(k).start()

        each(chunks, both)
        load_all()

    for load in loads[:3]:
        load.wait()
    lse32[...] = lse_ref[...].astype(jnp.float32)
    delta32[...] = delta_ref[...].astype(jnp.float32)
    seg_row = seg_ref[:, pl.ds(pl.multiple_of(tok * window, LANES), window)].astype(jnp.float32)
    seg_col = jnp.transpose(jnp.broadcast_to(seg_row, (LANES, window)))[:, :1]
    key_id = lax.broadcasted_iota(jnp.int32, (window, window), 0)
    query_id = lax.broadcasted_iota(jnp.int32, (window, window), 1)
    bias[...] = jnp.where((seg_col == seg_row) & (key_id <= query_id), 0.0, -1e30)
    dk_acc[...] = jnp.zeros_like(dk_acc)
    dv_acc[...] = jnp.zeros_like(dv_acc)
    for load in loads[3:7]:
        load.wait()

    @pl.when(middle)
    def _():
        head(0)
        enter()
        j_copy(0).start()
        each(chunks, lambda k: own_copy(k).start())

    for load in loads[7:9]:
        load.wait()

    @pl.loop(jnp.where(middle, 1, 0), groups)
    def _(r):
        head(r)

        @pl.when(middle)
        def _():
            j_copy(r).start()

    wide = groups * head_size
    joined[0, :, wide : wide + head_size] = (dk_acc[...] * scale).astype(jnp.bfloat16)
    joined[0, :, wide + head_size : wide + 2 * head_size] = dv_acc[...].astype(jnp.bfloat16)
    loads[9].wait()

    def tile(ref, lead, i, by_token):
        return ref.at[(*lead, slice(None), block_rows(i))] if by_token else ref.at[(*lead, i)]

    def part_copy(slot, yr, i, by_token):
        return remote(
            tile(part_out, (slot, yr), i, by_token),
            tile(part_in, (slot, yr), i, by_token),
            part_send.at[slot, yr, i],
            part_recv.at[slot, yr, i],
            core_peer,
        )

    def x_copy(yr, i, by_token):
        return remote(
            tile(x_out, (yr,), i, by_token),
            tile(x_in, (yr,), i, by_token),
            x_send.at[yr, i],
            x_recv.at[yr, i],
            x_peer,
        )

    def out_cols(yr, k):
        return pl.ds(pl.multiple_of(yr * rows + k * LANES, LANES), LANES)

    def out_tile(ref, yr, i, by_token):
        if by_token:
            return ref.at[block_rows(i), pl.ds(pl.multiple_of(yr * rows, LANES), rows)]
        return ref.at[:, out_cols(yr, i)]

    def back_copy(yr, i, by_token):
        return remote(
            out_tile(back_out, yr, i, by_token),
            out_tile(out_ref, yr, i, by_token),
            back_send.at[yr, i],
            back_recv.at[yr, i],
            back_peer,
        )

    def unit(slot, yr, k, side):
        value = dot(joined[side], w_all[slot, yr, chunk_rows(k)], 1, 1)

        @pl.when(mine == side)
        def _():
            keep[slot, yr, k] = value

        @pl.when(mine != side)
        def _():
            part_out[slot, yr, k] = value.astype(jnp.bfloat16)
            part_copy(slot, yr, k, False).start()

    def block_unit(slot, yr, i):
        value = dot(joined[1, block_rows(i)], w_all[slot, yr], 1, 1)

        @pl.when(mine == 1)
        def _():
            for k in range(chunks):
                keep[slot, yr, k, block_rows(i)] = value[:, k * LANES : (k + 1) * LANES]

        @pl.when(mine == 0)
        def _():
            low = value.astype(jnp.bfloat16)
            for k in range(chunks):
                part_out[slot, yr, k, block_rows(i)] = low[:, k * LANES : (k + 1) * LANES]
            part_copy(slot, yr, i, True).start()

    def small(ref, lead, a, b):
        return ref.at[(*lead, b, block_rows(a))]

    def small_part(a, b):
        return remote(
            small(part_out, (1, yo), a, b),
            small(part_in, (1, yo), a, b),
            small_part_send.at[a, b],
            small_part_recv.at[a, b],
            core_peer,
        )

    def small_x(a, b):
        return remote(
            small(x_out, (yo,), a, b),
            small(x_in, (yo,), a, b),
            small_x_send.at[a, b],
            small_x_recv.at[a, b],
            x_peer,
        )

    def small_back(a, b):
        return remote(
            back_out.at[block_rows(a), out_cols(yo, b)],
            out_ref.at[block_rows(a), out_cols(yo, b)],
            small_back_send.at[a, b],
            small_back_recv.at[a, b],
            back_peer,
        )

    def small_unit(a, b):
        value = dot(joined[1, block_rows(a)], w_all[1, yo, chunk_rows(b)], 1, 1)

        @pl.when(mine == 1)
        def _():
            keep[1, yo, b, block_rows(a)] = value

        @pl.when(mine == 0)
        def _():
            part_out[1, yo, b, block_rows(a)] = value.astype(jnp.bfloat16)
            small_part(a, b).start()

    def small_core_sum(a, b):
        small_part(a, b).wait_recv()
        kept = small(keep, (1, yo), a, b)
        value = kept[...] + small(part_in, (1, yo), a, b)[...].astype(jnp.float32)

        @pl.when(final == 1)
        def _():
            kept[...] = value

        @pl.when(final == 0)
        def _():
            small(x_out, (yo,), a, b)[...] = value.astype(jnp.bfloat16)
            small_x(a, b).start()

    def small_x_sum(a, b):
        small_x(a, b).wait_recv()
        value = small(keep, (1, yo), a, b)[...] + small(x_in, (yo,), a, b)[...].astype(jnp.float32)
        back_out[block_rows(a), out_cols(yo, b)] = value.astype(jnp.bfloat16)
        small_back(a, b).start()

    end = chunks - 1

    def direct_copy(source, peer):
        return remote(direct_out, direct_in.at[source], direct_send, direct_recv.at[source], peer)

    def direct_sum():
        part_copy(1, yo, end, False).wait_recv()
        value = keep[1, yo, end] + part_in[1, yo, end].astype(jnp.float32)
        direct_out[...] = value.astype(jnp.bfloat16)

        @pl.when(final == 1)
        def _():
            direct_copy(0, back_peer).start()

        @pl.when(final == 0)
        def _():
            direct_copy(1, cross_peer).start()

    def relayed_sum(k):
        whole = (k == end) & (mine == 1)

        @pl.when(whole)
        def _():
            direct_sum()

        @pl.when(jnp.logical_not(whole))
        def _():
            core_sum(1, yo, k, False)

    def relayed_x_sum(k):
        @pl.when((final == 1) & ((k < end) | (mine == 0)))
        def _():
            x_sum(yo, k, False)

    def added(step, body):
        def one(j):
            body(jnp.minimum(j, step), jnp.where(j <= step, step, j - step - 1))

        each(2 * step + 1, one)

    def all_small(body):
        each(chunks * chunks, lambda j: body(j // chunks, j % chunks))

    def core_sum(slot, yr, i, by_token):
        part_copy(slot, yr, i, by_token).wait_recv()
        kept = tile(keep, (slot, yr), i, by_token)
        value = kept[...] + tile(part_in, (slot, yr), i, by_token)[...].astype(jnp.float32)

        @pl.when(slot == final)
        def _():
            kept[...] = value

        @pl.when(slot != final)
        def _():
            tile(x_out, (yr,), i, by_token)[...] = value.astype(jnp.bfloat16)
            x_copy(yr, i, by_token).start()

    def x_sum(yr, i, by_token):
        x_copy(yr, i, by_token).wait_recv()
        value = tile(keep, (final, yr), i, by_token)[...]
        value += tile(x_in, (yr,), i, by_token)[...].astype(jnp.float32)
        value = value.astype(jnp.bfloat16)

        def put(ref):
            if by_token:
                for k in range(chunks):
                    ref[block_rows(i), out_cols(yr, k)] = value[k]
            else:
                ref[:, out_cols(yr, i)] = value

        if by_token:
            put(back_out)
            back_copy(yr, i, True).start()
        else:

            @pl.when(mine == 0)
            def _():
                put(out_ref)

            @pl.when(mine == 1)
            def _():
                put(back_out)
                back_copy(yr, i, False).start()

    def which(i):
        return jnp.where(i // chunks % 2 == 0, y, yo)

    lag, turns = 2, 4

    @pl.when(middle)
    def _():
        j_copy(groups).start()
        j_copy(groups + 1).start()
        each(pieces, lambda p: far_copy(p, piece_rows).start())
        steps = 3 * chunks

        @pl.loop(0, steps + lag)
        def _(i):
            k = i % chunks

            @pl.when((i >= chunks) & (i < 2 * chunks))
            def _():
                arrived_far(k, chunk_rows)
                relay_copy(k, chunk_rows).start()
                arrived_own(k)

            @pl.when(i < steps)
            def _():
                unit(i // (2 * chunks), which(i), k, 0)

            @pl.when((i >= lag) & (mine == 0))
            def _():
                core_sum((i - lag) // (2 * chunks), which(i - lag), (i - lag) % chunks, False)

        @pl.loop(0, chunks + 1)
        def _(i):
            live = i < chunks

            def partner_sum(slot, yr):
                @pl.when(live & (mine == 1))
                def _():
                    core_sum(slot, yr, i, True)

            @pl.when(live)
            def _():
                j_block(i).wait_recv()

            @pl.when(live)
            def _():
                block_unit(1, y, i)

            @pl.when(live)
            def _():
                block_unit(0, y, i)

            @pl.when(live)
            def _():
                block_unit(0, yo, i)

            partner_sum(1, y)
            partner_sum(0, y)
            @pl.when((i >= 1) & (mine == 1))
            def _():
                x_sum(y, i - 1, True)

                @pl.when(final == 0)
                def _():
                    x_sum(yo, i - 1, True)

                @pl.when(final == 1)
                def _():
                    added(i - 1, small_x_sum)

            partner_sum(0, yo)
            @pl.when(live)
            def _():
                arrived_relay(i, chunk_rows)

            @pl.when(live)
            def _():
                added(i, small_unit)

            @pl.when(live & (mine == 1))
            def _():
                added(i, small_core_sum)

            @pl.when(live)
            def _():
                unit(1, yo, i, 0)

            @pl.when(mine == 0)
            def _():
                @pl.when(i >= 1)
                def _():
                    x_sum(yo, i - 1, False)

                @pl.when(live)
                def _():
                    core_sum(1, yo, i, False)
                    x_sum(y, i, False)

    @pl.when(ends)
    def _():
        each(chunks, lambda b: j_block(b).start())

        @pl.loop(0, 2 * chunks + lag)
        def _(i):
            k = i % chunks

            @pl.when((i >= chunks) & (i < 2 * chunks))
            def _():
                arrived_own(k)


            @pl.when(i < 2 * chunks)
            def _():
                unit(0, which(i), k, 0)

            @pl.when((i >= lag) & (mine == 0))
            def _():
                core_sum(0, which(i - lag), (i - lag) % chunks, False)

        each(columns, lambda r: j_copy(r).wait_recv())

        @pl.loop(0, chunks + 2)
        def _(k):
            for i in range(turns):

                @pl.when(k < chunks)
                def _():
                    for j in range(per // turns):
                        p = k * per + i * (per // turns) + j
                        arrived_far(p, piece_rows)
                        relay_copy(p, piece_rows).start()

                @pl.when(k == 0)
                def _():
                    for j in range(i * 2 * chunks // turns, (i + 1) * 2 * chunks // turns):
                        unit(0, which(j), j % chunks, 1)

                @pl.when((k == 1) & (mine == 1))
                def _():
                    for j in range(i * 2 * chunks // turns, (i + 1) * 2 * chunks // turns):
                        core_sum(0, which(j), j % chunks, False)

                @pl.when((k >= 1) & (k <= chunks))
                def _():
                    if i == 0:
                        unit(1, y, k - 1, 1)
                        unit(1, y, k - 1, 0)
                    if i == 1:
                        core_sum(1, y, k - 1, False)
                    if i == 2:
                        for j in range(per):
                            arrived_relay((k - 1) * per + j, piece_rows)
                        unit(1, yo, k - 1, 1)
                        unit(1, yo, k - 1, 0)
                    if i == 3:
                        relayed_sum(k - 1)

                        @pl.when(final == 1)
                        def _():
                            x_sum(y, k - 1, False)

                @pl.when(k >= 2)
                def _():
                    if i == 0:
                        relayed_x_sum(k - 2)

                    @pl.when((final == 0) & (k < chunks))
                    def _():
                        if i < 2:
                            x_sum((y, yo)[i], 2 * k - 4, False)
                            x_sum((y, yo)[i], 2 * k - 3, False)


    def tiles(condition, copies, wait, count=chunks):
        @pl.when(condition)
        def _():
            each(count, lambda i: wait(copies(i)))

    def smalls(condition, copies, wait):
        @pl.when(condition)
        def _():
            all_small(lambda a, b: wait(copies(a, b)))

    def received(copy):
        copy.wait_recv()

    def sent(copy):
        copy.wait_send()

    back = mine == 1
    count_in = jnp.where(middle & (final == 1), end, chunks)
    count_out = jnp.where(ends & (final == 1), end, chunks)
    count_x = jnp.where(ends & back & (final == 0), end, chunks)
    tiles(back, lambda i: back_copy(y, i, False), received)
    tiles(back & (middle | (final == 0)), lambda i: back_copy(yo, i, False), received, count_in)
    smalls(back & ends & (final == 1), small_back, received)

    @pl.when(back & middle & (final == 1))
    def _():
        direct_copy(0, back_peer).wait_recv()
        direct_copy(1, back_peer).wait_recv()
        value = direct_in[0].astype(jnp.float32) + direct_in[1].astype(jnp.float32)
        out_ref[:, out_cols(yo, end)] = value.astype(jnp.bfloat16)

    @pl.when(back & ends)
    def _():
        direct_copy(0, back_peer).wait_send()

    tiles(back, lambda i: back_copy(y, i, False), sent)
    tiles(back & (ends | (final == 0)), lambda i: back_copy(yo, i, False), sent, count_out)
    smalls(back & middle & (final == 1), small_back, sent)
    by_small = middle & (final == 0) & (mine == 1)
    tiles(jnp.logical_not(by_small), lambda i: x_copy(yo, i, False), sent, count_x)
    tiles(True, lambda i: x_copy(y, i, False), sent)
    smalls(by_small, small_x, sent)
    by_small = middle & (mine == 0)
    tiles(jnp.logical_not(by_small), lambda i: part_copy(1, yo, i, False), sent)
    smalls(by_small, small_part, sent)

    @pl.loop(0, chunks)
    def _(i):
        part_copy(0, y, i, False).wait_send()
        part_copy(0, yo, i, False).wait_send()
        part_copy(1, y, i, False).wait_send()

    each(chunks, lambda k: own_copy(k).wait_send())

    @pl.when(middle)
    def _():
        each(pieces, lambda p: far_copy(p, piece_rows).wait_send())
        each(chunks, lambda k: relay_copy(k, chunk_rows).wait_send())

    @pl.when(ends)
    def _():
        each(chunks, lambda k: far_copy(k, chunk_rows).wait_send())
        each(pieces, lambda p: relay_copy(p, piece_rows).wait_send())

    @pl.when(middle)
    def _():
        each(columns, lambda r: j_copy(r).wait_send())

    @pl.when(ends)
    def _():
        each(chunks, lambda i: j_block(i).wait_send())


def fused(sides, q, k, v, do, lse, delta, segments, weight):
    window, _, query_width = q.shape
    head_size = k.shape[2]
    rows, _, width = weight.shape
    chunks, pieces = rows // LANES, rows // PIECE
    columns = width // head_size
    bf16, f32 = jnp.bfloat16, jnp.float32
    dma = pltpu.SemaphoreType.DMA
    vmem = pl.BlockSpec(memory_space=pltpu.VMEM)
    hbm = pl.BlockSpec(memory_space=pl.ANY)
    tile = (window, LANES)
    return pl.pallas_call(
        functools.partial(fused_kernel, sides),
        out_shape=jax.ShapeDtypeStruct((window, 2 * rows), bf16),
        in_specs=[hbm] * 8,
        out_specs=vmem,
        scratch_shapes=[
            pltpu.VMEM((window, query_width), bf16),
            pltpu.VMEM((window, head_size), bf16),
            pltpu.VMEM((window, head_size), bf16),
            pltpu.VMEM((window, query_width), bf16),
            pltpu.VMEM(lse.shape[1:], bf16),
            pltpu.VMEM(lse.shape[1:], bf16),
            pltpu.VMEM((1,) + segments.shape, segments.dtype),
            pltpu.VMEM((2, window, width), bf16),
            pltpu.VMEM((2, 2, rows, width), bf16),
            pltpu.VMEM((2, 2, chunks) + tile, f32),
            pltpu.VMEM((2, 2, chunks) + tile, bf16),
            pltpu.VMEM((2, 2, chunks) + tile, bf16),
            pltpu.VMEM((2, chunks) + tile, bf16),
            pltpu.VMEM((2, chunks) + tile, bf16),
            pltpu.VMEM((window, 2 * rows), bf16),
            pltpu.VMEM(tile, bf16),
            pltpu.VMEM((2,) + tile, bf16),
            pltpu.VMEM((window, window), f32),
            pltpu.VMEM(lse.shape[1:], f32),
            pltpu.VMEM(lse.shape[1:], f32),
            pltpu.VMEM((window, head_size), f32),
            pltpu.VMEM((window, head_size), f32),
            dma((10,)),
            dma((pieces,)),
            dma((pieces,)),
            dma((pieces,)),
            dma((pieces,)),
            dma((pieces,)),
            dma((pieces,)),
            dma((columns,)),
            dma((columns,)),
            dma((2, 2, chunks)),
            dma((2, 2, chunks)),
            dma((2, chunks)),
            dma((2, chunks)),
            dma((2, chunks)),
            dma((2, chunks)),
            *[dma((chunks, chunks))] * 6,
            dma,
            dma((2,)),
        ],
        compiler_params=pltpu.CompilerParams(
            collective_id=0, has_side_effects=True, vmem_limit_bytes=40 * 1024 * 1024
        ),
    )(
        *(
            pltpu.with_memory_space_constraint(array, pltpu.HBM)
            for array in (
                q.reshape(window, query_width),
                k.reshape(window, head_size),
                v.reshape(window, head_size),
                do.reshape(window, query_width),
                lse.reshape(lse.shape[1:]),
                delta.reshape(delta.shape[1:]),
                segments.reshape(1, -1),
                weight.reshape(rows, width),
            )
        )
    )


def solution(mesh):
    placed = (
        P("tok", "head", None),
        P("tok", "head", None),
        P("tok", "head", None),
        P("tok", "head", None),
        P("head", None, "tok"),
        P("head", None, "tok"),
        P(),
        P("tok", "head", None),
    )
    tok, heads = mesh.shape["tok"], mesh.shape["head"]
    sides = tok // heads

    def step(*args):
        window, kv_dev, _ = args[0].shape
        rows = args[7].shape[0]
        paired = sides == 2 and heads == sides * sides and tok == heads * sides and kv_dev == 1
        if paired and rows % LANES == 0 and window % (2 * LANES) == 0 and args[1].shape[2] == LANES:
            return fused(sides, *args)
        return on_device(*args)

    return jax.shard_map(
        step, mesh=mesh, in_specs=placed, out_specs=P("tok", "head"), check_vma=False
    )
```

```python
import functools

import jax
import jax.numpy as jnp
import numpy as np
from jax import lax
from jax.experimental import pallas as pl
from jax.experimental.pallas import tpu as pltpu
from jax.sharding import PartitionSpec as P

BLOCK = 128


def pair_lists(block_count):
    query_list = []
    key_list = []
    for query_block in range(block_count):
        for key_block in range(query_block + 1):
            query_list.append(query_block)
            key_list.append(key_block)
    return (np.array(query_list, np.int32), np.array(key_list, np.int32))


def live_pairs(seg_window, query_list, key_list, tile_rows):
    first_seg = jnp.take(seg_window, query_list * tile_rows)
    last_seg = jnp.take(seg_window, key_list * tile_rows + tile_rows - 1)
    return (first_seg == last_seg) | jnp.asarray(query_list == key_list)


def pair_grads(query_tile, dout_tile, key_tile, value_tile, lse_tile, delta_tile, allowed):
    tile_rows, groups, query_width = query_tile.shape
    head_size = key_tile.shape[2]
    heads_per_group = query_width // head_size
    query_heads = query_tile.reshape(tile_rows, groups, heads_per_group, head_size)
    dout_heads = dout_tile.reshape(tile_rows, groups, heads_per_group, head_size)
    scores = jnp.einsum(
        "agrd,bgd->grab", query_heads, key_tile, preferred_element_type=jnp.float32
    ) * head_size ** (-0.5)
    logits = scores - lse_tile.astype(jnp.float32)[:, :, :, None]
    soft_probs = jnp.where(allowed[None, None], jnp.exp(logits), 0.0)
    probs_low = soft_probs.astype(jnp.bfloat16)
    value_gradient = jnp.einsum(
        "grab,agrd->bgd", probs_low, dout_heads, preferred_element_type=jnp.float32
    )
    grad_prob = jnp.einsum(
        "agrd,bgd->grab", dout_heads, value_tile, preferred_element_type=jnp.float32
    )
    grad_score = (soft_probs * (grad_prob - delta_tile.astype(jnp.float32)[:, :, :, None])).astype(
        jnp.bfloat16
    )
    query_gradient = jnp.einsum(
        "grab,bgd->agrd", grad_score, key_tile, preferred_element_type=jnp.float32
    )
    key_gradient = jnp.einsum(
        "grab,agrd->bgd", grad_score, query_heads, preferred_element_type=jnp.float32
    )
    return (query_gradient.reshape(tile_rows, groups, query_width), key_gradient, value_gradient)


def on_device(
    query_rows,
    key_rows,
    value_rows,
    output_gradient,
    row_logsumexp,
    row_delta_sums,
    segments,
    query_key_value_weight,
):
    window, kv_dev, query_width = query_rows.shape
    head_size = key_rows.shape[2]
    tile_rows = BLOCK
    block_count = window // tile_rows
    query_list, key_list = pair_lists(block_count)
    query_table = jnp.asarray(query_list)
    key_table = jnp.asarray(key_list)
    myself = lax.axis_index("tok")
    own_seg = lax.dynamic_slice_in_dim(segments, myself * window, window)
    own_live = live_pairs(own_seg, query_list, key_list, tile_rows)
    block_ids = jnp.arange(block_count, dtype=jnp.int32)
    query_match = (query_table[:, None] == block_ids[None, :]) & own_live[:, None]
    key_match = key_table[:, None] == block_ids[None, :]
    block_local = jnp.any(query_match[:, :, None] & key_match[:, None, :], axis=0)
    token_local = jnp.repeat(jnp.repeat(block_local, tile_rows, axis=0), tile_rows, axis=1)
    offsets = jnp.arange(window, dtype=jnp.int32)
    allowed_all = (
        (own_seg[:, None] == own_seg[None, :])
        & (offsets[None, :] <= offsets[:, None])
        & token_local
    )
    local_out = pair_grads(
        query_rows,
        output_gradient,
        key_rows,
        value_rows,
        row_logsumexp,
        row_delta_sums,
        allowed_all,
    )
    acc_query = local_out[0].reshape(block_count, tile_rows, kv_dev, query_width)
    acc_key = local_out[1].reshape(block_count, tile_rows, kv_dev, head_size)
    acc_value = local_out[2].reshape(block_count, tile_rows, kv_dev, head_size)
    score_scale = head_size ** (-0.5)
    query_gradient = (acc_query * score_scale).reshape(window, kv_dev, query_width)
    key_gradient = (acc_key * score_scale).reshape(window, kv_dev, head_size)
    value_gradient = acc_value.reshape(window, kv_dev, head_size)
    stacked_gradients = (
        jnp.concatenate([query_gradient, key_gradient, value_gradient], axis=2)
        .astype(jnp.bfloat16)
        .reshape(window, -1)
    )
    weight_piece = lax.all_gather(query_key_value_weight, "tok", axis=0, tiled=True)
    flat_piece = weight_piece.reshape(weight_piece.shape[0], -1)
    partial_sum = lax.dot_general(
        stacked_gradients, flat_piece, (((1,), (1,)), ((), ())), preferred_element_type=jnp.float32
    )
    summed = lax.psum_scatter(
        partial_sum.astype(jnp.bfloat16), "head", scatter_dimension=1, tiled=True
    )
    return summed


MESH = pl.DeviceIdType.MESH
LANES = 128
PIECE = 32


def fused_kernel(
    sides,
    q_hbm,
    k_hbm,
    v_hbm,
    do_hbm,
    lse_hbm,
    delta_hbm,
    seg_hbm,
    w_hbm,
    out_ref,
    q_ref,
    k_ref,
    v_ref,
    do_ref,
    lse_ref,
    delta_ref,
    seg_ref,
    joined,
    w_all,
    keep,
    part_out,
    part_in,
    x_out,
    x_in,
    back_out,
    direct_out,
    direct_in,
    bias,
    lse32,
    delta32,
    dk_acc,
    dv_acc,
    load_sem,
    own_send,
    own_recv,
    far_send,
    far_recv,
    relay_send,
    relay_recv,
    j_send,
    j_recv,
    part_send,
    part_recv,
    x_send,
    x_recv,
    back_send,
    back_recv,
    small_part_send,
    small_part_recv,
    small_x_send,
    small_x_recv,
    small_back_send,
    small_back_recv,
    direct_send,
    direct_recv,
):
    window, head_size = k_ref.shape
    groups = q_ref.shape[1] // head_size
    rows = w_hbm.shape[0]
    chunks, pieces = rows // LANES, rows // PIECE
    per = LANES // PIECE
    block = window // chunks
    columns = groups + 2
    tok, h = lax.axis_index("tok"), lax.axis_index("head")
    z, y = tok // sides, tok % sides
    x, c = h // sides, h % sides
    yo, xo, co = 1 - y, 1 - x, 1 - c
    odd, upper = z % sides, z // sides
    partner = z + 1 - 2 * odd
    far = z + sides - 2 * sides * upper
    middle = upper != odd
    ends = jnp.logical_not(middle)
    mine = jnp.where(c == odd, 0, 1)
    final = jnp.where(x == upper, 0, 1)

    def device(dz, dy, dx, dc):
        return (dz * sides + dy, dx * sides + dc)

    y_peer = device(z, yo, x, c)
    far_peer = device(far, y, x, c)
    j_peer = device(partner, y, x, c)
    core_peer = device(z, y, x, co)
    x_peer = device(z, y, xo, c)
    back_peer = device(partner, y, x, co)

    loads = [
        pltpu.make_async_copy(src, dst, load_sem.at[i])
        for i, (src, dst) in enumerate(
            (
                (seg_hbm, seg_ref),
                (lse_hbm, lse_ref),
                (delta_hbm, delta_ref),
                (k_hbm, k_ref),
                (v_hbm, v_ref),
                (q_hbm.at[:, :head_size], q_ref.at[:, :head_size]),
                (do_hbm.at[:, :head_size], do_ref.at[:, :head_size]),
                (q_hbm.at[:, head_size:], q_ref.at[:, head_size:]),
                (do_hbm.at[:, head_size:], do_ref.at[:, head_size:]),
                (w_hbm, w_all.at[0, y]),
            )
        )
    ]
    barrier = pltpu.get_barrier_semaphore()
    cross_peer = device(partner, y, xo, co)
    peers = (y_peer, far_peer, j_peer, core_peer, x_peer, back_peer, cross_peer)
    for peer in peers:
        pl.semaphore_signal(barrier, inc=1, device_id=peer, device_id_type=MESH)

    def j_cols(r):
        return pl.ds(pl.multiple_of(r * head_size, head_size), head_size)

    scale = head_size ** (-0.5)
    half = window // 2

    def dot(a, b, da, db):
        return lax.dot_general(a, b, (((da,), (db,)), ((), ())), preferred_element_type=jnp.float32)

    def head(r):
        cols = j_cols(r)
        sums = []
        for start in (0, half):
            keys, queries = slice(start, start + half), slice(start, window)
            q, do = q_ref[queries, cols], do_ref[queries, cols]
            kk, vv = k_ref[keys, :], v_ref[keys, :]
            logits = dot(kk, q, 1, 1) * scale - lse32[pl.ds(r, 1), queries]
            probs = jnp.exp(logits + bias[keys, queries])
            dv_acc[keys, :] += dot(probs.astype(jnp.bfloat16), do, 1, 0)
            grad_prob = dot(vv, do, 1, 1)
            ds = (probs * (grad_prob - delta32[pl.ds(r, 1), queries])).astype(jnp.bfloat16)
            dk_acc[keys, :] += dot(ds, q, 1, 0)
            sums.append(dot(ds, kk, 0, 0))
        low = sums[0]
        joined[0, :half, cols] = (low[:half] * scale).astype(jnp.bfloat16)
        joined[0, half:, cols] = ((low[half:] + sums[1]) * scale).astype(jnp.bfloat16)

    def remote(src, dst, send, recv, peer):
        return pltpu.make_async_remote_copy(
            src_ref=src,
            dst_ref=dst,
            send_sem=send,
            recv_sem=recv,
            device_id=peer,
            device_id_type=MESH,
        )

    def piece_rows(p):
        return pl.ds(pl.multiple_of(p * PIECE, PIECE), PIECE)

    def chunk_rows(k):
        return pl.ds(pl.multiple_of(k * LANES, LANES), LANES)

    def block_rows(i):
        return pl.ds(pl.multiple_of(i * block, block), block)

    def own_copy(k):
        return remote(
            w_hbm.at[chunk_rows(k)],
            w_all.at[0, y, chunk_rows(k)],
            own_send.at[k],
            own_recv.at[k],
            y_peer,
        )

    def arrived_own(k):
        ref = w_all.at[0, yo, chunk_rows(k)]
        remote(ref, ref, own_send.at[k], own_recv.at[k], y_peer).wait_recv()

    def far_copy(p, part):
        return remote(
            w_hbm.at[part(p)],
            w_all.at[1, y, part(p)],
            far_send.at[p],
            far_recv.at[p],
            far_peer,
        )

    def relay_copy(p, part):
        ref = w_all.at[1, y, part(p)]
        return remote(ref, ref, relay_send.at[p], relay_recv.at[p], y_peer)

    def arrived_far(p, part):
        ref = w_all.at[1, y, part(p)]
        remote(ref, ref, far_send.at[p], far_recv.at[p], far_peer).wait_recv()

    def arrived_relay(p, part):
        ref = w_all.at[1, yo, part(p)]
        remote(ref, ref, relay_send.at[p], relay_recv.at[p], y_peer).wait_recv()

    def j_copy(r):
        return remote(
            joined.at[0, :, j_cols(r)],
            joined.at[1, :, j_cols(r)],
            j_send.at[r],
            j_recv.at[r],
            j_peer,
        )

    def j_block(i):
        return remote(
            joined.at[0, block_rows(i)],
            joined.at[1, block_rows(i)],
            j_send.at[i],
            j_recv.at[i],
            j_peer,
        )

    def each(count, body):
        lax.fori_loop(0, count, lambda i, carry: (body(i), carry)[1], 0)

    def enter():
        pl.semaphore_wait(barrier, len(peers))

    def load_all():
        for load in loads:
            load.start()

    @pl.when(middle)
    def _():
        load_all()

    @pl.when(ends)
    def _():
        enter()

        def both(k):
            far_copy(k, chunk_rows).start()
            own_copy(k).start()

        each(chunks, both)
        load_all()

    for load in loads[:3]:
        load.wait()
    lse32[...] = lse_ref[...].astype(jnp.float32)
    delta32[...] = delta_ref[...].astype(jnp.float32)
    seg_row = seg_ref[:, pl.ds(pl.multiple_of(tok * window, LANES), window)].astype(jnp.float32)
    seg_col = jnp.transpose(jnp.broadcast_to(seg_row, (LANES, window)))[:, :1]
    key_id = lax.broadcasted_iota(jnp.int32, (window, window), 0)
    query_id = lax.broadcasted_iota(jnp.int32, (window, window), 1)
    bias[...] = jnp.where((seg_col == seg_row) & (key_id <= query_id), 0.0, -1e30)
    dk_acc[...] = jnp.zeros_like(dk_acc)
    dv_acc[...] = jnp.zeros_like(dv_acc)
    for load in loads[3:7]:
        load.wait()

    @pl.when(middle)
    def _():
        head(0)
        enter()
        j_copy(0).start()
        each(chunks, lambda k: own_copy(k).start())

    for load in loads[7:9]:
        load.wait()

    @pl.loop(jnp.where(middle, 1, 0), groups)
    def _(r):
        head(r)

        @pl.when(middle)
        def _():
            j_copy(r).start()

    wide = groups * head_size
    joined[0, :, wide : wide + head_size] = (dk_acc[...] * scale).astype(jnp.bfloat16)
    joined[0, :, wide + head_size : wide + 2 * head_size] = dv_acc[...].astype(jnp.bfloat16)
    loads[9].wait()

    def tile(ref, lead, i, by_token):
        return ref.at[(*lead, slice(None), block_rows(i))] if by_token else ref.at[(*lead, i)]

    def part_copy(slot, yr, i, by_token):
        return remote(
            tile(part_out, (slot, yr), i, by_token),
            tile(part_in, (slot, yr), i, by_token),
            part_send.at[slot, yr, i],
            part_recv.at[slot, yr, i],
            core_peer,
        )

    def x_copy(yr, i, by_token):
        return remote(
            tile(x_out, (yr,), i, by_token),
            tile(x_in, (yr,), i, by_token),
            x_send.at[yr, i],
            x_recv.at[yr, i],
            x_peer,
        )

    def out_cols(yr, k):
        return pl.ds(pl.multiple_of(yr * rows + k * LANES, LANES), LANES)

    def out_tile(ref, yr, i, by_token):
        if by_token:
            return ref.at[block_rows(i), pl.ds(pl.multiple_of(yr * rows, LANES), rows)]
        return ref.at[:, out_cols(yr, i)]

    def back_copy(yr, i, by_token):
        return remote(
            out_tile(back_out, yr, i, by_token),
            out_tile(out_ref, yr, i, by_token),
            back_send.at[yr, i],
            back_recv.at[yr, i],
            back_peer,
        )

    def unit(slot, yr, k, side):
        value = dot(joined[side], w_all[slot, yr, chunk_rows(k)], 1, 1)

        @pl.when(mine == side)
        def _():
            keep[slot, yr, k] = value

        @pl.when(mine != side)
        def _():
            part_out[slot, yr, k] = value.astype(jnp.bfloat16)
            part_copy(slot, yr, k, False).start()

    def block_unit(slot, yr, i):
        value = dot(joined[1, block_rows(i)], w_all[slot, yr], 1, 1)

        @pl.when(mine == 1)
        def _():
            for k in range(chunks):
                keep[slot, yr, k, block_rows(i)] = value[:, k * LANES : (k + 1) * LANES]

        @pl.when(mine == 0)
        def _():
            low = value.astype(jnp.bfloat16)
            for k in range(chunks):
                part_out[slot, yr, k, block_rows(i)] = low[:, k * LANES : (k + 1) * LANES]
            part_copy(slot, yr, i, True).start()

    def small(ref, lead, a, b):
        return ref.at[(*lead, b, block_rows(a))]

    def small_part(a, b):
        return remote(
            small(part_out, (1, yo), a, b),
            small(part_in, (1, yo), a, b),
            small_part_send.at[a, b],
            small_part_recv.at[a, b],
            core_peer,
        )

    def small_x(a, b):
        return remote(
            small(x_out, (yo,), a, b),
            small(x_in, (yo,), a, b),
            small_x_send.at[a, b],
            small_x_recv.at[a, b],
            x_peer,
        )

    def small_back(a, b):
        return remote(
            back_out.at[block_rows(a), out_cols(yo, b)],
            out_ref.at[block_rows(a), out_cols(yo, b)],
            small_back_send.at[a, b],
            small_back_recv.at[a, b],
            back_peer,
        )

    def small_unit(a, b):
        value = dot(joined[1, block_rows(a)], w_all[1, yo, chunk_rows(b)], 1, 1)

        @pl.when(mine == 1)
        def _():
            keep[1, yo, b, block_rows(a)] = value

        @pl.when(mine == 0)
        def _():
            part_out[1, yo, b, block_rows(a)] = value.astype(jnp.bfloat16)
            small_part(a, b).start()

    def small_core_sum(a, b):
        small_part(a, b).wait_recv()
        kept = small(keep, (1, yo), a, b)
        value = kept[...] + small(part_in, (1, yo), a, b)[...].astype(jnp.float32)

        @pl.when(final == 1)
        def _():
            kept[...] = value

        @pl.when(final == 0)
        def _():
            small(x_out, (yo,), a, b)[...] = value.astype(jnp.bfloat16)
            small_x(a, b).start()

    def small_x_sum(a, b):
        small_x(a, b).wait_recv()
        value = small(keep, (1, yo), a, b)[...] + small(x_in, (yo,), a, b)[...].astype(jnp.float32)
        back_out[block_rows(a), out_cols(yo, b)] = value.astype(jnp.bfloat16)
        small_back(a, b).start()

    end = chunks - 1

    def direct_copy(source, peer):
        return remote(direct_out, direct_in.at[source], direct_send, direct_recv.at[source], peer)

    def direct_sum():
        part_copy(1, yo, end, False).wait_recv()
        value = keep[1, yo, end] + part_in[1, yo, end].astype(jnp.float32)
        direct_out[...] = value.astype(jnp.bfloat16)

        @pl.when(final == 1)
        def _():
            direct_copy(0, back_peer).start()

        @pl.when(final == 0)
        def _():
            direct_copy(1, cross_peer).start()

    def relayed_sum(k):
        whole = (k == end) & (mine == 1)

        @pl.when(whole)
        def _():
            direct_sum()

        @pl.when(jnp.logical_not(whole))
        def _():
            core_sum(1, yo, k, False)

    def relayed_x_sum(k):
        @pl.when((final == 1) & ((k < end) | (mine == 0)))
        def _():
            x_sum(yo, k, False)

    def added(step, body):
        def one(j):
            body(jnp.minimum(j, step), jnp.where(j <= step, step, j - step - 1))

        each(2 * step + 1, one)

    def all_small(body):
        each(chunks * chunks, lambda j: body(j // chunks, j % chunks))

    def core_sum(slot, yr, i, by_token):
        part_copy(slot, yr, i, by_token).wait_recv()
        kept = tile(keep, (slot, yr), i, by_token)
        value = kept[...] + tile(part_in, (slot, yr), i, by_token)[...].astype(jnp.float32)

        @pl.when(slot == final)
        def _():
            kept[...] = value

        @pl.when(slot != final)
        def _():
            tile(x_out, (yr,), i, by_token)[...] = value.astype(jnp.bfloat16)
            x_copy(yr, i, by_token).start()

    def x_sum(yr, i, by_token):
        x_copy(yr, i, by_token).wait_recv()
        value = tile(keep, (final, yr), i, by_token)[...]
        value += tile(x_in, (yr,), i, by_token)[...].astype(jnp.float32)
        value = value.astype(jnp.bfloat16)

        def put(ref):
            if by_token:
                for k in range(chunks):
                    ref[block_rows(i), out_cols(yr, k)] = value[k]
            else:
                ref[:, out_cols(yr, i)] = value

        if by_token:
            put(back_out)
            back_copy(yr, i, True).start()
        else:

            @pl.when(mine == 0)
            def _():
                put(out_ref)

            @pl.when(mine == 1)
            def _():
                put(back_out)
                back_copy(yr, i, False).start()

    def which(i):
        return jnp.where(i // chunks % 2 == 0, y, yo)

    lag, turns = 2, 4

    @pl.when(middle)
    def _():
        j_copy(groups).start()
        j_copy(groups + 1).start()
        each(pieces, lambda p: far_copy(p, piece_rows).start())
        steps = 3 * chunks

        @pl.loop(0, steps + lag)
        def _(i):
            k = i % chunks

            @pl.when((i >= chunks) & (i < 2 * chunks))
            def _():
                arrived_far(k, chunk_rows)
                relay_copy(k, chunk_rows).start()
                arrived_own(k)

            @pl.when(i < steps)
            def _():
                unit(i // (2 * chunks), which(i), k, 0)

            @pl.when((i >= lag) & (mine == 0))
            def _():
                core_sum((i - lag) // (2 * chunks), which(i - lag), (i - lag) % chunks, False)

        @pl.loop(0, chunks + 1)
        def _(i):
            live = i < chunks

            def partner_sum(slot, yr):
                @pl.when(live & (mine == 1))
                def _():
                    core_sum(slot, yr, i, True)

            @pl.when(live)
            def _():
                j_block(i).wait_recv()

            @pl.when(live)
            def _():
                block_unit(1, y, i)

            @pl.when(live)
            def _():
                block_unit(0, y, i)

            @pl.when(live)
            def _():
                block_unit(0, yo, i)

            partner_sum(1, y)
            partner_sum(0, y)
            @pl.when((i >= 1) & (mine == 1))
            def _():
                x_sum(y, i - 1, True)

                @pl.when(final == 0)
                def _():
                    x_sum(yo, i - 1, True)

                @pl.when(final == 1)
                def _():
                    added(i - 1, small_x_sum)

            partner_sum(0, yo)
            @pl.when(live)
            def _():
                arrived_relay(i, chunk_rows)

            @pl.when(live)
            def _():
                added(i, small_unit)

            @pl.when(live & (mine == 1))
            def _():
                added(i, small_core_sum)

            @pl.when(live)
            def _():
                unit(1, yo, i, 0)

            @pl.when(mine == 0)
            def _():
                @pl.when(i >= 1)
                def _():
                    x_sum(yo, i - 1, False)

                @pl.when(live)
                def _():
                    core_sum(1, yo, i, False)
                    x_sum(y, i, False)

    @pl.when(ends)
    def _():
        each(chunks, lambda b: j_block(b).start())

        @pl.loop(0, 2 * chunks + lag)
        def _(i):
            k = i % chunks

            @pl.when((i >= chunks) & (i < 2 * chunks))
            def _():
                arrived_own(k)


            @pl.when(i < 2 * chunks)
            def _():
                unit(0, which(i), k, 0)

            @pl.when((i >= lag) & (mine == 0))
            def _():
                core_sum(0, which(i - lag), (i - lag) % chunks, False)

        each(columns, lambda r: j_copy(r).wait_recv())

        @pl.loop(0, chunks + 2)
        def _(k):
            for i in range(turns):

                @pl.when(k < chunks)
                def _():
                    for j in range(per // turns):
                        p = k * per + i * (per // turns) + j
                        arrived_far(p, piece_rows)
                        relay_copy(p, piece_rows).start()

                @pl.when(k == 0)
                def _():
                    for j in range(i * 2 * chunks // turns, (i + 1) * 2 * chunks // turns):
                        unit(0, which(j), j % chunks, 1)

                @pl.when((k == 1) & (mine == 1))
                def _():
                    for j in range(i * 2 * chunks // turns, (i + 1) * 2 * chunks // turns):
                        core_sum(0, which(j), j % chunks, False)

                @pl.when((k >= 1) & (k <= chunks))
                def _():
                    if i == 0:
                        unit(1, y, k - 1, 1)
                        unit(1, y, k - 1, 0)
                    if i == 1:
                        core_sum(1, y, k - 1, False)
                    if i == 2:
                        for j in range(per):
                            arrived_relay((k - 1) * per + j, piece_rows)
                        unit(1, yo, k - 1, 1)
                        unit(1, yo, k - 1, 0)
                    if i == 3:
                        relayed_sum(k - 1)

                        @pl.when(final == 1)
                        def _():
                            x_sum(y, k - 1, False)

                @pl.when(k >= 2)
                def _():
                    if i == 0:
                        relayed_x_sum(k - 2)

                    @pl.when((final == 0) & (k < chunks))
                    def _():
                        if i < 2:
                            x_sum((y, yo)[i], 2 * k - 4, False)
                            x_sum((y, yo)[i], 2 * k - 3, False)


    def tiles(condition, copies, wait, count=chunks):
        @pl.when(condition)
        def _():
            each(count, lambda i: wait(copies(i)))

    def smalls(condition, copies, wait):
        @pl.when(condition)
        def _():
            all_small(lambda a, b: wait(copies(a, b)))

    def received(copy):
        copy.wait_recv()

    def sent(copy):
        copy.wait_send()

    back = mine == 1
    count_in = jnp.where(middle & (final == 1), end, chunks)
    count_out = jnp.where(ends & (final == 1), end, chunks)
    count_x = jnp.where(ends & back & (final == 0), end, chunks)
    tiles(back, lambda i: back_copy(y, i, False), received)
    tiles(back & (middle | (final == 0)), lambda i: back_copy(yo, i, False), received, count_in)
    smalls(back & ends & (final == 1), small_back, received)

    @pl.when(back & middle & (final == 1))
    def _():
        direct_copy(0, back_peer).wait_recv()
        direct_copy(1, back_peer).wait_recv()
        value = direct_in[0].astype(jnp.float32) + direct_in[1].astype(jnp.float32)
        out_ref[:, out_cols(yo, end)] = value.astype(jnp.bfloat16)

    @pl.when(back & ends)
    def _():
        direct_copy(0, back_peer).wait_send()

    tiles(back, lambda i: back_copy(y, i, False), sent)
    tiles(back & (ends | (final == 0)), lambda i: back_copy(yo, i, False), sent, count_out)
    smalls(back & middle & (final == 1), small_back, sent)
    by_small = middle & (final == 0) & (mine == 1)
    tiles(jnp.logical_not(by_small), lambda i: x_copy(yo, i, False), sent, count_x)
    tiles(True, lambda i: x_copy(y, i, False), sent)
    smalls(by_small, small_x, sent)
    by_small = middle & (mine == 0)
    tiles(jnp.logical_not(by_small), lambda i: part_copy(1, yo, i, False), sent)
    smalls(by_small, small_part, sent)

    @pl.loop(0, chunks)
    def _(i):
        part_copy(0, y, i, False).wait_send()
        part_copy(0, yo, i, False).wait_send()
        part_copy(1, y, i, False).wait_send()

    each(chunks, lambda k: own_copy(k).wait_send())

    @pl.when(middle)
    def _():
        each(pieces, lambda p: far_copy(p, piece_rows).wait_send())
        each(chunks, lambda k: relay_copy(k, chunk_rows).wait_send())

    @pl.when(ends)
    def _():
        each(chunks, lambda k: far_copy(k, chunk_rows).wait_send())
        each(pieces, lambda p: relay_copy(p, piece_rows).wait_send())

    @pl.when(middle)
    def _():
        each(columns, lambda r: j_copy(r).wait_send())

    @pl.when(ends)
    def _():
        each(chunks, lambda i: j_block(i).wait_send())


def fused(sides, q, k, v, do, lse, delta, segments, weight):
    window, _, query_width = q.shape
    head_size = k.shape[2]
    rows, _, width = weight.shape
    chunks, pieces = rows // LANES, rows // PIECE
    columns = width // head_size
    bf16, f32 = jnp.bfloat16, jnp.float32
    dma = pltpu.SemaphoreType.DMA
    vmem = pl.BlockSpec(memory_space=pltpu.VMEM)
    hbm = pl.BlockSpec(memory_space=pl.ANY)
    tile = (window, LANES)
    return pl.pallas_call(
        functools.partial(fused_kernel, sides),
        out_shape=jax.ShapeDtypeStruct((window, 2 * rows), bf16),
        in_specs=[hbm] * 8,
        out_specs=vmem,
        scratch_shapes=[
            pltpu.VMEM((window, query_width), bf16),
            pltpu.VMEM((window, head_size), bf16),
            pltpu.VMEM((window, head_size), bf16),
            pltpu.VMEM((window, query_width), bf16),
            pltpu.VMEM(lse.shape[1:], bf16),
            pltpu.VMEM(lse.shape[1:], bf16),
            pltpu.VMEM((1,) + segments.shape, segments.dtype),
            pltpu.VMEM((2, window, width), bf16),
            pltpu.VMEM((2, 2, rows, width), bf16),
            pltpu.VMEM((2, 2, chunks) + tile, f32),
            pltpu.VMEM((2, 2, chunks) + tile, bf16),
            pltpu.VMEM((2, 2, chunks) + tile, bf16),
            pltpu.VMEM((2, chunks) + tile, bf16),
            pltpu.VMEM((2, chunks) + tile, bf16),
            pltpu.VMEM((window, 2 * rows), bf16),
            pltpu.VMEM(tile, bf16),
            pltpu.VMEM((2,) + tile, bf16),
            pltpu.VMEM((window, window), f32),
            pltpu.VMEM(lse.shape[1:], f32),
            pltpu.VMEM(lse.shape[1:], f32),
            pltpu.VMEM((window, head_size), f32),
            pltpu.VMEM((window, head_size), f32),
            dma((10,)),
            dma((pieces,)),
            dma((pieces,)),
            dma((pieces,)),
            dma((pieces,)),
            dma((pieces,)),
            dma((pieces,)),
            dma((columns,)),
            dma((columns,)),
            dma((2, 2, chunks)),
            dma((2, 2, chunks)),
            dma((2, chunks)),
            dma((2, chunks)),
            dma((2, chunks)),
            dma((2, chunks)),
            *[dma((chunks, chunks))] * 6,
            dma,
            dma((2,)),
        ],
        compiler_params=pltpu.CompilerParams(
            collective_id=0, has_side_effects=True, vmem_limit_bytes=40 * 1024 * 1024
        ),
    )(
        *(
            pltpu.with_memory_space_constraint(array, pltpu.HBM)
            for array in (
                q.reshape(window, query_width),
                k.reshape(window, head_size),
                v.reshape(window, head_size),
                do.reshape(window, query_width),
                lse.reshape(lse.shape[1:]),
                delta.reshape(delta.shape[1:]),
                segments.reshape(1, -1),
                weight.reshape(rows, width),
            )
        )
    )


def solution(mesh):
    placed = (
        P("tok", "head", None),
        P("tok", "head", None),
        P("tok", "head", None),
        P("tok", "head", None),
        P("head", None, "tok"),
        P("head", None, "tok"),
        P(),
        P("tok", "head", None),
    )
    tok, heads = mesh.shape["tok"], mesh.shape["head"]
    sides = tok // heads

    def step(*args):
        window, kv_dev, _ = args[0].shape
        rows = args[7].shape[0]
        paired = sides == 2 and heads == sides * sides and tok == heads * sides and kv_dev == 1
        if paired and rows == heads * LANES and window == rows and args[1].shape[2] == LANES:
            return fused(sides, *args)
        return on_device(*args)

    return jax.shard_map(
        step, mesh=mesh, in_specs=placed, out_specs=P("tok", "head"), check_vma=False
    )
```

```python
import functools

import jax
import jax.numpy as jnp
import numpy as np
from jax import lax
from jax.experimental import pallas as pl
from jax.experimental.pallas import tpu as pltpu
from jax.sharding import PartitionSpec as P

BLOCK = 128


def pair_lists(block_count):
    query_list = []
    key_list = []
    for query_block in range(block_count):
        for key_block in range(query_block + 1):
            query_list.append(query_block)
            key_list.append(key_block)
    return (np.array(query_list, np.int32), np.array(key_list, np.int32))


def live_pairs(seg_window, query_list, key_list, tile_rows):
    first_seg = jnp.take(seg_window, query_list * tile_rows)
    last_seg = jnp.take(seg_window, key_list * tile_rows + tile_rows - 1)
    return (first_seg == last_seg) | jnp.asarray(query_list == key_list)


def pair_grads(query_tile, dout_tile, key_tile, value_tile, lse_tile, delta_tile, allowed):
    tile_rows, groups, query_width = query_tile.shape
    head_size = key_tile.shape[2]
    heads_per_group = query_width // head_size
    query_heads = query_tile.reshape(tile_rows, groups, heads_per_group, head_size)
    dout_heads = dout_tile.reshape(tile_rows, groups, heads_per_group, head_size)
    scores = jnp.einsum(
        "agrd,bgd->grab", query_heads, key_tile, preferred_element_type=jnp.float32
    ) * head_size ** (-0.5)
    logits = scores - lse_tile.astype(jnp.float32)[:, :, :, None]
    soft_probs = jnp.where(allowed[None, None], jnp.exp(logits), 0.0)
    probs_low = soft_probs.astype(jnp.bfloat16)
    value_gradient = jnp.einsum(
        "grab,agrd->bgd", probs_low, dout_heads, preferred_element_type=jnp.float32
    )
    grad_prob = jnp.einsum(
        "agrd,bgd->grab", dout_heads, value_tile, preferred_element_type=jnp.float32
    )
    grad_score = (soft_probs * (grad_prob - delta_tile.astype(jnp.float32)[:, :, :, None])).astype(
        jnp.bfloat16
    )
    query_gradient = jnp.einsum(
        "grab,bgd->agrd", grad_score, key_tile, preferred_element_type=jnp.float32
    )
    key_gradient = jnp.einsum(
        "grab,agrd->bgd", grad_score, query_heads, preferred_element_type=jnp.float32
    )
    return (query_gradient.reshape(tile_rows, groups, query_width), key_gradient, value_gradient)


def on_device(
    query_rows,
    key_rows,
    value_rows,
    output_gradient,
    row_logsumexp,
    row_delta_sums,
    segments,
    query_key_value_weight,
):
    window, kv_dev, query_width = query_rows.shape
    head_size = key_rows.shape[2]
    tile_rows = BLOCK
    block_count = window // tile_rows
    query_list, key_list = pair_lists(block_count)
    query_table = jnp.asarray(query_list)
    key_table = jnp.asarray(key_list)
    myself = lax.axis_index("tok")
    own_seg = lax.dynamic_slice_in_dim(segments, myself * window, window)
    own_live = live_pairs(own_seg, query_list, key_list, tile_rows)
    block_ids = jnp.arange(block_count, dtype=jnp.int32)
    query_match = (query_table[:, None] == block_ids[None, :]) & own_live[:, None]
    key_match = key_table[:, None] == block_ids[None, :]
    block_local = jnp.any(query_match[:, :, None] & key_match[:, None, :], axis=0)
    token_local = jnp.repeat(jnp.repeat(block_local, tile_rows, axis=0), tile_rows, axis=1)
    offsets = jnp.arange(window, dtype=jnp.int32)
    allowed_all = (
        (own_seg[:, None] == own_seg[None, :])
        & (offsets[None, :] <= offsets[:, None])
        & token_local
    )
    local_out = pair_grads(
        query_rows,
        output_gradient,
        key_rows,
        value_rows,
        row_logsumexp,
        row_delta_sums,
        allowed_all,
    )
    acc_query = local_out[0].reshape(block_count, tile_rows, kv_dev, query_width)
    acc_key = local_out[1].reshape(block_count, tile_rows, kv_dev, head_size)
    acc_value = local_out[2].reshape(block_count, tile_rows, kv_dev, head_size)
    score_scale = head_size ** (-0.5)
    query_gradient = (acc_query * score_scale).reshape(window, kv_dev, query_width)
    key_gradient = (acc_key * score_scale).reshape(window, kv_dev, head_size)
    value_gradient = acc_value.reshape(window, kv_dev, head_size)
    stacked_gradients = (
        jnp.concatenate([query_gradient, key_gradient, value_gradient], axis=2)
        .astype(jnp.bfloat16)
        .reshape(window, -1)
    )
    weight_piece = lax.all_gather(query_key_value_weight, "tok", axis=0, tiled=True)
    flat_piece = weight_piece.reshape(weight_piece.shape[0], -1)
    partial_sum = lax.dot_general(
        stacked_gradients, flat_piece, (((1,), (1,)), ((), ())), preferred_element_type=jnp.float32
    )
    summed = lax.psum_scatter(
        partial_sum.astype(jnp.bfloat16), "head", scatter_dimension=1, tiled=True
    )
    return summed


MESH = pl.DeviceIdType.MESH
LANES = 128
PIECE = 32


def fused_kernel(
    sides,
    q_hbm,
    k_hbm,
    v_hbm,
    do_hbm,
    lse_hbm,
    delta_hbm,
    seg_hbm,
    w_hbm,
    out_ref,
    q_ref,
    k_ref,
    v_ref,
    do_ref,
    lse_ref,
    delta_ref,
    seg_ref,
    joined,
    w_all,
    keep,
    part_out,
    part_in,
    x_out,
    x_in,
    back_out,
    direct_out,
    direct_in,
    bias,
    lse32,
    delta32,
    dk_acc,
    dv_acc,
    load_sem,
    own_send,
    own_recv,
    far_send,
    far_recv,
    relay_send,
    relay_recv,
    j_send,
    j_recv,
    part_send,
    part_recv,
    x_send,
    x_recv,
    back_send,
    back_recv,
    small_part_send,
    small_part_recv,
    small_x_send,
    small_x_recv,
    small_back_send,
    small_back_recv,
    direct_send,
    direct_recv,
):
    window, head_size = k_ref.shape
    groups = q_ref.shape[1] // head_size
    rows = w_hbm.shape[0]
    chunks, pieces = rows // LANES, rows // PIECE
    per = LANES // PIECE
    block = window // chunks
    columns = groups + 2
    tok, h = lax.axis_index("tok"), lax.axis_index("head")
    z, y = tok // sides, tok % sides
    x, c = h // sides, h % sides
    yo, xo, co = 1 - y, 1 - x, 1 - c
    odd, upper = z % sides, z // sides
    partner = z + 1 - 2 * odd
    far = z + sides - 2 * sides * upper
    middle = upper != odd
    ends = jnp.logical_not(middle)
    mine = jnp.where(c == odd, 0, 1)
    final = jnp.where(x == upper, 0, 1)

    def device(dz, dy, dx, dc):
        return (dz * sides + dy, dx * sides + dc)

    y_peer = device(z, yo, x, c)
    far_peer = device(far, y, x, c)
    j_peer = device(partner, y, x, c)
    core_peer = device(z, y, x, co)
    x_peer = device(z, y, xo, c)
    back_peer = device(partner, y, x, co)

    loads = [
        pltpu.make_async_copy(src, dst, load_sem.at[i])
        for i, (src, dst) in enumerate(
            (
                (seg_hbm, seg_ref),
                (lse_hbm, lse_ref),
                (delta_hbm, delta_ref),
                (k_hbm, k_ref),
                (v_hbm, v_ref),
                (q_hbm.at[:, :head_size], q_ref.at[:, :head_size]),
                (do_hbm.at[:, :head_size], do_ref.at[:, :head_size]),
                (q_hbm.at[:, head_size:], q_ref.at[:, head_size:]),
                (do_hbm.at[:, head_size:], do_ref.at[:, head_size:]),
                (w_hbm, w_all.at[0, y]),
            )
        )
    ]
    barrier = pltpu.get_barrier_semaphore()
    cross_peer = device(partner, y, xo, co)
    peers = (y_peer, far_peer, j_peer, core_peer, x_peer, back_peer, cross_peer)
    for peer in peers:
        pl.semaphore_signal(barrier, inc=1, device_id=peer, device_id_type=MESH)

    def j_cols(r):
        return pl.ds(pl.multiple_of(r * head_size, head_size), head_size)

    scale = head_size ** (-0.5)
    half = window // 2

    def dot(a, b, da, db):
        return lax.dot_general(a, b, (((da,), (db,)), ((), ())), preferred_element_type=jnp.float32)

    def head(r):
        cols = j_cols(r)
        sums = []
        for start in (0, half):
            keys, queries = slice(start, start + half), slice(start, window)
            q, do = q_ref[queries, cols], do_ref[queries, cols]
            kk, vv = k_ref[keys, :], v_ref[keys, :]
            logits = dot(kk, q, 1, 1) * scale - lse32[pl.ds(r, 1), queries]
            probs = jnp.exp(logits + bias[keys, queries])
            dv_acc[keys, :] += dot(probs.astype(jnp.bfloat16), do, 1, 0)
            grad_prob = dot(vv, do, 1, 1)
            ds = (probs * (grad_prob - delta32[pl.ds(r, 1), queries])).astype(jnp.bfloat16)
            dk_acc[keys, :] += dot(ds, q, 1, 0)
            sums.append(dot(ds, kk, 0, 0))
        low = sums[0]
        joined[0, :half, cols] = (low[:half] * scale).astype(jnp.bfloat16)
        joined[0, half:, cols] = ((low[half:] + sums[1]) * scale).astype(jnp.bfloat16)

    def remote(src, dst, send, recv, peer):
        return pltpu.make_async_remote_copy(
            src_ref=src,
            dst_ref=dst,
            send_sem=send,
            recv_sem=recv,
            device_id=peer,
            device_id_type=MESH,
        )

    def piece_rows(p):
        return pl.ds(pl.multiple_of(p * PIECE, PIECE), PIECE)

    def chunk_rows(k):
        return pl.ds(pl.multiple_of(k * LANES, LANES), LANES)

    def block_rows(i):
        return pl.ds(pl.multiple_of(i * block, block), block)

    def own_copy(k):
        return remote(
            w_hbm.at[chunk_rows(k)],
            w_all.at[0, y, chunk_rows(k)],
            own_send.at[k],
            own_recv.at[k],
            y_peer,
        )

    def arrived_own(k):
        ref = w_all.at[0, yo, chunk_rows(k)]
        remote(ref, ref, own_send.at[k], own_recv.at[k], y_peer).wait_recv()

    def far_copy(p, part):
        return remote(
            w_hbm.at[part(p)],
            w_all.at[1, y, part(p)],
            far_send.at[p],
            far_recv.at[p],
            far_peer,
        )

    def relay_copy(p, part):
        ref = w_all.at[1, y, part(p)]
        return remote(ref, ref, relay_send.at[p], relay_recv.at[p], y_peer)

    def arrived_far(p, part):
        ref = w_all.at[1, y, part(p)]
        remote(ref, ref, far_send.at[p], far_recv.at[p], far_peer).wait_recv()

    def arrived_relay(p, part):
        ref = w_all.at[1, yo, part(p)]
        remote(ref, ref, relay_send.at[p], relay_recv.at[p], y_peer).wait_recv()

    def j_copy(r):
        return remote(
            joined.at[0, :, j_cols(r)],
            joined.at[1, :, j_cols(r)],
            j_send.at[r],
            j_recv.at[r],
            j_peer,
        )

    def j_pair(r):
        cols = pl.ds(pl.multiple_of(r * head_size, head_size), 2 * head_size)
        return remote(
            joined.at[0, :, cols], joined.at[1, :, cols], j_send.at[r], j_recv.at[r], j_peer
        )

    def all_j(wait):
        wait(j_copy(0))
        each((columns - 2) // 2, lambda i: wait(j_pair(2 * i + 1)))
        wait(j_copy(columns - 1))

    def j_block(i):
        return remote(
            joined.at[0, block_rows(i)],
            joined.at[1, block_rows(i)],
            j_send.at[i],
            j_recv.at[i],
            j_peer,
        )

    def each(count, body):
        lax.fori_loop(0, count, lambda i, carry: (body(i), carry)[1], 0)

    def enter():
        pl.semaphore_wait(barrier, len(peers))

    def load_all():
        for load in loads:
            load.start()

    @pl.when(middle)
    def _():
        load_all()

    @pl.when(ends)
    def _():
        enter()

        def both(k):
            far_copy(k, chunk_rows).start()
            own_copy(k).start()

        each(chunks, both)
        load_all()

    for load in loads[:3]:
        load.wait()
    lse32[...] = lse_ref[...].astype(jnp.float32)
    delta32[...] = delta_ref[...].astype(jnp.float32)
    seg_row = seg_ref[:, pl.ds(pl.multiple_of(tok * window, LANES), window)].astype(jnp.float32)
    seg_col = jnp.transpose(jnp.broadcast_to(seg_row, (LANES, window)))[:, :1]
    key_id = lax.broadcasted_iota(jnp.int32, (window, window), 0)
    query_id = lax.broadcasted_iota(jnp.int32, (window, window), 1)
    bias[...] = jnp.where((seg_col == seg_row) & (key_id <= query_id), 0.0, -1e30)
    dk_acc[...] = jnp.zeros_like(dk_acc)
    dv_acc[...] = jnp.zeros_like(dv_acc)
    for load in loads[3:7]:
        load.wait()

    @pl.when(middle)
    def _():
        head(0)
        enter()
        j_copy(0).start()
        each(chunks, lambda k: own_copy(k).start())

    for load in loads[7:9]:
        load.wait()

    @pl.loop(jnp.where(middle, 1, 0), groups)
    def _(r):
        head(r)

        @pl.when(middle & (r > 0) & (r % 2 == 0))
        def _():
            j_pair(r - 1).start()

    wide = groups * head_size
    joined[0, :, wide : wide + head_size] = (dk_acc[...] * scale).astype(jnp.bfloat16)
    joined[0, :, wide + head_size : wide + 2 * head_size] = dv_acc[...].astype(jnp.bfloat16)
    loads[9].wait()

    def tile(ref, lead, i, by_token):
        return ref.at[(*lead, slice(None), block_rows(i))] if by_token else ref.at[(*lead, i)]

    def part_copy(slot, yr, i, by_token):
        return remote(
            tile(part_out, (slot, yr), i, by_token),
            tile(part_in, (slot, yr), i, by_token),
            part_send.at[slot, yr, i],
            part_recv.at[slot, yr, i],
            core_peer,
        )

    def x_copy(yr, i, by_token):
        return remote(
            tile(x_out, (yr,), i, by_token),
            tile(x_in, (yr,), i, by_token),
            x_send.at[yr, i],
            x_recv.at[yr, i],
            x_peer,
        )

    def out_cols(yr, k):
        return pl.ds(pl.multiple_of(yr * rows + k * LANES, LANES), LANES)

    def out_tile(ref, yr, i, by_token):
        if by_token:
            return ref.at[block_rows(i), pl.ds(pl.multiple_of(yr * rows, LANES), rows)]
        return ref.at[:, out_cols(yr, i)]

    def back_copy(yr, i, by_token):
        return remote(
            out_tile(back_out, yr, i, by_token),
            out_tile(out_ref, yr, i, by_token),
            back_send.at[yr, i],
            back_recv.at[yr, i],
            back_peer,
        )

    def unit(slot, yr, k, side):
        value = dot(joined[side], w_all[slot, yr, chunk_rows(k)], 1, 1)

        @pl.when(mine == side)
        def _():
            keep[slot, yr, k] = value

        @pl.when(mine != side)
        def _():
            part_out[slot, yr, k] = value.astype(jnp.bfloat16)
            part_copy(slot, yr, k, False).start()

    def block_unit(slot, yr, i):
        value = dot(joined[1, block_rows(i)], w_all[slot, yr], 1, 1)

        @pl.when(mine == 1)
        def _():
            for k in range(chunks):
                keep[slot, yr, k, block_rows(i)] = value[:, k * LANES : (k + 1) * LANES]

        @pl.when(mine == 0)
        def _():
            low = value.astype(jnp.bfloat16)
            for k in range(chunks):
                part_out[slot, yr, k, block_rows(i)] = low[:, k * LANES : (k + 1) * LANES]
            part_copy(slot, yr, i, True).start()

    def small(ref, lead, a, b):
        return ref.at[(*lead, b, block_rows(a))]

    def small_part(a, b):
        return remote(
            small(part_out, (1, yo), a, b),
            small(part_in, (1, yo), a, b),
            small_part_send.at[a, b],
            small_part_recv.at[a, b],
            core_peer,
        )

    def small_x(a, b):
        return remote(
            small(x_out, (yo,), a, b),
            small(x_in, (yo,), a, b),
            small_x_send.at[a, b],
            small_x_recv.at[a, b],
            x_peer,
        )

    def small_back(a, b):
        return remote(
            back_out.at[block_rows(a), out_cols(yo, b)],
            out_ref.at[block_rows(a), out_cols(yo, b)],
            small_back_send.at[a, b],
            small_back_recv.at[a, b],
            back_peer,
        )

    def small_unit(a, b):
        value = dot(joined[1, block_rows(a)], w_all[1, yo, chunk_rows(b)], 1, 1)

        @pl.when(mine == 1)
        def _():
            keep[1, yo, b, block_rows(a)] = value

        @pl.when(mine == 0)
        def _():
            part_out[1, yo, b, block_rows(a)] = value.astype(jnp.bfloat16)
            small_part(a, b).start()

    def small_core_sum(a, b):
        small_part(a, b).wait_recv()
        kept = small(keep, (1, yo), a, b)
        value = kept[...] + small(part_in, (1, yo), a, b)[...].astype(jnp.float32)

        @pl.when(final == 1)
        def _():
            kept[...] = value

        @pl.when(final == 0)
        def _():
            small(x_out, (yo,), a, b)[...] = value.astype(jnp.bfloat16)
            small_x(a, b).start()

    def small_x_sum(a, b):
        small_x(a, b).wait_recv()
        value = small(keep, (1, yo), a, b)[...] + small(x_in, (yo,), a, b)[...].astype(jnp.float32)
        back_out[block_rows(a), out_cols(yo, b)] = value.astype(jnp.bfloat16)
        small_back(a, b).start()

    end = chunks - 1

    def direct_copy(source, peer):
        return remote(direct_out, direct_in.at[source], direct_send, direct_recv.at[source], peer)

    def direct_sum():
        part_copy(1, yo, end, False).wait_recv()
        value = keep[1, yo, end] + part_in[1, yo, end].astype(jnp.float32)
        direct_out[...] = value.astype(jnp.bfloat16)

        @pl.when(final == 1)
        def _():
            direct_copy(0, back_peer).start()

        @pl.when(final == 0)
        def _():
            direct_copy(1, cross_peer).start()

    def relayed_sum(k):
        whole = (k == end) & (mine == 1)

        @pl.when(whole)
        def _():
            direct_sum()

        @pl.when(jnp.logical_not(whole))
        def _():
            core_sum(1, yo, k, False)

    def relayed_x_sum(k):
        @pl.when((final == 1) & ((k < end) | (mine == 0)))
        def _():
            x_sum(yo, k, False)

    def added(step, body):
        def one(j):
            body(jnp.minimum(j, step), jnp.where(j <= step, step, j - step - 1))

        each(2 * step + 1, one)

    def all_small(body):
        each(chunks * chunks, lambda j: body(j // chunks, j % chunks))

    def core_sum(slot, yr, i, by_token):
        part_copy(slot, yr, i, by_token).wait_recv()
        kept = tile(keep, (slot, yr), i, by_token)
        value = kept[...] + tile(part_in, (slot, yr), i, by_token)[...].astype(jnp.float32)

        @pl.when(slot == final)
        def _():
            kept[...] = value

        @pl.when(slot != final)
        def _():
            tile(x_out, (yr,), i, by_token)[...] = value.astype(jnp.bfloat16)
            x_copy(yr, i, by_token).start()

    def x_sum(yr, i, by_token):
        x_copy(yr, i, by_token).wait_recv()
        value = tile(keep, (final, yr), i, by_token)[...]
        value += tile(x_in, (yr,), i, by_token)[...].astype(jnp.float32)
        value = value.astype(jnp.bfloat16)

        def put(ref):
            if by_token:
                for k in range(chunks):
                    ref[block_rows(i), out_cols(yr, k)] = value[k]
            else:
                ref[:, out_cols(yr, i)] = value

        if by_token:
            put(back_out)
            back_copy(yr, i, True).start()
        else:

            @pl.when(mine == 0)
            def _():
                put(out_ref)

            @pl.when(mine == 1)
            def _():
                put(back_out)
                back_copy(yr, i, False).start()

    def which(i):
        return jnp.where(i // chunks % 2 == 0, y, yo)

    lag, turns = 2, 4

    @pl.when(middle)
    def _():
        j_pair(groups - 1).start()
        j_copy(groups + 1).start()
        each(pieces, lambda p: far_copy(p, piece_rows).start())
        steps = 3 * chunks

        @pl.loop(0, steps + lag)
        def _(i):
            k = i % chunks

            @pl.when((i >= chunks) & (i < 2 * chunks))
            def _():
                arrived_far(k, chunk_rows)
                relay_copy(k, chunk_rows).start()
                arrived_own(k)

            @pl.when(i < steps)
            def _():
                unit(i // (2 * chunks), which(i), k, 0)

            @pl.when((i >= lag) & (mine == 0))
            def _():
                core_sum((i - lag) // (2 * chunks), which(i - lag), (i - lag) % chunks, False)

        @pl.loop(0, chunks + 1)
        def _(i):
            live = i < chunks

            def partner_sum(slot, yr):
                @pl.when(live & (mine == 1))
                def _():
                    core_sum(slot, yr, i, True)

            @pl.when(live)
            def _():
                j_block(i).wait_recv()

            @pl.when(live)
            def _():
                block_unit(1, y, i)

            @pl.when(live)
            def _():
                block_unit(0, y, i)

            @pl.when(live)
            def _():
                block_unit(0, yo, i)

            partner_sum(1, y)
            partner_sum(0, y)
            @pl.when((i >= 1) & (mine == 1))
            def _():
                x_sum(y, i - 1, True)

                @pl.when(final == 0)
                def _():
                    x_sum(yo, i - 1, True)

                @pl.when(final == 1)
                def _():
                    added(i - 1, small_x_sum)

            partner_sum(0, yo)
            @pl.when(live)
            def _():
                arrived_relay(i, chunk_rows)

            @pl.when(live)
            def _():
                added(i, small_unit)

            @pl.when(live & (mine == 1))
            def _():
                added(i, small_core_sum)

            @pl.when(live)
            def _():
                unit(1, yo, i, 0)

            @pl.when(mine == 0)
            def _():
                @pl.when(i >= 1)
                def _():
                    x_sum(yo, i - 1, False)

                @pl.when(live)
                def _():
                    core_sum(1, yo, i, False)
                    x_sum(y, i, False)

    @pl.when(ends)
    def _():
        each(chunks, lambda b: j_block(b).start())

        @pl.loop(0, 2 * chunks + lag)
        def _(i):
            k = i % chunks

            @pl.when((i >= chunks) & (i < 2 * chunks))
            def _():
                arrived_own(k)


            @pl.when(i < 2 * chunks)
            def _():
                unit(0, which(i), k, 0)

            @pl.when((i >= lag) & (mine == 0))
            def _():
                core_sum(0, which(i - lag), (i - lag) % chunks, False)

        all_j(lambda copy: copy.wait_recv())

        @pl.loop(0, chunks + 2)
        def _(k):
            for i in range(turns):

                @pl.when(k < chunks)
                def _():
                    for j in range(per // turns):
                        p = k * per + i * (per // turns) + j
                        arrived_far(p, piece_rows)
                        relay_copy(p, piece_rows).start()

                @pl.when(k == 0)
                def _():
                    for j in range(i * 2 * chunks // turns, (i + 1) * 2 * chunks // turns):
                        unit(0, which(j), j % chunks, 1)

                @pl.when((k == 1) & (mine == 1))
                def _():
                    for j in range(i * 2 * chunks // turns, (i + 1) * 2 * chunks // turns):
                        core_sum(0, which(j), j % chunks, False)

                @pl.when((k >= 1) & (k <= chunks))
                def _():
                    if i == 0:
                        unit(1, y, k - 1, 1)
                        unit(1, y, k - 1, 0)
                    if i == 1:
                        core_sum(1, y, k - 1, False)
                    if i == 2:
                        for j in range(per):
                            arrived_relay((k - 1) * per + j, piece_rows)
                        unit(1, yo, k - 1, 1)
                        unit(1, yo, k - 1, 0)
                    if i == 3:
                        relayed_sum(k - 1)

                        @pl.when(final == 1)
                        def _():
                            x_sum(y, k - 1, False)

                @pl.when(k >= 2)
                def _():
                    if i == 0:
                        relayed_x_sum(k - 2)

                    @pl.when((final == 0) & (k < chunks))
                    def _():
                        if i < 2:
                            x_sum((y, yo)[i], 2 * k - 4, False)
                            x_sum((y, yo)[i], 2 * k - 3, False)


    def tiles(condition, copies, wait, count=chunks):
        @pl.when(condition)
        def _():
            each(count, lambda i: wait(copies(i)))

    def smalls(condition, copies, wait):
        @pl.when(condition)
        def _():
            all_small(lambda a, b: wait(copies(a, b)))

    def received(copy):
        copy.wait_recv()

    def sent(copy):
        copy.wait_send()

    back = mine == 1
    count_in = jnp.where(middle & (final == 1), end, chunks)
    count_out = jnp.where(ends & (final == 1), end, chunks)
    count_x = jnp.where(ends & back & (final == 0), end, chunks)
    tiles(back, lambda i: back_copy(y, i, False), received)
    tiles(back & (middle | (final == 0)), lambda i: back_copy(yo, i, False), received, count_in)
    smalls(back & ends & (final == 1), small_back, received)

    @pl.when(back & middle & (final == 1))
    def _():
        direct_copy(0, back_peer).wait_recv()
        direct_copy(1, back_peer).wait_recv()
        value = direct_in[0].astype(jnp.float32) + direct_in[1].astype(jnp.float32)
        out_ref[:, out_cols(yo, end)] = value.astype(jnp.bfloat16)

    @pl.when(back & ends)
    def _():
        direct_copy(0, back_peer).wait_send()

    tiles(back, lambda i: back_copy(y, i, False), sent)
    tiles(back & (ends | (final == 0)), lambda i: back_copy(yo, i, False), sent, count_out)
    smalls(back & middle & (final == 1), small_back, sent)
    by_small = middle & (final == 0) & (mine == 1)
    tiles(jnp.logical_not(by_small), lambda i: x_copy(yo, i, False), sent, count_x)
    tiles(True, lambda i: x_copy(y, i, False), sent)
    smalls(by_small, small_x, sent)
    by_small = middle & (mine == 0)
    tiles(jnp.logical_not(by_small), lambda i: part_copy(1, yo, i, False), sent)
    smalls(by_small, small_part, sent)

    @pl.loop(0, chunks)
    def _(i):
        part_copy(0, y, i, False).wait_send()
        part_copy(0, yo, i, False).wait_send()
        part_copy(1, y, i, False).wait_send()

    each(chunks, lambda k: own_copy(k).wait_send())

    @pl.when(middle)
    def _():
        each(pieces, lambda p: far_copy(p, piece_rows).wait_send())
        each(chunks, lambda k: relay_copy(k, chunk_rows).wait_send())

    @pl.when(ends)
    def _():
        each(chunks, lambda k: far_copy(k, chunk_rows).wait_send())
        each(pieces, lambda p: relay_copy(p, piece_rows).wait_send())

    @pl.when(middle)
    def _():
        all_j(lambda copy: copy.wait_send())

    @pl.when(ends)
    def _():
        each(chunks, lambda i: j_block(i).wait_send())


def fused(sides, q, k, v, do, lse, delta, segments, weight):
    window, _, query_width = q.shape
    head_size = k.shape[2]
    rows, _, width = weight.shape
    chunks, pieces = rows // LANES, rows // PIECE
    columns = width // head_size
    bf16, f32 = jnp.bfloat16, jnp.float32
    dma = pltpu.SemaphoreType.DMA
    vmem = pl.BlockSpec(memory_space=pltpu.VMEM)
    hbm = pl.BlockSpec(memory_space=pl.ANY)
    tile = (window, LANES)
    return pl.pallas_call(
        functools.partial(fused_kernel, sides),
        out_shape=jax.ShapeDtypeStruct((window, 2 * rows), bf16),
        in_specs=[hbm] * 8,
        out_specs=vmem,
        scratch_shapes=[
            pltpu.VMEM((window, query_width), bf16),
            pltpu.VMEM((window, head_size), bf16),
            pltpu.VMEM((window, head_size), bf16),
            pltpu.VMEM((window, query_width), bf16),
            pltpu.VMEM(lse.shape[1:], bf16),
            pltpu.VMEM(lse.shape[1:], bf16),
            pltpu.VMEM((1,) + segments.shape, segments.dtype),
            pltpu.VMEM((2, window, width), bf16),
            pltpu.VMEM((2, 2, rows, width), bf16),
            pltpu.VMEM((2, 2, chunks) + tile, f32),
            pltpu.VMEM((2, 2, chunks) + tile, bf16),
            pltpu.VMEM((2, 2, chunks) + tile, bf16),
            pltpu.VMEM((2, chunks) + tile, bf16),
            pltpu.VMEM((2, chunks) + tile, bf16),
            pltpu.VMEM((window, 2 * rows), bf16),
            pltpu.VMEM(tile, bf16),
            pltpu.VMEM((2,) + tile, bf16),
            pltpu.VMEM((window, window), f32),
            pltpu.VMEM(lse.shape[1:], f32),
            pltpu.VMEM(lse.shape[1:], f32),
            pltpu.VMEM((window, head_size), f32),
            pltpu.VMEM((window, head_size), f32),
            dma((10,)),
            dma((pieces,)),
            dma((pieces,)),
            dma((pieces,)),
            dma((pieces,)),
            dma((pieces,)),
            dma((pieces,)),
            dma((columns,)),
            dma((columns,)),
            dma((2, 2, chunks)),
            dma((2, 2, chunks)),
            dma((2, chunks)),
            dma((2, chunks)),
            dma((2, chunks)),
            dma((2, chunks)),
            *[dma((chunks, chunks))] * 6,
            dma,
            dma((2,)),
        ],
        compiler_params=pltpu.CompilerParams(
            collective_id=0, has_side_effects=True, vmem_limit_bytes=40 * 1024 * 1024
        ),
    )(
        *(
            pltpu.with_memory_space_constraint(array, pltpu.HBM)
            for array in (
                q.reshape(window, query_width),
                k.reshape(window, head_size),
                v.reshape(window, head_size),
                do.reshape(window, query_width),
                lse.reshape(lse.shape[1:]),
                delta.reshape(delta.shape[1:]),
                segments.reshape(1, -1),
                weight.reshape(rows, width),
            )
        )
    )


def solution(mesh):
    placed = (
        P("tok", "head", None),
        P("tok", "head", None),
        P("tok", "head", None),
        P("tok", "head", None),
        P("head", None, "tok"),
        P("head", None, "tok"),
        P(),
        P("tok", "head", None),
    )
    tok, heads = mesh.shape["tok"], mesh.shape["head"]
    sides = tok // heads

    def step(*args):
        window, kv_dev, _ = args[0].shape
        rows = args[7].shape[0]
        paired = sides == 2 and heads == sides * sides and tok == heads * sides and kv_dev == 1
        if paired and rows == heads * LANES and window == rows and args[1].shape[2] == LANES:
            return fused(sides, *args)
        return on_device(*args)

    return jax.shard_map(
        step, mesh=mesh, in_specs=placed, out_specs=P("tok", "head"), check_vma=False
    )
```

```python
import functools

import jax
import jax.numpy as jnp
import numpy as np
from jax import lax
from jax.experimental import pallas as pl
from jax.experimental.pallas import tpu as pltpu
from jax.sharding import PartitionSpec as P

BLOCK = 128


def pair_lists(block_count):
    query_list = []
    key_list = []
    for query_block in range(block_count):
        for key_block in range(query_block + 1):
            query_list.append(query_block)
            key_list.append(key_block)
    return (np.array(query_list, np.int32), np.array(key_list, np.int32))


def live_pairs(seg_window, query_list, key_list, tile_rows):
    first_seg = jnp.take(seg_window, query_list * tile_rows)
    last_seg = jnp.take(seg_window, key_list * tile_rows + tile_rows - 1)
    return (first_seg == last_seg) | jnp.asarray(query_list == key_list)


def pair_grads(query_tile, dout_tile, key_tile, value_tile, lse_tile, delta_tile, allowed):
    tile_rows, groups, query_width = query_tile.shape
    head_size = key_tile.shape[2]
    heads_per_group = query_width // head_size
    query_heads = query_tile.reshape(tile_rows, groups, heads_per_group, head_size)
    dout_heads = dout_tile.reshape(tile_rows, groups, heads_per_group, head_size)
    scores = jnp.einsum(
        "agrd,bgd->grab", query_heads, key_tile, preferred_element_type=jnp.float32
    ) * head_size ** (-0.5)
    logits = scores - lse_tile.astype(jnp.float32)[:, :, :, None]
    soft_probs = jnp.where(allowed[None, None], jnp.exp(logits), 0.0)
    probs_low = soft_probs.astype(jnp.bfloat16)
    value_gradient = jnp.einsum(
        "grab,agrd->bgd", probs_low, dout_heads, preferred_element_type=jnp.float32
    )
    grad_prob = jnp.einsum(
        "agrd,bgd->grab", dout_heads, value_tile, preferred_element_type=jnp.float32
    )
    grad_score = (soft_probs * (grad_prob - delta_tile.astype(jnp.float32)[:, :, :, None])).astype(
        jnp.bfloat16
    )
    query_gradient = jnp.einsum(
        "grab,bgd->agrd", grad_score, key_tile, preferred_element_type=jnp.float32
    )
    key_gradient = jnp.einsum(
        "grab,agrd->bgd", grad_score, query_heads, preferred_element_type=jnp.float32
    )
    return (query_gradient.reshape(tile_rows, groups, query_width), key_gradient, value_gradient)


def on_device(
    query_rows,
    key_rows,
    value_rows,
    output_gradient,
    row_logsumexp,
    row_delta_sums,
    segments,
    query_key_value_weight,
):
    window, kv_dev, query_width = query_rows.shape
    head_size = key_rows.shape[2]
    tile_rows = BLOCK
    block_count = window // tile_rows
    query_list, key_list = pair_lists(block_count)
    query_table = jnp.asarray(query_list)
    key_table = jnp.asarray(key_list)
    myself = lax.axis_index("tok")
    own_seg = lax.dynamic_slice_in_dim(segments, myself * window, window)
    own_live = live_pairs(own_seg, query_list, key_list, tile_rows)
    block_ids = jnp.arange(block_count, dtype=jnp.int32)
    query_match = (query_table[:, None] == block_ids[None, :]) & own_live[:, None]
    key_match = key_table[:, None] == block_ids[None, :]
    block_local = jnp.any(query_match[:, :, None] & key_match[:, None, :], axis=0)
    token_local = jnp.repeat(jnp.repeat(block_local, tile_rows, axis=0), tile_rows, axis=1)
    offsets = jnp.arange(window, dtype=jnp.int32)
    allowed_all = (
        (own_seg[:, None] == own_seg[None, :])
        & (offsets[None, :] <= offsets[:, None])
        & token_local
    )
    local_out = pair_grads(
        query_rows,
        output_gradient,
        key_rows,
        value_rows,
        row_logsumexp,
        row_delta_sums,
        allowed_all,
    )
    acc_query = local_out[0].reshape(block_count, tile_rows, kv_dev, query_width)
    acc_key = local_out[1].reshape(block_count, tile_rows, kv_dev, head_size)
    acc_value = local_out[2].reshape(block_count, tile_rows, kv_dev, head_size)
    score_scale = head_size ** (-0.5)
    query_gradient = (acc_query * score_scale).reshape(window, kv_dev, query_width)
    key_gradient = (acc_key * score_scale).reshape(window, kv_dev, head_size)
    value_gradient = acc_value.reshape(window, kv_dev, head_size)
    stacked_gradients = (
        jnp.concatenate([query_gradient, key_gradient, value_gradient], axis=2)
        .astype(jnp.bfloat16)
        .reshape(window, -1)
    )
    weight_piece = lax.all_gather(query_key_value_weight, "tok", axis=0, tiled=True)
    flat_piece = weight_piece.reshape(weight_piece.shape[0], -1)
    partial_sum = lax.dot_general(
        stacked_gradients, flat_piece, (((1,), (1,)), ((), ())), preferred_element_type=jnp.float32
    )
    summed = lax.psum_scatter(
        partial_sum.astype(jnp.bfloat16), "head", scatter_dimension=1, tiled=True
    )
    return summed


MESH = pl.DeviceIdType.MESH
LANES = 128
PIECE = 32


def fused_kernel(
    sides,
    q_hbm,
    k_hbm,
    v_hbm,
    do_hbm,
    lse_hbm,
    delta_hbm,
    seg_hbm,
    w_hbm,
    out_ref,
    q_ref,
    k_ref,
    v_ref,
    do_ref,
    lse_ref,
    delta_ref,
    seg_ref,
    joined,
    w_all,
    keep,
    part_out,
    part_in,
    x_out,
    x_in,
    back_out,
    direct_out,
    direct_in,
    bias,
    lse32,
    delta32,
    dk_acc,
    dv_acc,
    load_sem,
    own_send,
    own_recv,
    far_send,
    far_recv,
    relay_send,
    relay_recv,
    j_send,
    j_recv,
    part_send,
    part_recv,
    x_send,
    x_recv,
    back_send,
    back_recv,
    small_part_send,
    small_part_recv,
    small_x_send,
    small_x_recv,
    small_back_send,
    small_back_recv,
    direct_send,
    direct_recv,
):
    window, head_size = k_ref.shape
    groups = q_ref.shape[1] // head_size
    rows = w_hbm.shape[0]
    chunks, pieces = rows // LANES, rows // PIECE
    per = LANES // PIECE
    block = window // chunks
    columns = groups + 2
    tok, h = lax.axis_index("tok"), lax.axis_index("head")
    z, y = tok // sides, tok % sides
    x, c = h // sides, h % sides
    yo, xo, co = 1 - y, 1 - x, 1 - c
    odd, upper = z % sides, z // sides
    partner = z + 1 - 2 * odd
    far = z + sides - 2 * sides * upper
    middle = upper != odd
    ends = jnp.logical_not(middle)
    mine = jnp.where(c == odd, 0, 1)
    final = jnp.where(x == upper, 0, 1)

    def device(dz, dy, dx, dc):
        return (dz * sides + dy, dx * sides + dc)

    y_peer = device(z, yo, x, c)
    far_peer = device(far, y, x, c)
    j_peer = device(partner, y, x, c)
    core_peer = device(z, y, x, co)
    x_peer = device(z, y, xo, c)
    back_peer = device(partner, y, x, co)

    loads = [
        pltpu.make_async_copy(src, dst, load_sem.at[i])
        for i, (src, dst) in enumerate(
            (
                (seg_hbm, seg_ref),
                (lse_hbm, lse_ref),
                (delta_hbm, delta_ref),
                (k_hbm, k_ref),
                (v_hbm, v_ref),
                (q_hbm.at[:, :head_size], q_ref.at[:, :head_size]),
                (do_hbm.at[:, :head_size], do_ref.at[:, :head_size]),
                (q_hbm.at[:, head_size:], q_ref.at[:, head_size:]),
                (do_hbm.at[:, head_size:], do_ref.at[:, head_size:]),
                (w_hbm, w_all.at[0, y]),
            )
        )
    ]
    barrier = pltpu.get_barrier_semaphore()
    cross_peer = device(partner, y, xo, co)
    peers = (far_peer, cross_peer, j_peer, back_peer, y_peer, x_peer, core_peer)
    for peer in peers:
        pl.semaphore_signal(barrier, inc=1, device_id=peer, device_id_type=MESH)

    def j_cols(r):
        return pl.ds(pl.multiple_of(r * head_size, head_size), head_size)

    scale = head_size ** (-0.5)
    half = window // 2

    def dot(a, b, da, db):
        return lax.dot_general(a, b, (((da,), (db,)), ((), ())), preferred_element_type=jnp.float32)

    def head(r):
        cols = j_cols(r)
        sums = []
        for start in (0, half):
            keys, queries = slice(start, start + half), slice(start, window)
            q, do = q_ref[queries, cols], do_ref[queries, cols]
            kk, vv = k_ref[keys, :], v_ref[keys, :]
            logits = dot(kk, q, 1, 1) * scale - lse32[pl.ds(r, 1), queries]
            probs = jnp.exp(logits + bias[keys, queries])
            dv_acc[keys, :] += dot(probs.astype(jnp.bfloat16), do, 1, 0)
            grad_prob = dot(vv, do, 1, 1)
            ds = (probs * (grad_prob - delta32[pl.ds(r, 1), queries])).astype(jnp.bfloat16)
            dk_acc[keys, :] += dot(ds, q, 1, 0)
            sums.append(dot(ds, kk, 0, 0))
        low = sums[0]
        joined[0, :half, cols] = (low[:half] * scale).astype(jnp.bfloat16)
        joined[0, half:, cols] = ((low[half:] + sums[1]) * scale).astype(jnp.bfloat16)

    def remote(src, dst, send, recv, peer):
        return pltpu.make_async_remote_copy(
            src_ref=src,
            dst_ref=dst,
            send_sem=send,
            recv_sem=recv,
            device_id=peer,
            device_id_type=MESH,
        )

    def piece_rows(p):
        return pl.ds(pl.multiple_of(p * PIECE, PIECE), PIECE)

    def chunk_rows(k):
        return pl.ds(pl.multiple_of(k * LANES, LANES), LANES)

    def block_rows(i):
        return pl.ds(pl.multiple_of(i * block, block), block)

    def own_copy(k):
        return remote(
            w_hbm.at[chunk_rows(k)],
            w_all.at[0, y, chunk_rows(k)],
            own_send.at[k],
            own_recv.at[k],
            y_peer,
        )

    def arrived_own(k):
        ref = w_all.at[0, yo, chunk_rows(k)]
        remote(ref, ref, own_send.at[k], own_recv.at[k], y_peer).wait_recv()

    def far_copy(p, part):
        return remote(
            w_hbm.at[part(p)],
            w_all.at[1, y, part(p)],
            far_send.at[p],
            far_recv.at[p],
            far_peer,
        )

    def relay_copy(p, part):
        ref = w_all.at[1, y, part(p)]
        return remote(ref, ref, relay_send.at[p], relay_recv.at[p], y_peer)

    def arrived_far(p, part):
        ref = w_all.at[1, y, part(p)]
        remote(ref, ref, far_send.at[p], far_recv.at[p], far_peer).wait_recv()

    def arrived_relay(p, part):
        ref = w_all.at[1, yo, part(p)]
        remote(ref, ref, relay_send.at[p], relay_recv.at[p], y_peer).wait_recv()

    def j_copy(r):
        return remote(
            joined.at[0, :, j_cols(r)],
            joined.at[1, :, j_cols(r)],
            j_send.at[r],
            j_recv.at[r],
            j_peer,
        )

    def j_pair(r):
        cols = pl.ds(pl.multiple_of(r * head_size, head_size), 2 * head_size)
        return remote(
            joined.at[0, :, cols], joined.at[1, :, cols], j_send.at[r], j_recv.at[r], j_peer
        )

    def all_j(wait):
        wait(j_copy(0))
        each((columns - 2) // 2, lambda i: wait(j_pair(2 * i + 1)))
        wait(j_copy(columns - 1))

    def j_block(i):
        return remote(
            joined.at[0, block_rows(i)],
            joined.at[1, block_rows(i)],
            j_send.at[i],
            j_recv.at[i],
            j_peer,
        )

    def each(count, body):
        lax.fori_loop(0, count, lambda i, carry: (body(i), carry)[1], 0)

    def enter():
        pl.semaphore_wait(barrier, len(peers))

    def load_all():
        for load in loads:
            load.start()

    @pl.when(middle)
    def _():
        load_all()

    @pl.when(ends)
    def _():
        enter()

        def both(k):
            far_copy(k, chunk_rows).start()
            own_copy(k).start()

        each(chunks, both)
        load_all()

    for load in loads[:3]:
        load.wait()
    lse32[...] = lse_ref[...].astype(jnp.float32)
    delta32[...] = delta_ref[...].astype(jnp.float32)
    seg_row = seg_ref[:, pl.ds(pl.multiple_of(tok * window, LANES), window)].astype(jnp.float32)
    seg_col = jnp.transpose(jnp.broadcast_to(seg_row, (LANES, window)))[:, :1]
    key_id = lax.broadcasted_iota(jnp.int32, (window, window), 0)
    query_id = lax.broadcasted_iota(jnp.int32, (window, window), 1)
    bias[...] = jnp.where((seg_col == seg_row) & (key_id <= query_id), 0.0, -1e30)
    dk_acc[...] = jnp.zeros_like(dk_acc)
    dv_acc[...] = jnp.zeros_like(dv_acc)
    for load in loads[3:7]:
        load.wait()

    @pl.when(middle)
    def _():
        head(0)
        enter()
        j_copy(0).start()
        each(chunks, lambda k: own_copy(k).start())

    for load in loads[7:9]:
        load.wait()

    @pl.loop(jnp.where(middle, 1, 0), groups)
    def _(r):
        head(r)

        @pl.when(middle & (r > 0) & (r % 2 == 0))
        def _():
            j_pair(r - 1).start()

    wide = groups * head_size
    joined[0, :, wide : wide + head_size] = (dk_acc[...] * scale).astype(jnp.bfloat16)
    joined[0, :, wide + head_size : wide + 2 * head_size] = dv_acc[...].astype(jnp.bfloat16)
    loads[9].wait()

    def tile(ref, lead, i, by_token):
        return ref.at[(*lead, slice(None), block_rows(i))] if by_token else ref.at[(*lead, i)]

    def part_copy(slot, yr, i, by_token):
        return remote(
            tile(part_out, (slot, yr), i, by_token),
            tile(part_in, (slot, yr), i, by_token),
            part_send.at[slot, yr, i],
            part_recv.at[slot, yr, i],
            core_peer,
        )

    def x_copy(yr, i, by_token):
        return remote(
            tile(x_out, (yr,), i, by_token),
            tile(x_in, (yr,), i, by_token),
            x_send.at[yr, i],
            x_recv.at[yr, i],
            x_peer,
        )

    def out_cols(yr, k):
        return pl.ds(pl.multiple_of(yr * rows + k * LANES, LANES), LANES)

    def out_tile(ref, yr, i, by_token):
        if by_token:
            return ref.at[block_rows(i), pl.ds(pl.multiple_of(yr * rows, LANES), rows)]
        return ref.at[:, out_cols(yr, i)]

    def back_copy(yr, i, by_token):
        return remote(
            out_tile(back_out, yr, i, by_token),
            out_tile(out_ref, yr, i, by_token),
            back_send.at[yr, i],
            back_recv.at[yr, i],
            back_peer,
        )

    def unit(slot, yr, k, side):
        value = dot(joined[side], w_all[slot, yr, chunk_rows(k)], 1, 1)

        @pl.when(mine == side)
        def _():
            keep[slot, yr, k] = value

        @pl.when(mine != side)
        def _():
            part_out[slot, yr, k] = value.astype(jnp.bfloat16)
            part_copy(slot, yr, k, False).start()

    def block_unit(slot, yr, i):
        value = dot(joined[1, block_rows(i)], w_all[slot, yr], 1, 1)

        @pl.when(mine == 1)
        def _():
            for k in range(chunks):
                keep[slot, yr, k, block_rows(i)] = value[:, k * LANES : (k + 1) * LANES]

        @pl.when(mine == 0)
        def _():
            low = value.astype(jnp.bfloat16)
            for k in range(chunks):
                part_out[slot, yr, k, block_rows(i)] = low[:, k * LANES : (k + 1) * LANES]
            part_copy(slot, yr, i, True).start()

    def small(ref, lead, a, b):
        return ref.at[(*lead, b, block_rows(a))]

    def small_part(a, b):
        return remote(
            small(part_out, (1, yo), a, b),
            small(part_in, (1, yo), a, b),
            small_part_send.at[a, b],
            small_part_recv.at[a, b],
            core_peer,
        )

    def small_x(a, b):
        return remote(
            small(x_out, (yo,), a, b),
            small(x_in, (yo,), a, b),
            small_x_send.at[a, b],
            small_x_recv.at[a, b],
            x_peer,
        )

    def small_back(a, b):
        return remote(
            back_out.at[block_rows(a), out_cols(yo, b)],
            out_ref.at[block_rows(a), out_cols(yo, b)],
            small_back_send.at[a, b],
            small_back_recv.at[a, b],
            back_peer,
        )

    def small_unit(a, b):
        value = dot(joined[1, block_rows(a)], w_all[1, yo, chunk_rows(b)], 1, 1)

        @pl.when(mine == 1)
        def _():
            keep[1, yo, b, block_rows(a)] = value

        @pl.when(mine == 0)
        def _():
            part_out[1, yo, b, block_rows(a)] = value.astype(jnp.bfloat16)
            small_part(a, b).start()

    def small_core_sum(a, b):
        small_part(a, b).wait_recv()
        kept = small(keep, (1, yo), a, b)
        value = kept[...] + small(part_in, (1, yo), a, b)[...].astype(jnp.float32)

        @pl.when(final == 1)
        def _():
            kept[...] = value

        @pl.when(final == 0)
        def _():
            small(x_out, (yo,), a, b)[...] = value.astype(jnp.bfloat16)
            small_x(a, b).start()

    def small_x_sum(a, b):
        small_x(a, b).wait_recv()
        value = small(keep, (1, yo), a, b)[...] + small(x_in, (yo,), a, b)[...].astype(jnp.float32)
        back_out[block_rows(a), out_cols(yo, b)] = value.astype(jnp.bfloat16)
        small_back(a, b).start()

    end = chunks - 1

    def direct_copy(source, peer):
        return remote(direct_out, direct_in.at[source], direct_send, direct_recv.at[source], peer)

    def direct_sum():
        part_copy(1, yo, end, False).wait_recv()
        value = keep[1, yo, end] + part_in[1, yo, end].astype(jnp.float32)
        direct_out[...] = value.astype(jnp.bfloat16)

        @pl.when(final == 1)
        def _():
            direct_copy(0, back_peer).start()

        @pl.when(final == 0)
        def _():
            direct_copy(1, cross_peer).start()

    def relayed_sum(k):
        whole = (k == end) & (mine == 1)

        @pl.when(whole)
        def _():
            direct_sum()

        @pl.when(jnp.logical_not(whole))
        def _():
            core_sum(1, yo, k, False)

    def relayed_x_sum(k):
        @pl.when((final == 1) & ((k < end) | (mine == 0)))
        def _():
            x_sum(yo, k, False)

    def added(step, body):
        def one(j):
            body(jnp.minimum(j, step), jnp.where(j <= step, step, j - step - 1))

        each(2 * step + 1, one)

    def all_small(body):
        each(chunks * chunks, lambda j: body(j // chunks, j % chunks))

    def core_sum(slot, yr, i, by_token):
        part_copy(slot, yr, i, by_token).wait_recv()
        kept = tile(keep, (slot, yr), i, by_token)
        value = kept[...] + tile(part_in, (slot, yr), i, by_token)[...].astype(jnp.float32)

        @pl.when(slot == final)
        def _():
            kept[...] = value

        @pl.when(slot != final)
        def _():
            tile(x_out, (yr,), i, by_token)[...] = value.astype(jnp.bfloat16)
            x_copy(yr, i, by_token).start()

    def x_sum(yr, i, by_token):
        x_copy(yr, i, by_token).wait_recv()
        value = tile(keep, (final, yr), i, by_token)[...]
        value += tile(x_in, (yr,), i, by_token)[...].astype(jnp.float32)
        value = value.astype(jnp.bfloat16)

        def put(ref):
            if by_token:
                for k in range(chunks):
                    ref[block_rows(i), out_cols(yr, k)] = value[k]
            else:
                ref[:, out_cols(yr, i)] = value

        if by_token:
            put(back_out)
            back_copy(yr, i, True).start()
        else:

            @pl.when(mine == 0)
            def _():
                put(out_ref)

            @pl.when(mine == 1)
            def _():
                put(back_out)
                back_copy(yr, i, False).start()

    def which(i):
        return jnp.where(i // chunks % 2 == 0, y, yo)

    lag, turns = 2, 4

    @pl.when(middle)
    def _():
        j_pair(groups - 1).start()
        j_copy(groups + 1).start()
        each(pieces, lambda p: far_copy(p, piece_rows).start())
        steps = 3 * chunks

        @pl.loop(0, steps + lag)
        def _(i):
            k = i % chunks

            @pl.when((i >= chunks) & (i < 2 * chunks))
            def _():
                arrived_far(k, chunk_rows)
                relay_copy(k, chunk_rows).start()
                arrived_own(k)

            @pl.when(i < steps)
            def _():
                unit(i // (2 * chunks), which(i), k, 0)

            @pl.when((i >= lag) & (mine == 0))
            def _():
                core_sum((i - lag) // (2 * chunks), which(i - lag), (i - lag) % chunks, False)

        @pl.loop(0, chunks + 1)
        def _(i):
            live = i < chunks

            def partner_sum(slot, yr):
                @pl.when(live & (mine == 1))
                def _():
                    core_sum(slot, yr, i, True)

            @pl.when(live)
            def _():
                j_block(i).wait_recv()

            @pl.when(live)
            def _():
                block_unit(1, y, i)

            @pl.when(live)
            def _():
                block_unit(0, y, i)

            @pl.when(live)
            def _():
                block_unit(0, yo, i)

            partner_sum(1, y)
            partner_sum(0, y)
            @pl.when((i >= 1) & (mine == 1))
            def _():
                x_sum(y, i - 1, True)

                @pl.when(final == 0)
                def _():
                    x_sum(yo, i - 1, True)

                @pl.when(final == 1)
                def _():
                    added(i - 1, small_x_sum)

            partner_sum(0, yo)
            @pl.when(live)
            def _():
                arrived_relay(i, chunk_rows)

            @pl.when(live)
            def _():
                added(i, small_unit)

            @pl.when(live & (mine == 1))
            def _():
                added(i, small_core_sum)

            @pl.when(live)
            def _():
                unit(1, yo, i, 0)

            @pl.when(mine == 0)
            def _():
                @pl.when(i >= 1)
                def _():
                    x_sum(yo, i - 1, False)

                @pl.when(live)
                def _():
                    core_sum(1, yo, i, False)
                    x_sum(y, i, False)

    @pl.when(ends)
    def _():
        each(chunks, lambda b: j_block(b).start())

        @pl.loop(0, 2 * chunks + lag)
        def _(i):
            k = i % chunks

            @pl.when((i >= chunks) & (i < 2 * chunks))
            def _():
                arrived_own(k)


            @pl.when(i < 2 * chunks)
            def _():
                unit(0, which(i), k, 0)

            @pl.when((i >= lag) & (mine == 0))
            def _():
                core_sum(0, which(i - lag), (i - lag) % chunks, False)

        all_j(lambda copy: copy.wait_recv())

        @pl.loop(0, chunks + 2)
        def _(k):
            for i in range(turns):

                @pl.when(k < chunks)
                def _():
                    for j in range(per // turns):
                        p = k * per + i * (per // turns) + j
                        arrived_far(p, piece_rows)
                        relay_copy(p, piece_rows).start()

                @pl.when(k == 0)
                def _():
                    for j in range(i * 2 * chunks // turns, (i + 1) * 2 * chunks // turns):
                        unit(0, which(j), j % chunks, 1)

                @pl.when((k == 1) & (mine == 1))
                def _():
                    for j in range(i * 2 * chunks // turns, (i + 1) * 2 * chunks // turns):
                        core_sum(0, which(j), j % chunks, False)

                @pl.when((k >= 1) & (k <= chunks))
                def _():
                    if i == 0:
                        unit(1, y, k - 1, 1)
                        unit(1, y, k - 1, 0)
                    if i == 1:
                        core_sum(1, y, k - 1, False)
                    if i == 2:
                        for j in range(per):
                            arrived_relay((k - 1) * per + j, piece_rows)
                        unit(1, yo, k - 1, 1)
                        unit(1, yo, k - 1, 0)
                    if i == 3:
                        relayed_sum(k - 1)

                        @pl.when(final == 1)
                        def _():
                            x_sum(y, k - 1, False)

                @pl.when(k >= 2)
                def _():
                    if i == 0:
                        relayed_x_sum(k - 2)

                    @pl.when((final == 0) & (k < chunks))
                    def _():
                        if i < 2:
                            x_sum((y, yo)[i], 2 * k - 4, False)
                            x_sum((y, yo)[i], 2 * k - 3, False)


    def tiles(condition, copies, wait, count=chunks):
        @pl.when(condition)
        def _():
            each(count, lambda i: wait(copies(i)))

    def smalls(condition, copies, wait):
        @pl.when(condition)
        def _():
            all_small(lambda a, b: wait(copies(a, b)))

    def received(copy):
        copy.wait_recv()

    def sent(copy):
        copy.wait_send()

    back = mine == 1
    count_in = jnp.where(middle & (final == 1), end, chunks)
    count_out = jnp.where(ends & (final == 1), end, chunks)
    count_x = jnp.where(ends & back & (final == 0), end, chunks)
    tiles(back, lambda i: back_copy(y, i, False), received)
    tiles(back & (middle | (final == 0)), lambda i: back_copy(yo, i, False), received, count_in)
    smalls(back & ends & (final == 1), small_back, received)

    @pl.when(back & middle & (final == 1))
    def _():
        direct_copy(0, back_peer).wait_recv()
        direct_copy(1, back_peer).wait_recv()
        value = direct_in[0].astype(jnp.float32) + direct_in[1].astype(jnp.float32)
        out_ref[:, out_cols(yo, end)] = value.astype(jnp.bfloat16)

    @pl.when(back & ends)
    def _():
        direct_copy(0, back_peer).wait_send()

    tiles(back, lambda i: back_copy(y, i, False), sent)
    tiles(back & (ends | (final == 0)), lambda i: back_copy(yo, i, False), sent, count_out)
    smalls(back & middle & (final == 1), small_back, sent)
    by_small = middle & (final == 0) & (mine == 1)
    tiles(jnp.logical_not(by_small), lambda i: x_copy(yo, i, False), sent, count_x)
    tiles(True, lambda i: x_copy(y, i, False), sent)
    smalls(by_small, small_x, sent)
    by_small = middle & (mine == 0)
    tiles(jnp.logical_not(by_small), lambda i: part_copy(1, yo, i, False), sent)
    smalls(by_small, small_part, sent)

    @pl.loop(0, chunks)
    def _(i):
        part_copy(0, y, i, False).wait_send()
        part_copy(0, yo, i, False).wait_send()
        part_copy(1, y, i, False).wait_send()

    each(chunks, lambda k: own_copy(k).wait_send())

    @pl.when(middle)
    def _():
        each(pieces, lambda p: far_copy(p, piece_rows).wait_send())
        each(chunks, lambda k: relay_copy(k, chunk_rows).wait_send())

    @pl.when(ends)
    def _():
        each(chunks, lambda k: far_copy(k, chunk_rows).wait_send())
        each(pieces, lambda p: relay_copy(p, piece_rows).wait_send())

    @pl.when(middle)
    def _():
        all_j(lambda copy: copy.wait_send())

    @pl.when(ends)
    def _():
        each(chunks, lambda i: j_block(i).wait_send())


def fused(sides, q, k, v, do, lse, delta, segments, weight):
    window, _, query_width = q.shape
    head_size = k.shape[2]
    rows, _, width = weight.shape
    chunks, pieces = rows // LANES, rows // PIECE
    columns = width // head_size
    bf16, f32 = jnp.bfloat16, jnp.float32
    dma = pltpu.SemaphoreType.DMA
    vmem = pl.BlockSpec(memory_space=pltpu.VMEM)
    hbm = pl.BlockSpec(memory_space=pl.ANY)
    tile = (window, LANES)
    return pl.pallas_call(
        functools.partial(fused_kernel, sides),
        out_shape=jax.ShapeDtypeStruct((window, 2 * rows), bf16),
        in_specs=[hbm] * 8,
        out_specs=vmem,
        scratch_shapes=[
            pltpu.VMEM((window, query_width), bf16),
            pltpu.VMEM((window, head_size), bf16),
            pltpu.VMEM((window, head_size), bf16),
            pltpu.VMEM((window, query_width), bf16),
            pltpu.VMEM(lse.shape[1:], bf16),
            pltpu.VMEM(lse.shape[1:], bf16),
            pltpu.VMEM((1,) + segments.shape, segments.dtype),
            pltpu.VMEM((2, window, width), bf16),
            pltpu.VMEM((2, 2, rows, width), bf16),
            pltpu.VMEM((2, 2, chunks) + tile, f32),
            pltpu.VMEM((2, 2, chunks) + tile, bf16),
            pltpu.VMEM((2, 2, chunks) + tile, bf16),
            pltpu.VMEM((2, chunks) + tile, bf16),
            pltpu.VMEM((2, chunks) + tile, bf16),
            pltpu.VMEM((window, 2 * rows), bf16),
            pltpu.VMEM(tile, bf16),
            pltpu.VMEM((2,) + tile, bf16),
            pltpu.VMEM((window, window), f32),
            pltpu.VMEM(lse.shape[1:], f32),
            pltpu.VMEM(lse.shape[1:], f32),
            pltpu.VMEM((window, head_size), f32),
            pltpu.VMEM((window, head_size), f32),
            dma((10,)),
            dma((pieces,)),
            dma((pieces,)),
            dma((pieces,)),
            dma((pieces,)),
            dma((pieces,)),
            dma((pieces,)),
            dma((columns,)),
            dma((columns,)),
            dma((2, 2, chunks)),
            dma((2, 2, chunks)),
            dma((2, chunks)),
            dma((2, chunks)),
            dma((2, chunks)),
            dma((2, chunks)),
            *[dma((chunks, chunks))] * 6,
            dma,
            dma((2,)),
        ],
        compiler_params=pltpu.CompilerParams(
            collective_id=0, has_side_effects=True, vmem_limit_bytes=40 * 1024 * 1024
        ),
    )(
        *(
            pltpu.with_memory_space_constraint(array, pltpu.HBM)
            for array in (
                q.reshape(window, query_width),
                k.reshape(window, head_size),
                v.reshape(window, head_size),
                do.reshape(window, query_width),
                lse.reshape(lse.shape[1:]),
                delta.reshape(delta.shape[1:]),
                segments.reshape(1, -1),
                weight.reshape(rows, width),
            )
        )
    )


def solution(mesh):
    placed = (
        P("tok", "head", None),
        P("tok", "head", None),
        P("tok", "head", None),
        P("tok", "head", None),
        P("head", None, "tok"),
        P("head", None, "tok"),
        P(),
        P("tok", "head", None),
    )
    tok, heads = mesh.shape["tok"], mesh.shape["head"]
    sides = tok // heads

    def step(*args):
        window, kv_dev, _ = args[0].shape
        rows = args[7].shape[0]
        paired = sides == 2 and heads == sides * sides and tok == heads * sides and kv_dev == 1
        if paired and rows == heads * LANES and window == rows and args[1].shape[2] == LANES:
            return fused(sides, *args)
        return on_device(*args)

    return jax.shard_map(
        step, mesh=mesh, in_specs=placed, out_specs=P("tok", "head"), check_vma=False
    )
```
